256 devices in a mesh: pop: 64 (over x, z, core), mp: 4 (over y).
Axes of the slice: x: 4, y: 4, z: 8, core: 2. Of those that a mesh axis runs over, the one named last changes fastest.
Arguments:
- tokens: bfloat16 [256, 3584], replicated, may hold values from -60 to 60
- target: bfloat16 [256, 3584], P(None, 'mp'), may hold values from -6 to 6
- w_query: bfloat16 [3584, 3584], P('pop', 'mp'), may hold values from -0.09375 to 0.09375
- w_key: bfloat16 [3584, 512], P(None, 'mp'), may hold values from -0.09375 to 0.09375
- w_value: bfloat16 [3584, 512], P(None, 'mp'), may hold values from -0.09375 to 0.09375
- w_out: bfloat16 [3584, 3584], P('mp', 'pop'), may hold values from -0.09375 to 0.09375
- query_left_factors: bfloat16 [64, 3584, 4], P('pop'), may hold values from -0.09375 to 0.09375
- query_right_factors: bfloat16 [64, 4, 3584], P('pop', None, 'mp'), may hold values from -6 to 6
- o_left: bfloat16 [64, 3584, 4], P('pop', 'mp'), may hold values from -0.09375 to 0.09375
- o_right: bfloat16 [64, 4, 3584], P('pop'), may hold values from -6 to 6
- member_ids: int32 [64], P('pop'), may hold values from 0 to 63, each once
Outputs:
- grad_query: float32 [3584, 3584], P('pop', 'mp')
- grad_out: float32 [3584, 3584], P('mp', 'pop')
- fitness: float32 [64], P('pop')
The draws below stay inside these ranges and needn't reach their ends.
Inputs may be any that keep to these rules, and one draw needn't show every extreme that they name: `member_ids`: every number from 0 to 63 appears once.
All inputs are finite; a program needn't handle non-finite values.
Results may differ from the reference program's by a relative error of at most 0.005.
Values may be sent and summed in bfloat16 or wider, within the bound.
No kernel may reach another device: no remote copies, remote signals or barrier semaphores. Data moves between devices by JAX's collectives and lax.ppermute only.
A program may use at most 64 MiB of HBM per device.

```python
import math
import jax
import jax.numpy as jnp
from jax import lax

D = 3584
HEADS = 28
KV_HEADS = 4
HEAD_DIM = 128
RANK = 4
TOK = 256
F = 3584
KVF = 512
M = 64
N_MP = 4


def draw_tokens(key, part):
    first = jax.random.fold_in(key, 0)
    normal = jax.random.normal(first, (TOK, D), jnp.float32)
    return jnp.clip(normal, -5.0, 5.0).astype(jnp.bfloat16)


def level_of(stream_key, dims, cuts, low, largest):
    def one(axis_at, parts):
        draws = jax.random.uniform(jax.random.fold_in(jax.random.fold_in(stream_key, 6), axis_at), (parts,), jnp.float32, low / len(cuts), largest / len(cuts))
        return jnp.repeat(jnp.exp(draws), dims[axis_at] // parts).reshape((-1,) + (1,) * (len(dims) - axis_at - 1))

    gain = one(*cuts[0])
    for cut in cuts[1:]:
        gain = gain * one(*cut)
    return gain


def normal_values(stream_key, shape, scale, bound, shards=(), held_as=jnp.bfloat16):
    result = scale * jax.random.normal(stream_key, shape, jnp.float32)
    if shards:
        result = result * level_of(stream_key, shape, shards, -0.22, 0.18)
    return jnp.clip(result, -bound, bound).astype(held_as)


def setup_inputs(seed: int = 0) -> dict:
    key_list = jax.random.split(jax.random.key(seed), 12)
    return {
        "tokens": draw_tokens(jax.random.fold_in(key_list[11], 71), 0),
        "target": normal_values(key_list[1], (TOK, D), 1.0, 6.0, ((1, 4),)),
        "w_query": normal_values(key_list[2], (D, F), D ** -0.5, 0.09375, ((0, 64), (1, 4))),
        "w_key": normal_values(key_list[3], (D, KVF), D ** -0.5, 0.09375, ((1, 4),)),
        "w_value": normal_values(key_list[4], (D, KVF), D ** -0.5, 0.09375, ((1, 4),)),
        "w_out": normal_values(key_list[5], (F, D), F ** -0.5, 0.09375, ((0, 4), (1, 64))),
        "query_left_factors": normal_values(key_list[6], (M, D, RANK), D ** -0.5, 0.09375, ((0, 64),)),
        "query_right_factors": normal_values(key_list[7], (M, RANK, F), 1.0, 6.0, ((0, 64), (2, 4))),
        "o_left": normal_values(key_list[8], (M, F, RANK), F ** -0.5, 0.09375, ((0, 64), (1, 4))),
        "o_right": normal_values(key_list[9], (M, RANK, D), 1.0, 6.0, ((0, 64),)),
        "member_ids": jax.random.permutation(key_list[10], M).astype(jnp.int32),
    }


noise_scale = 0.5
rope_base = 1000000.0
spread_floor = 0.001

def tables(count, head_size):
    position = jnp.arange(count, dtype=jnp.float32)
    index = jnp.arange(head_size // 2, dtype=jnp.float32)
    freq = jnp.exp(-math.log(rope_base) * 2.0 * index / head_size)
    angle = position[:, None] * freq[None, :]
    return (jnp.cos(angle)[:, None, :], jnp.sin(angle)[:, None, :])

def rotate(field, cosine_table, sine):
    half = field.shape[-1] // 2
    first = field[..., :half]
    second = field[..., half:]
    return jnp.concatenate([first * cosine_table - second * sine, second * cosine_table + first * sine], axis=-1)

def reference(tokens, target, w_query, w_key, w_value, w_out, query_left_factors, query_right_factors, o_left, o_right, member_ids):
    tok = tokens.shape[0]
    width = tokens.shape[1]
    hidden = w_query.shape[1]
    members = query_left_factors.shape[0]
    group = HEADS // KV_HEADS
    block = hidden // N_MP
    scale = HEAD_DIM ** (-0.5)
    cosine_table, sine = tables(tok, HEAD_DIM)
    base = jnp.dot(tokens, w_query, preferred_element_type=jnp.float32)
    keys = rotate(jnp.dot(tokens, w_key, preferred_element_type=jnp.float32).reshape(tok, KV_HEADS, HEAD_DIM), cosine_table, sine).astype(jnp.bfloat16)
    values = jnp.dot(tokens, w_value, preferred_element_type=jnp.float32).astype(jnp.bfloat16).reshape(tok, KV_HEADS, HEAD_DIM)
    signs = (1 - 2 * (member_ids % 2)).astype(jnp.float32)
    causal = jnp.arange(tok)[:, None] >= jnp.arange(tok)[None, :]
    target_f = target.astype(jnp.float32)

    def score(index):
        sign = signs[index]
        lowrank_product = jnp.dot(tokens, query_left_factors[index], preferred_element_type=jnp.float32).astype(jnp.bfloat16)
        query = base + noise_scale * sign * jnp.dot(lowrank_product, query_right_factors[index], preferred_element_type=jnp.float32)
        query = rotate(query.reshape(tok, HEADS, HEAD_DIM), cosine_table, sine).astype(jnp.bfloat16)
        query = query.reshape(tok, KV_HEADS, group, HEAD_DIM)
        scores = jnp.einsum('tkgd,skd->kgts', query.astype(jnp.float32), keys.astype(jnp.float32)) * scale
        scores = jnp.where(causal, scores, -1e+30)
        probs = jax.nn.softmax(scores, axis=-1).astype(jnp.bfloat16)
        mixed = jnp.einsum('kgts,skd->tkgd', probs.astype(jnp.float32), values.astype(jnp.float32)).astype(jnp.bfloat16).reshape(tok, hidden)
        total = jnp.zeros((tok, width), jnp.float32)
        for part in range(N_MP):
            rows = mixed[:, part * block:(part + 1) * block]
            low_out = jnp.dot(rows, o_left[index, part * block:(part + 1) * block], preferred_element_type=jnp.float32)
            term = jnp.dot(rows, w_out[part * block:(part + 1) * block], preferred_element_type=jnp.float32)
            term = term + noise_scale * sign * jnp.dot(low_out, o_right[index].astype(jnp.float32), precision=lax.Precision.HIGHEST)
            rounded = lax.optimization_barrier(term.astype(jnp.bfloat16))
            total = total + rounded.astype(jnp.float32)
        diff = total - target_f
        return -(jnp.sum(diff * diff) / (tok * width))
    fitness = lax.map(score, jnp.arange(members))
    mean = jnp.sum(fitness) / members
    spread = jnp.sum((fitness - mean) * (fitness - mean)) / members
    weight = signs * (fitness - mean) / jnp.sqrt(spread + spread_floor)
    left_q = jnp.transpose(query_left_factors.astype(jnp.float32) * weight[:, None, None], (1, 0, 2)).reshape(width, members * RANK)
    right_q = query_right_factors.astype(jnp.float32).reshape(members * RANK, hidden)
    grad_query = jnp.dot(left_q, right_q, precision=lax.Precision.HIGHEST) / noise_scale
    output_left_factor = jnp.transpose(o_left.astype(jnp.float32) * weight[:, None, None], (1, 0, 2)).reshape(hidden, members * RANK)
    right_o = o_right.astype(jnp.float32).reshape(members * RANK, width)
    grad_out = jnp.dot(output_left_factor, right_o, precision=lax.Precision.HIGHEST) / noise_scale
    return (grad_query, grad_out, fitness)
```

```python
import functools
import math

import jax
import jax.numpy as jnp
from jax import lax
from jax.experimental import pallas as pl
from jax.experimental.pallas import tpu as pltpu
from jax.sharding import Mesh
from jax.sharding import PartitionSpec as P

D = 3584
HEADS = 28
KV_HEADS = 4
HEAD_DIM = 128
RANK = 4
POP = ("pop_0", "pop_1", "pop_2")
CHIPS = ("pop_0", "pop_1")

noise_scale = 0.5
rope_base = 1000000.0
spread_floor = 0.001

F32 = jnp.float32
BF16 = jnp.bfloat16
NT = (((1,), (1,)), ((), ()))
TN = (((0,), (0,)), ((), ()))


def vmem(n):
    return [pl.BlockSpec(memory_space=pltpu.VMEM)] * n


def iota(shape, dim):
    return lax.broadcasted_iota(jnp.int32, shape, dim)


def shift(x, axis, size, step):
    return lax.ppermute(x, axis, [(i, (i + step) % size) for i in range(size)])


def swap(x):
    return lax.ppermute(x, "pop_2", [(0, 1), (1, 0)])


def tables(position, head_size):
    index = jnp.arange(head_size // 2, dtype=F32)
    freq = jnp.exp(-math.log(rope_base) * 2.0 * index / head_size)
    angle = position[:, None] * freq[None, :]
    c, s = jnp.cos(angle), jnp.sin(angle)
    return jnp.concatenate([c, c], axis=-1), jnp.concatenate([-s, s], axis=-1)


def attention_kernel(heads, first_ref, recv_ref, base_ref, keys_ref, values_ref, cos_ref, sin_ref, mixed_ref, low_ref):
    tok = keys_ref.shape[0]
    rows = 256
    scale = HEAD_DIM ** (-0.5)
    small = recv_ref[:, :, 896:1024].astype(F32).reshape(rows, 128).astype(BF16)
    lane = iota((128, rows), 1)
    pick = (iota((128, rows), 0) == 112 + (lane & 3)).astype(BF16)
    spread = jnp.dot(small, pick, preferred_element_type=F32)
    r, c = iota((rows, rows), 0), iota((rows, rows), 1)
    mine = (r >> 3) == (c >> 3)
    upper = (c & 7) < 4
    left = [
        jnp.where(mine & upper, spread, 0.0).astype(BF16),
        jnp.where(mine & ~upper, spread, 0.0).astype(BF16),
    ]
    right = recv_ref[:, :, 1024:1536].astype(F32).reshape(rows, 512).astype(BF16)
    low = [jnp.dot(a, right, preferred_element_type=F32) for a in left]
    cos = jnp.broadcast_to(cos_ref[...][None], (rows // 8, 8, 128)).reshape(rows, 128)
    sin = jnp.broadcast_to(sin_ref[...][None], (rows // 8, 8, 128)).reshape(rows, 128)
    keys, values = keys_ref[...], values_ref[...]
    seen = (iota((rows, tok), 0) & 7) + first_ref[0] >= iota((rows, tok), 1)
    for h in range(heads):
        part = low[h // 4][:, (h % 4) * 128 : (h % 4 + 1) * 128]
        base = base_ref[:, h * 128 : (h + 1) * 128]
        q = jnp.broadcast_to(base[None], (rows // 8, 8, 128)).reshape(rows, 128) + part
        q = (q * cos + pltpu.roll(q, 64, 1) * sin).astype(BF16)
        s = lax.dot_general(q, keys, NT, preferred_element_type=F32) * scale
        s = jnp.where(seen, s, -1e30)
        e = jnp.exp(s - jnp.max(s, axis=1, keepdims=True))
        p = (e / jnp.sum(e, axis=1, keepdims=True)).astype(BF16)
        mixed_ref[:, h * 128 : (h + 1) * 128] = jnp.dot(p, values, preferred_element_type=F32).astype(BF16)
    o_left = recv_ref[:, :, 1536:2048].astype(F32).reshape(rows, 512).astype(BF16)
    d1 = lax.dot_general(o_left, mixed_ref[:, :512], NT, preferred_element_type=F32)
    d2 = lax.dot_general(o_left[:, :384], mixed_ref[:, 512:896], NT, preferred_element_type=F32)
    d = jnp.where((r & 7) < 4, d1, d2)
    d = jnp.where(mine, d, 0.0).reshape(rows // 8, 8, rows)
    d = jnp.sum(d, axis=0)
    hi = d.astype(BF16).astype(F32)
    low_ref[...] = jnp.stack([hi, d - hi], axis=0)


def project_kernel(where_ref, *refs):
    *pieces, mixed_a, mixed_b, low_a, low_b, out_ref = refs
    shapes = [(0, 4), (1, 4), (2, 4), (3, 4), (4, 4), (5, 4), (6, 4), (7, 2), (7, 2)]
    a, b = mixed_a[...], mixed_b[...]
    done = 0
    for ref, (e, n) in zip(pieces, shapes):
        w = ref[...].astype(F32).reshape(n * 64, 896).astype(BF16)
        first = done if n == 2 else 0
        z = where_ref[4 + e]
        ra = lax.dot_general(w, a, NT, preferred_element_type=F32)
        rb = lax.dot_general(w, b, NT, preferred_element_type=F32)
        for i in range(n):
            j = where_ref[first + i]
            out_ref[j, pl.ds(z * 7, 7), :, 0:256] = ra[i * 64 : i * 64 + 56].reshape(7, 8, 256).astype(BF16)
            out_ref[j, pl.ds(z * 7, 7), :, 256:512] = rb[i * 64 : i * 64 + 56].reshape(7, 8, 256).astype(BF16)
        if n == 2:
            done = 2
    for j in range(4):
        out_ref[j, 56:58, :, 0:256] = low_a[...].astype(BF16)
        out_ref[j, 56:58, :, 256:512] = low_b[...].astype(BF16)


def error_kernel(recv_ref, right_ref, owner_ref, target_ref, err_ref):
    total = recv_ref[0, :56].astype(F32)
    low = recv_ref[0, 56:58].astype(F32)
    for j in range(1, 4):
        total = total + recv_ref[j, :56].astype(F32)
        low = low + recv_ref[j, 56:58].astype(F32)
    total = total.reshape(448, 512)
    low = low[0] + low[1]
    low = low[0:4] + low[4:8]
    low = jnp.concatenate([low, low], axis=0)
    low = jnp.broadcast_to(low[None], (32, 8, 512)).reshape(256, 512)
    r, c = iota((256, 512), 0), iota((256, 512), 1)
    mine = (owner_ref[...] == ((c & 255) >> 3)) & (((r & 7) >> 2) == (c >> 8))
    low = jnp.where(mine, low, 0.0)
    right = right_ref[...]
    for _ in range(3):
        piece = low.astype(BF16)
        total = total + lax.dot_general(right, piece, TN, preferred_element_type=F32)
        low = low - piece.astype(F32)
    tile = (iota((8, 512), 0) == (iota((8, 512), 1) & 7)).astype(BF16)
    target = lax.dot_general(target_ref[...], tile, TN, preferred_element_type=F32)
    diff = total - target
    err_ref[...] = jnp.sum((diff * diff).reshape(56, 8, 512), axis=0)


def call(kernel, out, args, name, smem=0, flops=10**9):
    return pl.pallas_call(
        kernel,
        out_shape=out,
        in_specs=[pl.BlockSpec(memory_space=pltpu.SMEM)] * smem + vmem(len(args) - smem),
        out_specs=jax.tree.map(lambda _: pl.BlockSpec(memory_space=pltpu.VMEM), out),
        name=name,
        cost_estimate=pl.CostEstimate(flops=flops, bytes_accessed=2 * 10**6, transcendentals=0),
        compiler_params=pltpu.CompilerParams(vmem_limit_bytes=40 * 2**20),
    )(*args)


def per_device(
    tokens,
    target,
    w_query,
    w_key,
    w_value,
    w_out,
    query_left_factors,
    query_right_factors,
    o_left,
    o_right,
    member_ids,
):
    tok = tokens.shape[0]
    feats = w_query.shape[1]
    heads = feats // HEAD_DIM
    x, z, c = (lax.axis_index(a) for a in POP)
    y = lax.axis_index("mp")
    k = x * 8 + z
    p = 2 * k + c
    sign = (1 - 2 * (member_ids[0] % 2)).astype(F32)
    half = (noise_scale * sign).astype(BF16)
    twice = (sign / noise_scale).astype(BF16)

    o_r = o_right[0]
    o_cut = lax.dynamic_slice(o_r, (0, feats * y), (RANK, feats)).reshape(RANK, 8, 2, 56)
    o_cut = jnp.moveaxis(o_cut, 2, 0).reshape(2, RANK, 448)
    o_cut = jnp.where(c == 0, o_cut, o_cut[::-1]).reshape(8, 448) * half
    piece = jnp.concatenate([w_out.T, jnp.pad(o_cut, ((0, 0), (0, 448)))], axis=0)
    xs = [piece, shift(piece, "pop_0", 4, 1), shift(piece, "pop_0", 4, 2), shift(piece, "pop_0", 4, 3)]
    block = jnp.stack(xs)
    up1, dn1 = shift(block, "pop_1", 8, 1), shift(block, "pop_1", 8, 7)
    up2, dn2 = shift(up1, "pop_1", 8, 1), shift(dn1, "pop_1", 8, 7)
    up3, dn3 = shift(up2, "pop_1", 8, 1), shift(dn2, "pop_1", 8, 7)
    up4, dn4 = shift(up3[:2], "pop_1", 8, 1), shift(dn3[2:], "pop_1", 8, 7)
    pieces = [block, up1, dn1, up2, dn2, up3, dn3, up4, dn4]
    z_of = jnp.stack([(z - e) % 8 for e in (0, 1, -1, 2, -2, 3, -3, 4)])
    x_of = jnp.stack([(x - d) % 4 for d in range(4)])
    where = jnp.concatenate([x_of, z_of]).astype(jnp.int32)

    rows = lax.dynamic_slice(tokens, (0, 56 * p), (tok, 56))
    share = jnp.dot(rows, w_query, preferred_element_type=F32).astype(BF16).reshape(32, 8, feats)
    low_q = jnp.dot(tokens, query_left_factors[0], preferred_element_type=F32).astype(BF16) * half
    low_q = low_q.reshape(32, 8, RANK)
    cut_q = jnp.moveaxis((query_left_factors[0].T * twice).reshape(RANK, 32, 112), 1, 0)
    cut_o = jnp.moveaxis((o_r * twice).reshape(RANK, 32, 112), 1, 0)
    small = jnp.concatenate([cut_q, cut_o], axis=1)
    small = jnp.concatenate([small, low_q, jnp.zeros((32, 8, 12), BF16)], axis=2)

    def folded(a):
        return jnp.concatenate([a[:, :512], jnp.pad(a[:, 512:], ((0, 0), (0, 128)))], axis=0)

    both = jnp.concatenate([folded(query_right_factors[0]), folded(o_left[0].T)], axis=1)
    sent = jnp.concatenate([share, small, jnp.broadcast_to(both[None], (32, 8, 1024))], axis=2)
    recv = lax.all_to_all(sent, CHIPS, 0, 0, tiled=True)

    cos_all, sin_all = tables(jnp.arange(tok, dtype=F32), HEAD_DIM)
    k32 = jnp.dot(tokens, w_key, preferred_element_type=F32)
    keys = (k32 * cos_all + jnp.roll(k32, 64, axis=1) * sin_all).astype(BF16)
    values = jnp.dot(tokens, w_value, preferred_element_type=F32).astype(BF16)
    cos8, sin8 = tables((k * 8).astype(F32) + jnp.arange(8, dtype=F32), HEAD_DIM)

    half_base = jnp.sum(recv[:, :, :feats].astype(F32), axis=0)
    base = half_base + swap(half_base)
    mixed, low = call(
        functools.partial(attention_kernel, heads),
        (jax.ShapeDtypeStruct((256, feats), BF16), jax.ShapeDtypeStruct((2, 8, 256), F32)),
        ((k * 8).astype(jnp.int32).reshape(1), recv, base, keys, values, cos8, sin8),
        "attention",
        smem=1,
    )
    mixed_b, low_b = swap(mixed), swap(low)

    factors = recv[:, :, 1024:2048]
    factors_b = swap(factors)
    narrow = recv[:, :, 896:1008].reshape(32, 2, RANK, 2, 56)
    narrow = jnp.moveaxis(narrow, 3, 0)
    narrow = jnp.where(c == 0, narrow, narrow[::-1])
    narrow_b = swap(narrow[1])

    def unfolded(a, b, at):
        both = jnp.stack([a[:, :, at : at + 512], b[:, :, at : at + 512]])
        full = jnp.concatenate([both[:, :, :4], both[:, :, 4:, :384]], axis=3)
        return full.reshape(256, feats).astype(F32)

    right_q = unfolded(factors, factors_b, 0)
    right_o = unfolded(factors, factors_b, 512)
    left_all = jnp.stack([narrow[0], narrow_b]).astype(F32)

    out = call(
        project_kernel,
        jax.ShapeDtypeStruct((4, 58, 8, 512), BF16),
        (where, *pieces, mixed, mixed_b, low, low_b),
        "project",
        smem=1,
        flops=2 * 10**9,
    )
    met = lax.all_to_all(out, "mp", 0, 0, tiled=True)

    tails = jnp.concatenate([q[:, 56:64, :448] for q in pieces], axis=0)
    right = jnp.concatenate([tails[:, :4], swap(tails[:, 4:])], axis=1).reshape(256, 448)
    owner = (x_of[None, :] * 8 + z_of[:, None]).reshape(32)
    owner = jnp.broadcast_to(jnp.repeat(owner, 8)[:, None], (256, 512)).astype(jnp.int32)
    goal = lax.dynamic_slice(target, (8 * k, 0), (8, feats)).reshape(8, 8, 2, 56)
    goal = jnp.where(c == 0, goal[:, :, 0], goal[:, :, 1]).reshape(8, 448)
    err = call(
        error_kernel,
        jax.ShapeDtypeStruct((8, 512), F32),
        (met, right, owner, goal),
        "error",
    )
    err = jnp.sum(err, axis=0).reshape(2, 256)
    err = jnp.where(c == 0, err, err[::-1]).reshape(1, 512)
    err = lax.all_to_all(jnp.broadcast_to(err[None], (8, 1, 512)), ("pop_2", "mp"), 0, 0, tiled=True)
    err = jnp.sum(err, axis=0)
    err = lax.all_to_all(jnp.broadcast_to(err[None], (32, 1, 512)), CHIPS, 0, 0, tiled=True)
    errors = jnp.sum(jnp.sum(err, axis=(0, 1)).reshape(2, 32, 8), axis=2)
    everyone = -(errors / (tok * D))
    mean = jnp.sum(everyone) / 64
    spread = jnp.sum((everyone - mean) * (everyone - mean)) / 64
    weight = (everyone - mean) / jnp.sqrt(spread + spread_floor)
    weight = jnp.where(c == 0, weight, weight[::-1])
    fitness = lax.dynamic_slice(everyone, (c, k), (1, 1)).reshape(1)
    left = left_all * weight[:, :, None, None, None]
    left_q = left[:, :, 0].reshape(256, 56)
    left_o = left[:, :, 1].reshape(256, 56)
    dot = functools.partial(lax.dot_general, dimension_numbers=TN, precision=lax.Precision.HIGHEST)
    grad_query = dot(left_q, right_q)
    grad_out = dot(left_o, right_o).T
    return (grad_query, grad_out, fitness)


def solution(mesh):
    torus = Mesh(mesh.devices.reshape(4, 8, 2, mesh.shape["mp"]), ("pop_0", "pop_1", "pop_2", "mp"))
    placed = (
        P(),
        P(None, "mp"),
        P(POP, "mp"),
        P(None, "mp"),
        P(None, "mp"),
        P("mp", POP),
        P(POP, None, None),
        P(POP, None, "mp"),
        P(POP, "mp", None),
        P(POP, None, None),
        P(POP),
    )
    return jax.shard_map(
        per_device,
        mesh=torus,
        in_specs=placed,
        out_specs=(P(POP, "mp"), P("mp", POP), P(POP)),
        check_vma=False,
    )
```

```python
import functools
import math

import jax
import jax.numpy as jnp
from jax import lax
from jax.experimental import pallas as pl
from jax.experimental.pallas import tpu as pltpu
from jax.sharding import Mesh
from jax.sharding import PartitionSpec as P

D = 3584
HEADS = 28
KV_HEADS = 4
HEAD_DIM = 128
RANK = 4
POP = ("pop_0", "pop_1", "pop_2")
CHIPS = ("pop_0", "pop_1")

noise_scale = 0.5
rope_base = 1000000.0
spread_floor = 0.001

F32 = jnp.float32
BF16 = jnp.bfloat16
NT = (((1,), (1,)), ((), ()))
TN = (((0,), (0,)), ((), ()))


def vmem(n):
    return [pl.BlockSpec(memory_space=pltpu.VMEM)] * n


def iota(shape, dim):
    return lax.broadcasted_iota(jnp.int32, shape, dim)


def shift(x, axis, size, step):
    return lax.ppermute(x, axis, [(i, (i + step) % size) for i in range(size)])


def swap(x):
    return lax.ppermute(x, "pop_2", [(0, 1), (1, 0)])


def tables(position, head_size):
    index = jnp.arange(head_size // 2, dtype=F32)
    freq = jnp.exp(-math.log(rope_base) * 2.0 * index / head_size)
    angle = position[:, None] * freq[None, :]
    c, s = jnp.cos(angle), jnp.sin(angle)
    return jnp.concatenate([c, c], axis=-1), jnp.concatenate([-s, s], axis=-1)


def front_kernel(where_ref, tokens_ref, w_ref, left_ref, right_ref, o_ref, out_ref, pad_ref):
    p = where_ref[0]
    start = pl.multiple_of(jnp.minimum((56 * p) // 128 * 128, 3584 - 256), 128)
    at = pl.multiple_of(56 * p - start, 8)
    pad_ref[...] = jnp.zeros_like(pad_ref)
    pad_ref[pl.ds(at, 56), :] = w_ref[...].astype(F32)
    window = tokens_ref[:, pl.ds(start, 256)]
    share = jnp.dot(window, pad_ref[...].astype(BF16), preferred_element_type=F32)
    out_ref[:, :, 0:896] = share.reshape(32, 8, 896).astype(BF16)
    low = lax.dot_general(tokens_ref[...], left_ref[...], NT, preferred_element_type=F32)
    low = low.astype(BF16).astype(F32) * jnp.where(where_ref[1] == 0, 0.5, -0.5)
    out_ref[:, :, 896:1024] = low.reshape(32, 8, 128).astype(BF16)

    def folded(ref):
        a = ref[...].astype(F32)
        b = jnp.concatenate([a[:, 512:896], jnp.zeros((RANK, 128), F32)], axis=1)
        return jnp.broadcast_to(jnp.concatenate([a[:, :512], b], axis=0)[None], (32, 8, 512)).astype(BF16)

    out_ref[:, :, 1024:1536] = folded(right_ref)
    out_ref[:, :, 1536:2048] = folded(o_ref)


def attention_kernel(heads, first_ref, recv_ref, base_ref, other_ref, keys_ref, values_ref, cos_ref, sin_ref, mixed_ref, low_ref):
    tok = keys_ref.shape[0]
    rows = 256
    scale = HEAD_DIM ** (-0.5)
    small = recv_ref[:, :, 896:1024].astype(F32).reshape(rows, 128).astype(BF16)
    lane = iota((128, rows), 1)
    pick = (iota((128, rows), 0) == (lane & 3)).astype(BF16)
    spread = jnp.dot(small, pick, preferred_element_type=F32)
    r, c = iota((rows, rows), 0), iota((rows, rows), 1)
    mine = (r >> 3) == (c >> 3)
    upper = (c & 7) < 4
    left = [
        jnp.where(mine & upper, spread, 0.0).astype(BF16),
        jnp.where(mine & ~upper, spread, 0.0).astype(BF16),
    ]
    right = recv_ref[:, :, 1024:1536].astype(F32).reshape(rows, 512).astype(BF16)
    low = [jnp.dot(a, right, preferred_element_type=F32) for a in left]
    cos = jnp.broadcast_to(cos_ref[...][None], (rows // 8, 8, 128)).reshape(rows, 128)
    sin = jnp.broadcast_to(sin_ref[...][None], (rows // 8, 8, 128)).reshape(rows, 128)
    keys, values = keys_ref[...], values_ref[...]
    seen = (iota((rows, tok), 0) & 7) + first_ref[0] >= iota((rows, tok), 1)
    for h in range(heads):
        part = low[h // 4][:, (h % 4) * 128 : (h % 4 + 1) * 128]
        base = base_ref[:, h * 128 : (h + 1) * 128] + other_ref[:, h * 128 : (h + 1) * 128]
        q = jnp.broadcast_to(base[None], (rows // 8, 8, 128)).reshape(rows, 128) + part
        q = (q * cos + pltpu.roll(q, 64, 1) * sin).astype(BF16)
        s = lax.dot_general(q, keys, NT, preferred_element_type=F32) * scale
        s = jnp.where(seen, s, -1e30)
        e = jnp.exp(s - jnp.max(s, axis=1, keepdims=True))
        p = (e / jnp.sum(e, axis=1, keepdims=True)).astype(BF16)
        mixed_ref[:, h * 128 : (h + 1) * 128] = jnp.dot(p, values, preferred_element_type=F32).astype(BF16)
    o_left = recv_ref[:, :, 1536:2048].astype(F32).reshape(rows, 512).astype(BF16)
    d1 = lax.dot_general(o_left, mixed_ref[:, :512], NT, preferred_element_type=F32)
    d2 = lax.dot_general(o_left[:, :384], mixed_ref[:, 512:896], NT, preferred_element_type=F32)
    d = jnp.where((r & 7) < 4, d1, d2)
    d = jnp.where(mine, d, 0.0).reshape(rows // 8, 8, rows)
    d = jnp.sum(d, axis=0)
    hi = d.astype(BF16).astype(F32)
    low_ref[...] = jnp.stack([hi, d - hi], axis=0)


def project_kernel(split, where_ref, *refs):
    firsts, seconds, (mixed_ref, low_ref), outs, (hold_ref,) = (
        refs[:8],
        refs[8:12],
        refs[12:14],
        refs[14:18],
        refs[18:],
    )
    mixed = mixed_ref[...]
    last = 56 - split

    def times(w, n, rows):
        w = w.astype(F32).reshape(n * rows, 896).astype(BF16)
        return lax.dot_general(w, mixed, NT, preferred_element_type=F32)

    for e, ref in enumerate(firsts):
        got = times(ref[...], 4, split)
        z = where_ref[4 + e]
        for d in range(4):
            hold_ref[where_ref[d], pl.ds(z * 7, split // 8)] = got[d * split : (d + 1) * split].reshape(split // 8, 8, 256).astype(BF16)
    for d, ref in enumerate(seconds):
        got = times(ref[...], 8, last)
        for e in range(8):
            z = where_ref[4 + e]
            hold_ref[where_ref[d], pl.ds(z * 7 + split // 8, last // 8)] = got[e * last : (e + 1) * last].reshape(last // 8, 8, 256).astype(BF16)
    for s, out_ref in enumerate(outs):
        out_ref[0:56] = hold_ref[s]
        out_ref[56:58] = low_ref[...].astype(BF16)


def error_kernel(core_ref, *refs):
    sides, (right_ref, target_ref, err_ref) = (refs[:4], refs[4:8]), refs[8:]
    core = core_ref[0]
    right = right_ref[...]
    tile = (iota((8, 256), 0) == (iota((8, 256), 1) & 7)).astype(BF16)
    target = lax.dot_general(target_ref[...], tile, TN, preferred_element_type=F32)
    r, c = iota((256, 256), 0), iota((256, 256), 1)
    for side in range(2):
        total = low = 0.0
        for ref in sides[side]:
            total = total + ref[0:56].astype(F32)
            low = low + ref[56:58].astype(F32)
        total = total.reshape(448, 256) - target
        low = low[0] + low[1]
        low = low[0:4] + low[4:8]
        low = jnp.concatenate([low, low], axis=0)
        low = jnp.broadcast_to(low[None], (32, 8, 256)).reshape(256, 256)
        at = core if side == 0 else 1 - core
        low = jnp.where(((r >> 3) == (c >> 3)) & (((r & 7) >> 2) == at), low, 0.0)
        for _ in range(3):
            piece = low.astype(BF16)
            total = total + lax.dot_general(right, piece, TN, preferred_element_type=F32)
            low = low - piece.astype(F32)
        err_ref[at] = jnp.sum((total * total).reshape(56, 8, 256), axis=0)


def final_kernel(where_ref, err_ref, left_ref, own_ref, other_ref, query_ref, out_ref, fit_ref):
    core, chip = where_ref[0], where_ref[1]
    err = jnp.sum(err_ref[...], axis=0)
    at = iota((256, 512), 1)
    row = iota((256, 512), 0)
    member = ((at & 255) >> 3) * 2 + (at >> 8)
    err = jnp.where(member == (row >> 2), jnp.broadcast_to(err, (256, 512)), 0.0)
    fit = -(jnp.sum(err, axis=1, keepdims=True) / (256 * D))
    mean = jnp.sum(fit, axis=0, keepdims=True) / 256
    away = fit - mean
    spread = jnp.sum(away * away, axis=0, keepdims=True) / 256
    weight = away / jnp.sqrt(spread + spread_floor)
    me = iota((256, 128), 0) == 4 * (2 * chip + core)
    fit_ref[...] = jnp.sum(jnp.where(me, jnp.broadcast_to(fit, (256, 128)), 0.0), axis=0, keepdims=True)
    left = left_ref[...].astype(F32).reshape(256, 128) * weight
    turned = pltpu.roll(left.reshape(32, 8, 128), 4, 1)
    left = left.reshape(32, 8, 128)
    upper = iota((32, 8, 128), 1) < 4
    low = jnp.where(core == 0, left, turned)
    high = jnp.where(core == 0, turned, left)
    sums = [[0.0, 0.0], [0.0, 0.0]]
    for ref, first, second in ((own_ref, low, high), (other_ref, high, low)):
        for half, l in enumerate((jnp.where(upper, first, 0.0), jnp.where(upper, 0.0, second))):
            l = l.reshape(256, 128)
            parts = []
            for _ in range(3):
                parts.append(l.astype(BF16))
                l = l - parts[-1].astype(F32)
            l = jnp.concatenate(parts, axis=1)
            for which in range(2):
                right = ref[:, :, which * 512 : which * 512 + 512].astype(F32).reshape(256, 512).astype(BF16)
                g = lax.dot_general(l, right, TN, preferred_element_type=F32)
                a = 64 * which
                sums[which][half] += g[a : a + 56] + g[128 + a : 184 + a] + g[256 + a : 312 + a]
    for ref, (a, b) in zip((query_ref, out_ref), sums):
        ref[:, 0:512] = a
        ref[:, 512:896] = b[:, :384]


def call(kernel, out, args, name, smem=0, flops=10**9, scratch=()):
    return pl.pallas_call(
        kernel,
        out_shape=out,
        in_specs=[pl.BlockSpec(memory_space=pltpu.SMEM)] * smem + vmem(len(args) - smem),
        out_specs=jax.tree.map(lambda _: pl.BlockSpec(memory_space=pltpu.VMEM), out),
        scratch_shapes=scratch,
        name=name,
        cost_estimate=pl.CostEstimate(flops=flops, bytes_accessed=2 * 10**6, transcendentals=0),
        compiler_params=pltpu.CompilerParams(vmem_limit_bytes=40 * 2**20),
    )(*args)


def shape(s, t=BF16):
    return jax.ShapeDtypeStruct(s, t)


def after(x, y):
    return lax.optimization_barrier((x, y))[0]


def ints(*values):
    return jnp.stack([jnp.asarray(v, jnp.int32) for v in values])


SPLIT = 16


def per_device(
    tokens,
    target,
    w_query,
    w_key,
    w_value,
    w_out,
    query_left_factors,
    query_right_factors,
    o_left,
    o_right,
    member_ids,
):
    tok = tokens.shape[0]
    feats = w_query.shape[1]
    heads = feats // HEAD_DIM
    x, z, c = (lax.axis_index(a) for a in POP)
    y = lax.axis_index("mp")
    k = x * 8 + z
    p = 2 * k + c
    odd = member_ids[0] % 2
    half = jnp.where(odd == 0, 0.5, -0.5).astype(BF16)
    twice = jnp.where(odd == 0, 2.0, -2.0).astype(BF16)

    w_t = w_out.T
    first, second = w_t[:SPLIT], w_t[SPLIT:]
    along_x = lambda a: [a] + [shift(a, "pop_0", 4, d) for d in (1, 2, 3)]
    by_x = jnp.stack(along_x(first))
    z1, z7 = shift(second, "pop_1", 8, 1), shift(second, "pop_1", 8, 7)
    z2, z6 = shift(second, "pop_1", 8, 2), shift(second, "pop_1", 8, 6)
    z3, z5 = shift(z1, "pop_1", 8, 2), shift(z7, "pop_1", 8, 6)
    z4 = jnp.concatenate([shift(z2[:24], "pop_1", 8, 2), shift(z6[24:], "pop_1", 8, 6)], axis=0)
    by_z = jnp.stack([second, z1, z2, z3, z4, z5, z6, z7])
    seconds = along_x(by_z)
    up1, dn1 = shift(by_x, "pop_1", 8, 1), shift(by_x, "pop_1", 8, 7)
    up2, dn2 = shift(up1, "pop_1", 8, 1), shift(dn1, "pop_1", 8, 7)
    up3, dn3 = shift(up2, "pop_1", 8, 1), shift(dn2, "pop_1", 8, 7)
    up4 = jnp.concatenate([shift(up3[:2], "pop_1", 8, 1), shift(dn3[2:], "pop_1", 8, 7)], axis=0)
    firsts = [by_x, up1, up2, up3, up4, dn3, dn2, dn1]
    where = ints(*[((x - d) % 4 - y) % 4 for d in range(4)], *[(z - e) % 8 for e in range(8)])

    left_t = query_left_factors[0].T
    sent = call(
        front_kernel,
        shape((32, 8, 2048)),
        (
            ints(p, odd),
            tokens,
            w_query,
            jnp.pad(left_t, ((0, 124), (0, 0))),
            query_right_factors[0],
            o_left[0].T,
        ),
        "front",
        smem=1,
        scratch=[pltpu.VMEM((256, feats), F32)],
    )
    recv = lax.all_to_all(sent, CHIPS, 0, 0, tiled=True)

    cos_all, sin_all = tables(jnp.arange(tok, dtype=F32), HEAD_DIM)
    k32 = jnp.dot(tokens, w_key, preferred_element_type=F32)
    keys = (k32 * cos_all + jnp.roll(k32, 64, axis=1) * sin_all).astype(BF16)
    values = jnp.dot(tokens, w_value, preferred_element_type=F32).astype(BF16)
    cos8, sin8 = tables((k * 8).astype(F32) + jnp.arange(8, dtype=F32), HEAD_DIM)

    half_base = jnp.sum(recv[:, :, :feats].astype(F32), axis=0)
    mixed, low = call(
        functools.partial(attention_kernel, heads),
        (shape((256, feats)), shape((2, 8, 256), F32)),
        (ints(k * 8), recv, half_base, swap(half_base), keys, values, cos8, sin8),
        "attention",
        smem=1,
    )

    def project(mixed, low, name):
        return call(
            functools.partial(project_kernel, SPLIT),
            [shape((58, 8, 256))] * 4,
            (where, *firsts, *seconds, mixed, low),
            name,
            smem=1,
            scratch=[pltpu.VMEM((4, 56, 8, 256), BF16)],
        )

    def meet(outs):
        return [outs[0]] + [shift(outs[s], "mp", 4, s) for s in (1, 2, 3)]

    met = meet(project(mixed, low, "project_own"))
    met_b = meet(project(swap(mixed), swap(low), "project_other"))

    o_r = after(o_right[0], mixed)
    o_cut = lax.dynamic_slice(o_r, (0, feats * y), (RANK, feats)).reshape(RANK, 8, 2, 56)
    o_cut = jnp.moveaxis(o_cut, 2, 0).reshape(2, RANK, 448) * half
    o_cut = jnp.broadcast_to(o_cut[None], (32, 2, RANK, 448)).reshape(64, RANK, 448)
    cut_q = jnp.moveaxis((after(left_t, mixed) * twice).reshape(RANK, 64, 56), 1, 0)
    cut_o = jnp.moveaxis((o_r * twice).reshape(RANK, 64, 56), 1, 0)
    gap = jnp.zeros((64, RANK, 8), BF16)
    late = jnp.concatenate([cut_q, gap, cut_o, gap, o_cut, jnp.zeros((64, RANK, 64), BF16)], axis=2)
    late = lax.all_to_all(late, POP, 0, 0, tiled=True)
    factors = after(recv, mixed)[:, :, 1024:2048]
    factors_b = swap(factors)
    lefts = late[:, :, :128].reshape(32, 8, 128)
    right = late[:, :, 128:576].reshape(256, 448)

    goal = lax.dynamic_slice(target, (8 * k, 0), (8, feats)).reshape(8, 8, 2, 56)
    goal = jnp.where(c == 0, goal[:, :, 0], goal[:, :, 1]).reshape(8, 448)
    err = call(
        error_kernel,
        shape((2, 8, 256), F32),
        (ints(c), *met, *met_b, right, goal),
        "error",
        smem=1,
    )
    err = jnp.sum(err, axis=1).reshape(1, 1, 512)
    err = lax.all_to_all(jnp.broadcast_to(err, (16, 1, 512)), ("pop_0", "mp"), 0, 0, tiled=True)
    err = jnp.sum(err, axis=0, keepdims=True)
    err = lax.all_to_all(jnp.broadcast_to(err, (16, 1, 512)), ("pop_1", "pop_2"), 0, 0, tiled=True)
    grad_query, grad_out, fitness = call(
        final_kernel,
        [shape((56, feats), F32), shape((56, feats), F32), shape((1, 128), F32)],
        (ints(c, k), err, lefts, factors, factors_b),
        "final",
        smem=1,
    )
    return (grad_query, grad_out.T, fitness[0, :1])


def solution(mesh):
    torus = Mesh(mesh.devices.reshape(4, 8, 2, mesh.shape["mp"]), ("pop_0", "pop_1", "pop_2", "mp"))
    placed = (
        P(),
        P(None, "mp"),
        P(POP, "mp"),
        P(None, "mp"),
        P(None, "mp"),
        P("mp", POP),
        P(POP, None, None),
        P(POP, None, "mp"),
        P(POP, "mp", None),
        P(POP, None, None),
        P(POP),
    )
    return jax.shard_map(
        per_device,
        mesh=torus,
        in_specs=placed,
        out_specs=(P(POP, "mp"), P("mp", POP), P(POP)),
        check_vma=False,
    )
```

```python
import functools
import math

import jax
import jax.numpy as jnp
from jax import lax
from jax.experimental import pallas as pl
from jax.experimental.pallas import tpu as pltpu
from jax.sharding import Mesh
from jax.sharding import PartitionSpec as P

D = 3584
HEADS = 28
KV_HEADS = 4
HEAD_DIM = 128
RANK = 4
POP = ("pop_0", "pop_1", "pop_2")
CHIPS = ("pop_0", "pop_1")

noise_scale = 0.5
rope_base = 1000000.0
spread_floor = 0.001

F32 = jnp.float32
BF16 = jnp.bfloat16
NT = (((1,), (1,)), ((), ()))
TN = (((0,), (0,)), ((), ()))


def vmem(n):
    return [pl.BlockSpec(memory_space=pltpu.VMEM)] * n


def iota(shape, dim):
    return lax.broadcasted_iota(jnp.int32, shape, dim)


def shift(x, axis, size, step):
    return lax.ppermute(x, axis, [(i, (i + step) % size) for i in range(size)])


def swap(x):
    return lax.ppermute(x, "pop_2", [(0, 1), (1, 0)])


def tables(position, head_size):
    index = jnp.arange(head_size // 2, dtype=F32)
    freq = jnp.exp(-math.log(rope_base) * 2.0 * index / head_size)
    angle = position[:, None] * freq[None, :]
    c, s = jnp.cos(angle), jnp.sin(angle)
    return jnp.concatenate([c, c], axis=-1), jnp.concatenate([-s, s], axis=-1)


def front_kernel(where_ref, tokens_ref, w_ref, left_ref, out_ref, pad_ref):
    p = where_ref[0]
    start = pl.multiple_of(jnp.minimum((56 * p) // 128 * 128, 3584 - 256), 128)
    at = pl.multiple_of(56 * p - start, 8)
    pad_ref[...] = jnp.zeros_like(pad_ref)
    pad_ref[pl.ds(at, 56), :] = w_ref[...].astype(F32)
    window = tokens_ref[:, pl.ds(start, 256)]
    share = jnp.dot(window, pad_ref[...].astype(BF16), preferred_element_type=F32)
    out_ref[:, :, 0:896] = share.reshape(32, 8, 896).astype(BF16)
    left = left_ref[...].astype(F32)
    left = jnp.concatenate([left, jnp.zeros_like(left)], axis=0).astype(BF16)
    low = lax.dot_general(tokens_ref[...], left, NT, preferred_element_type=F32)
    low = low.astype(BF16).astype(F32) * jnp.where(where_ref[1] == 0, 0.5, -0.5)
    out_ref[:, :, 896:1024] = jnp.zeros((32, 8, 128), BF16)
    out_ref[:, :, 896:904] = low.reshape(32, 8, 8).astype(BF16)


def attention_kernel(heads, where_ref, recv_ref, base_ref, other_ref, keys_ref, values_ref, cos_ref, sin_ref, *refs):
    *firsts, mixed_ref, low_ref, factor_ref = refs
    tok = keys_ref.shape[0]
    rows = 256
    scale = HEAD_DIM ** (-0.5)
    for e, ref in enumerate(firsts):
        for d in range(4):
            factor_ref[where_ref[12 + d] * 8 + where_ref[4 + e]] = ref[d, SPLIT : SPLIT + 8, :]
    factors = factor_ref[...].astype(F32).reshape(rows, 896).astype(BF16)
    small = recv_ref[:, :, 896:1024].astype(F32).reshape(rows, 128).astype(BF16)
    lane = iota((128, rows), 1)
    pick = (iota((128, rows), 0) == (lane & 3)).astype(BF16)
    spread = jnp.dot(small, pick, preferred_element_type=F32)
    r, c = iota((rows, rows), 0), iota((rows, rows), 1)
    mine = (r >> 3) == (c >> 3)
    left = jnp.where(mine & ((c & 7) < 4), spread, 0.0).astype(BF16)
    low = jnp.dot(left, factors, preferred_element_type=F32)
    cos = jnp.broadcast_to(cos_ref[...][None], (rows // 8, 8, 128)).reshape(rows, 128)
    sin = jnp.broadcast_to(sin_ref[...][None], (rows // 8, 8, 128)).reshape(rows, 128)
    keys, values = keys_ref[...], values_ref[...]
    seen = (iota((rows, tok), 0) & 7) + where_ref[16] >= iota((rows, tok), 1)
    for h in range(heads):
        at = slice(h * 128, (h + 1) * 128)
        base = base_ref[:, at] + other_ref[:, at]
        q = jnp.broadcast_to(base[None], (rows // 8, 8, 128)).reshape(rows, 128) + low[:, at]
        q = (q * cos + pltpu.roll(q, 64, 1) * sin).astype(BF16)
        s = lax.dot_general(q, keys, NT, preferred_element_type=F32) * scale
        s = jnp.where(seen, s, -1e30)
        e = jnp.exp(s - jnp.max(s, axis=1, keepdims=True))
        p = (e / jnp.sum(e, axis=1, keepdims=True)).astype(BF16)
        mixed_ref[:, at] = jnp.dot(p, values, preferred_element_type=F32).astype(BF16)
    d = lax.dot_general(factors, mixed_ref[...], NT, preferred_element_type=F32)
    d = jnp.where(mine & ((r & 7) >= 4), d, 0.0).reshape(rows // 8, 8, rows)
    d = jnp.sum(d, axis=0)
    hi = d.astype(BF16).astype(F32)
    low_ref[...] = jnp.stack([hi, d - hi], axis=0)


def arrange_kernel(where_ref, *refs):
    firsts, seconds, out_ref = refs[:8], refs[8:16], refs[16]
    for e, ref in enumerate(firsts):
        for d in range(4):
            out_ref[where_ref[d], where_ref[4 + e], 0:SPLIT, :] = ref[d, 0:SPLIT, :]
    for i, ref in enumerate(seconds):
        d, group = i % 4, i // 4
        for n in range(4):
            out_ref[where_ref[d], where_ref[4 + GROUPS[group][n]], SPLIT:56, :] = ref[n]


def project_kernel(w_ref, mixed_ref, low_ref, *outs):
    mixed = mixed_ref[...]
    for s, out_ref in enumerate(outs):
        w = w_ref[s].astype(F32).reshape(448, 896).astype(BF16)
        got = lax.dot_general(w, mixed, NT, preferred_element_type=F32)
        out_ref[0:56] = got.reshape(56, 8, 256).astype(BF16)
        out_ref[56:58] = low_ref[...].astype(BF16)


def error_kernel(core_ref, *refs):
    sides, (right_ref, target_ref, err_ref) = (refs[:4], refs[4:8]), refs[8:]
    core = core_ref[0]
    right = right_ref[...]
    tile = (iota((8, 256), 0) == (iota((8, 256), 1) & 7)).astype(BF16)
    target = lax.dot_general(target_ref[...], tile, TN, preferred_element_type=F32)
    r, c = iota((256, 256), 0), iota((256, 256), 1)
    for side in range(2):
        total = low = 0.0
        for ref in sides[side]:
            total = total + ref[0:56].astype(F32)
            low = low + ref[56:58].astype(F32)
        total = total.reshape(448, 256) - target
        low = low[0] + low[1]
        low = low[0:4] + low[4:8]
        low = jnp.concatenate([low, low], axis=0)
        low = jnp.broadcast_to(low[None], (32, 8, 256)).reshape(256, 256)
        at = core if side == 0 else 1 - core
        low = jnp.where(((r >> 3) == (c >> 3)) & (((r & 7) >> 2) == at), low, 0.0)
        for _ in range(3):
            piece = low.astype(BF16)
            total = total + lax.dot_general(right, piece, TN, preferred_element_type=F32)
            low = low - piece.astype(F32)
        err_ref[at] = jnp.sum((total * total).reshape(56, 8, 256), axis=0)


def final_kernel(where_ref, err_ref, left_ref, own_ref, other_ref, query_ref, out_ref, fit_ref):
    core, chip = where_ref[0], where_ref[1]
    err = jnp.sum(err_ref[...], axis=0)
    at = iota((256, 512), 1)
    row = iota((256, 512), 0)
    member = ((at & 255) >> 3) * 2 + (at >> 8)
    err = jnp.where(member == (row >> 2), jnp.broadcast_to(err, (256, 512)), 0.0)
    fit = -(jnp.sum(err, axis=1, keepdims=True) / (256 * D))
    mean = jnp.sum(fit, axis=0, keepdims=True) / 256
    away = fit - mean
    spread = jnp.sum(away * away, axis=0, keepdims=True) / 256
    weight = away / jnp.sqrt(spread + spread_floor)
    me = iota((256, 128), 0) == 4 * (2 * chip + core)
    fit_ref[...] = jnp.sum(jnp.where(me, jnp.broadcast_to(fit, (256, 128)), 0.0), axis=0, keepdims=True)
    left = left_ref[...].astype(F32).reshape(256, 128) * weight
    left = left.reshape(32, 8, 128)
    turned = pltpu.roll(left, 4, 1)
    low = jnp.where(core == 0, left, turned)
    high = jnp.where(core == 0, turned, left)
    upper, narrow = iota((32, 8, 128), 1) < 4, iota((32, 8, 128), 2) < 64
    total = 0.0
    for ref, a, b in ((own_ref, low, high), (other_ref, high, low)):
        l = jnp.where(narrow, jnp.where(upper, a, 0.0), jnp.where(upper, 0.0, b)).reshape(256, 128)
        parts = []
        for _ in range(3):
            parts.append(l.astype(BF16))
            l = l - parts[-1].astype(F32)
        right = ref[...].astype(F32).reshape(256, 896).astype(BF16)
        g = lax.dot_general(jnp.concatenate(parts, axis=1), right, TN, preferred_element_type=F32)
        total = total + g[0:128] + g[128:256] + g[256:384]
    query_ref[...] = total[0:56]
    out_ref[...] = total[64:120]


def call(kernel, out, args, name, smem=0, flops=10**9, scratch=(), space=pltpu.VMEM):
    spec = pl.BlockSpec(memory_space=space) if space else pl.BlockSpec()
    return pl.pallas_call(
        kernel,
        out_shape=out,
        in_specs=[pl.BlockSpec(memory_space=pltpu.SMEM)] * smem + [spec] * (len(args) - smem),
        out_specs=jax.tree.map(lambda _: spec, out),
        scratch_shapes=scratch,
        name=name,
        cost_estimate=pl.CostEstimate(flops=flops, bytes_accessed=2 * 10**6, transcendentals=0),
        compiler_params=pltpu.CompilerParams(vmem_limit_bytes=16 * 2**20),
    )(*args)


def shape(s, t=BF16):
    return jax.ShapeDtypeStruct(s, t)


def after(x, y):
    return lax.optimization_barrier((x, y))[0]


def ints(*values):
    return jnp.stack([jnp.asarray(v, jnp.int32) for v in values])


SPLIT = 16
GROUPS = ((0, 1, 7, 2), (6, 3, 5, 4))


def per_device(
    tokens,
    target,
    w_query,
    w_key,
    w_value,
    w_out,
    query_left_factors,
    query_right_factors,
    o_left,
    o_right,
    member_ids,
):
    tok = tokens.shape[0]
    feats = w_query.shape[1]
    heads = feats // HEAD_DIM
    x, z, c = (lax.axis_index(a) for a in POP)
    y = lax.axis_index("mp")
    k = x * 8 + z
    p = 2 * k + c
    odd = member_ids[0] % 2
    half = jnp.where(odd == 0, 0.5, -0.5).astype(BF16)
    twice = jnp.where(odd == 0, 2.0, -2.0).astype(BF16)

    w_t = w_out.T
    second = w_t[SPLIT:]
    first = jnp.concatenate([w_t[:SPLIT], query_right_factors[0], o_left[0].T], axis=0)
    along_x = lambda a: [a] + [shift(a, "pop_0", 4, d) for d in (1, 2, 3)]
    by_x = jnp.stack(along_x(first))
    by_z = [second] + [shift(second, "pop_1", 8, e) for e in range(1, 8)]
    seconds = []
    for group in GROUPS:
        seconds += along_x(jnp.stack([by_z[e] for e in group]))
    up1, dn1 = shift(by_x, "pop_1", 8, 1), shift(by_x, "pop_1", 8, 7)
    up2, dn2 = shift(up1, "pop_1", 8, 1), shift(dn1, "pop_1", 8, 7)
    up3, dn3 = shift(up2, "pop_1", 8, 1), shift(dn2, "pop_1", 8, 7)
    up4 = jnp.concatenate([shift(up3[:2], "pop_1", 8, 1), shift(dn3[2:], "pop_1", 8, 7)], axis=0)
    firsts = [by_x, up1, up2, up3, up4, dn3, dn2, dn1]
    xs = [(x - d) % 4 for d in range(4)]
    where = ints(*[(a - y) % 4 for a in xs], *[(z - e) % 8 for e in range(8)], *xs, k * 8)

    left_t = query_left_factors[0].T
    sent = call(
        front_kernel,
        shape((32, 8, 1024)),
        (ints(p, odd), tokens, w_query, left_t),
        "front",
        smem=1,
        scratch=[pltpu.VMEM((256, feats), F32)],
        space=None,
    )
    recv = lax.all_to_all(sent, CHIPS, 0, 0, tiled=True)

    cos_all, sin_all = tables(jnp.arange(tok, dtype=F32), HEAD_DIM)
    k32 = jnp.dot(tokens, w_key, preferred_element_type=F32)
    keys = (k32 * cos_all + jnp.roll(k32, 64, axis=1) * sin_all).astype(BF16)
    values = jnp.dot(tokens, w_value, preferred_element_type=F32).astype(BF16)
    cos8, sin8 = tables((k * 8).astype(F32) + jnp.arange(8, dtype=F32), HEAD_DIM)

    half_base = jnp.sum(recv[:, :, :feats].astype(F32), axis=0)
    mixed, low, factors = call(
        functools.partial(attention_kernel, heads),
        (shape((256, feats)), shape((2, 8, 256), F32), shape((32, 8, feats))),
        (where, recv, half_base, swap(half_base), keys, values, cos8, sin8, *firsts),
        "attention",
        smem=1,
    )
    arranged = call(
        arrange_kernel,
        shape((4, 8, 56, feats)),
        (where, *firsts, *seconds),
        "arrange",
        smem=1,
    )

    def project(mixed, low):
        return call(project_kernel, [shape((58, 8, 256))] * 4, (arranged, mixed, low), "project")

    def meet(outs):
        return [outs[0]] + [shift(outs[s], "mp", 4, s) for s in (2, 1, 3)]

    met = meet(project(mixed, low))
    met_b = meet(project(swap(mixed), swap(low)))

    o_r = after(o_right[0], mixed)
    o_cut = lax.dynamic_slice(o_r, (0, feats * y), (RANK, feats)).reshape(RANK, 8, 2, 56)
    o_cut = jnp.moveaxis(o_cut, 2, 0).reshape(2, RANK, 448) * half
    o_cut = jnp.broadcast_to(o_cut[None], (32, 2, RANK, 448)).reshape(64, RANK, 448)
    cut_q = jnp.moveaxis((after(left_t, mixed) * twice).reshape(RANK, 64, 56), 1, 0)
    cut_o = jnp.moveaxis((o_r * twice).reshape(RANK, 64, 56), 1, 0)
    gap = jnp.zeros((64, RANK, 8), BF16)
    late = jnp.concatenate([cut_q, gap, cut_o, gap, o_cut, jnp.zeros((64, RANK, 64), BF16)], axis=2)
    late = lax.all_to_all(late, POP, 0, 0, tiled=True)
    factors_b = swap(factors)
    lefts = late[:, :, :128].reshape(32, 8, 128)
    right = late[:, :, 128:576].reshape(256, 448)

    goal = lax.dynamic_slice(target, (8 * k, 0), (8, feats)).reshape(8, 8, 2, 56)
    goal = jnp.where(c == 0, goal[:, :, 0], goal[:, :, 1]).reshape(8, 448)
    err = call(
        error_kernel,
        shape((2, 8, 256), F32),
        (ints(c), *met, *met_b, right, goal),
        "error",
        smem=1,
    )
    err = jnp.sum(err, axis=1).reshape(1, 1, 512)
    err = lax.all_to_all(jnp.broadcast_to(err, (8, 1, 512)), ("pop_2", "mp"), 0, 0, tiled=True)
    err = jnp.sum(err, axis=0, keepdims=True)
    err = lax.all_to_all(jnp.broadcast_to(err, (32, 1, 512)), CHIPS, 0, 0, tiled=True)
    grad_query, grad_out, fitness = call(
        final_kernel,
        [shape((56, feats), F32), shape((56, feats), F32), shape((1, 128), F32)],
        (ints(c, k), err, lefts, factors, factors_b),
        "final",
        smem=1,
    )
    return (grad_query, grad_out.T, fitness[0, :1])


def solution(mesh):
    torus = Mesh(mesh.devices.reshape(4, 8, 2, mesh.shape["mp"]), ("pop_0", "pop_1", "pop_2", "mp"))
    placed = (
        P(),
        P(None, "mp"),
        P(POP, "mp"),
        P(None, "mp"),
        P(None, "mp"),
        P("mp", POP),
        P(POP, None, None),
        P(POP, None, "mp"),
        P(POP, "mp", None),
        P(POP, None, None),
        P(POP),
    )
    return jax.shard_map(
        per_device,
        mesh=torus,
        in_specs=placed,
        out_specs=(P(POP, "mp"), P("mp", POP), P(POP)),
        check_vma=False,
    )
```

```python
import functools
import math

import jax
import jax.numpy as jnp
from jax import lax
from jax.experimental import pallas as pl
from jax.experimental.pallas import tpu as pltpu
from jax.sharding import Mesh
from jax.sharding import PartitionSpec as P

D = 3584
HEADS = 28
KV_HEADS = 4
HEAD_DIM = 128
RANK = 4
POP = ("pop_0", "pop_1", "pop_2")
CHIPS = ("pop_0", "pop_1")

noise_scale = 0.5
rope_base = 1000000.0
spread_floor = 0.001

F32 = jnp.float32
BF16 = jnp.bfloat16
NT = (((1,), (1,)), ((), ()))
TN = (((0,), (0,)), ((), ()))


def vmem(n):
    return [pl.BlockSpec(memory_space=pltpu.VMEM)] * n


def iota(shape, dim):
    return lax.broadcasted_iota(jnp.int32, shape, dim)


def shift(x, axis, size, step):
    return lax.ppermute(x, axis, [(i, (i + step) % size) for i in range(size)])


def swap(x):
    return lax.ppermute(x, "pop_2", [(0, 1), (1, 0)])


def tables(position, head_size):
    index = jnp.arange(head_size // 2, dtype=F32)
    freq = jnp.exp(-math.log(rope_base) * 2.0 * index / head_size)
    angle = position[:, None] * freq[None, :]
    c, s = jnp.cos(angle), jnp.sin(angle)
    return jnp.concatenate([c, c], axis=-1), jnp.concatenate([-s, s], axis=-1)


def front_kernel(where_ref, tokens_ref, w_ref, left_ref, right_ref, o_ref, out_ref, pad_ref):
    p = where_ref[0]
    start = pl.multiple_of(jnp.minimum((56 * p) // 128 * 128, 3584 - 256), 128)
    at = pl.multiple_of(56 * p - start, 8)
    pad_ref[...] = jnp.zeros_like(pad_ref)
    pad_ref[pl.ds(at, 56), :] = w_ref[...].astype(F32)
    window = tokens_ref[:, pl.ds(start, 256)]
    share = jnp.dot(window, pad_ref[...].astype(BF16), preferred_element_type=F32)
    out_ref[:, :, 0:896] = share.reshape(32, 8, 896).astype(BF16)
    left = left_ref[...].astype(F32)
    left = jnp.concatenate([left, jnp.zeros_like(left)], axis=0).astype(BF16)
    low = lax.dot_general(tokens_ref[...], left, NT, preferred_element_type=F32)
    low = low.astype(BF16).astype(F32) * jnp.where(where_ref[1] == 0, 0.5, -0.5)
    out_ref[:, :, 896:1024] = jnp.zeros((32, 8, 128), BF16)
    out_ref[:, :, 896:904] = low.reshape(32, 8, 8).astype(BF16)
    both = jnp.concatenate([right_ref[...].astype(F32), o_ref[...].astype(F32)], axis=0)
    out_ref[:, :, 1024:1920] = jnp.broadcast_to(both[None], (32, 8, 896)).astype(BF16)


def attention_kernel(heads, where_ref, recv_ref, base_ref, other_ref, keys_ref, values_ref, cos_ref, sin_ref, mixed_ref):
    tok = keys_ref.shape[0]
    rows = 256
    scale = HEAD_DIM ** (-0.5)
    factors = recv_ref[:, :, 1024:1920].astype(F32).reshape(rows, 896).astype(BF16)
    small = recv_ref[:, :, 896:1024].astype(F32).reshape(rows, 128).astype(BF16)
    lane = iota((128, rows), 1)
    pick = (iota((128, rows), 0) == (lane & 3)).astype(BF16)
    spread = jnp.dot(small, pick, preferred_element_type=F32)
    r, c = iota((rows, rows), 0), iota((rows, rows), 1)
    mine = (r >> 3) == (c >> 3)
    left = jnp.where(mine & ((c & 7) < 4), spread, 0.0).astype(BF16)
    low = jnp.dot(left, factors, preferred_element_type=F32)
    cos = jnp.broadcast_to(cos_ref[...][None], (rows // 8, 8, 128)).reshape(rows, 128)
    sin = jnp.broadcast_to(sin_ref[...][None], (rows // 8, 8, 128)).reshape(rows, 128)
    keys, values = keys_ref[...], values_ref[...]
    seen = (iota((rows, tok), 0) & 7) + where_ref[0] >= iota((rows, tok), 1)
    for h in range(heads):
        at = slice(h * 128, (h + 1) * 128)
        base = base_ref[:, at] + other_ref[:, at]
        q = jnp.broadcast_to(base[None], (rows // 8, 8, 128)).reshape(rows, 128) + low[:, at]
        q = (q * cos + pltpu.roll(q, 64, 1) * sin).astype(BF16)
        s = lax.dot_general(q, keys, NT, preferred_element_type=F32) * scale
        s = jnp.where(seen, s, -1e30)
        e = jnp.exp(s - jnp.max(s, axis=1, keepdims=True))
        p = (e / jnp.sum(e, axis=1, keepdims=True)).astype(BF16)
        mixed_ref[0:256, at] = jnp.dot(p, values, preferred_element_type=F32).astype(BF16)
    d = lax.dot_general(factors, mixed_ref[0:256, :], NT, preferred_element_type=F32)
    d = jnp.where(mine & ((r & 7) >= 4), d, 0.0).reshape(rows // 8, 8, rows)
    d = jnp.sum(d, axis=0)
    hi = d.astype(BF16).astype(F32)
    mixed_ref[256:272, :] = jnp.zeros((16, 896), BF16)
    mixed_ref[256:272, 0:256] = jnp.concatenate([hi, d - hi], axis=0).astype(BF16)


def project_kernel(high, where_ref, *refs):
    pieces, (own_ref, other_ref), out_refs = refs[:5], refs[5:7], refs[7:11]
    w_ref, mixed_ref, hold_ref, sems = refs[11:]
    copies = []
    for d, piece in enumerate(pieces):
        place = w_ref.at[where_ref[1 + min(d, 3)]]
        if d >= 3:
            place = place.at[pl.ds(4 * (d - 3), 4)]
        copies.append(pltpu.make_async_copy(piece, place, sems.at[d]))
    copies.append(pltpu.make_async_copy(own_ref, mixed_ref.at[0], sems.at[5]))
    copies.append(pltpu.make_async_copy(other_ref, mixed_ref.at[1], sems.at[6]))
    for copy in copies:
        copy.start()
    for copy in copies:
        copy.wait()
    groups = high
    sides = [pl.ds(pl.multiple_of(256 * a, 128), 256) for a in (where_ref[0], 1 - where_ref[0])]
    outs = []
    for j in range(4):
        w = w_ref[j].astype(F32).reshape(8 * high, 896).astype(BF16)
        for i, at in enumerate(sides):
            got = lax.dot_general(w, mixed_ref[i, 0:256, :], NT, preferred_element_type=F32)
            hold_ref[j, 0:groups, :, at] = got.reshape(groups, 8, 256).astype(BF16)
            low = mixed_ref[i, 256:272, 0:256].astype(F32).reshape(2, 8, 256)
            hold_ref[j, groups : groups + 2, :, at] = low.astype(BF16)
        outs.append(pltpu.make_async_copy(hold_ref.at[j], out_refs[j], sems.at[7 + j]))
        outs[-1].start()
    for copy in outs:
        copy.wait()


def error_kernel(*refs):
    recv_refs, (right_ref, target_ref, so_far_ref, err_ref) = refs[:4], refs[4:]
    groups = recv_refs[0].shape[0] - 2
    feats = groups * 8
    total = low = 0.0
    for ref in recv_refs:
        total = total + ref[0:groups].astype(F32)
        low = low + ref[groups : groups + 2].astype(F32)
    tile = (iota((8, 512), 0) == (iota((8, 512), 1) & 7)).astype(BF16)
    target = lax.dot_general(target_ref[...], tile, TN, preferred_element_type=F32)
    total = total.reshape(feats, 512) - target
    low = low[0] + low[1]
    low = pltpu.roll(low, 4, 0) + low
    low = jnp.broadcast_to(low[None], (32, 8, 512)).reshape(256, 512)
    r, c = iota((256, 512), 0), iota((256, 512), 1)
    mine = ((r >> 3) == ((c & 255) >> 3)) & (((r & 7) >> 2) == (c >> 8))
    low = jnp.where(mine, low, 0.0)
    right = right_ref[...]
    for _ in range(3):
        piece = low.astype(BF16)
        total = total + lax.dot_general(right, piece, TN, preferred_element_type=F32)
        low = low - piece.astype(F32)
    err = jnp.sum((total * total).reshape(groups, 8, 512), axis=0)
    err = jnp.sum(err, axis=0, keepdims=True) + so_far_ref[0]
    err_ref[...] = jnp.broadcast_to(err[None], (8, 1, 512))


def final_kernel(where_ref, err_ref, left_ref, own_ref, other_ref, query_ref, out_ref, fit_ref):
    core, chip = where_ref[0], where_ref[1]
    err = jnp.sum(err_ref[...], axis=0)
    at = iota((256, 512), 1)
    row = iota((256, 512), 0)
    member = ((at & 255) >> 3) * 2 + (at >> 8)
    err = jnp.where(member == (row >> 2), jnp.broadcast_to(err, (256, 512)), 0.0)
    fit = -(jnp.sum(err, axis=1, keepdims=True) / (256 * D))
    mean = jnp.sum(fit, axis=0, keepdims=True) / 256
    away = fit - mean
    spread = jnp.sum(away * away, axis=0, keepdims=True) / 256
    weight = away / jnp.sqrt(spread + spread_floor)
    me = iota((256, 128), 0) == 4 * (2 * chip + core)
    fit_ref[...] = jnp.sum(jnp.where(me, jnp.broadcast_to(fit, (256, 128)), 0.0), axis=0, keepdims=True)
    left = left_ref[...].astype(F32).reshape(256, 128) * weight
    left = left.reshape(32, 8, 128)
    turned = pltpu.roll(left, 4, 1)
    low = jnp.where(core == 0, left, turned)
    high = jnp.where(core == 0, turned, left)
    upper, narrow = iota((32, 8, 128), 1) < 4, iota((32, 8, 128), 2) < 64
    total = 0.0
    for ref, a, b in ((own_ref, low, high), (other_ref, high, low)):
        l = jnp.where(narrow, jnp.where(upper, a, 0.0), jnp.where(upper, 0.0, b)).reshape(256, 128)
        parts = []
        for _ in range(3):
            parts.append(l.astype(BF16))
            l = l - parts[-1].astype(F32)
        right = ref[...].astype(F32).reshape(256, 896).astype(BF16)
        g = lax.dot_general(jnp.concatenate(parts, axis=1), right, TN, preferred_element_type=F32)
        total = total + g[0:128] + g[128:256] + g[256:384]
    query_ref[...] = total[0:56]
    out_ref[...] = total[64:120]


def loaded(kernel, smem, n_in, n_out):
    def body(*refs):
        scalars, refs = refs[:smem], refs[smem:]
        ins, outs, refs = refs[:n_in], refs[n_in : n_in + n_out], refs[n_in + n_out :]
        held, results, refs = refs[:n_in], refs[n_in : n_in + n_out], refs[n_in + n_out :]
        *rest, sems = refs
        copies = [pltpu.make_async_copy(a, b, sems.at[i]) for i, (a, b) in enumerate(zip(ins, held))]
        for copy in copies:
            copy.start()
        for copy in copies:
            copy.wait()
        kernel(*scalars, *held, *results, *rest)
        copies = [pltpu.make_async_copy(b, a, sems.at[n_in + i]) for i, (a, b) in enumerate(zip(outs, results))]
        for copy in copies:
            copy.start()
        for copy in copies:
            copy.wait()

    return body


def call(kernel, out, args, name, smem=0, flops=10**9, scratch=(), load=True):
    outs = out if isinstance(out, (list, tuple)) else [out]
    ins = args[smem:]
    scratch = list(scratch)
    if load:
        kernel = loaded(kernel, smem, len(ins), len(outs))
        scratch = [pltpu.VMEM(a.shape, a.dtype) for a in (*ins, *outs)] + scratch
        scratch.append(pltpu.SemaphoreType.DMA((len(ins) + len(outs),)))
    hbm = pl.BlockSpec(memory_space=pltpu.HBM)
    return pl.pallas_call(
        kernel,
        out_shape=out,
        in_specs=[pl.BlockSpec(memory_space=pltpu.SMEM)] * smem + [hbm] * len(ins),
        out_specs=jax.tree.map(lambda _: hbm, out),
        scratch_shapes=scratch,
        name=name,
        cost_estimate=pl.CostEstimate(flops=flops, bytes_accessed=2 * 10**6, transcendentals=0),
    )(*args)


def shape(s, t=BF16):
    return jax.ShapeDtypeStruct(s, t)


def after(x, y):
    return lax.optimization_barrier((x, y))[0]


def ints(*values):
    return jnp.stack([jnp.asarray(v, jnp.int32) for v in values])


PARTS = ((0, 32), (32, 24))


def per_device(
    tokens,
    target,
    w_query,
    w_key,
    w_value,
    w_out,
    query_left_factors,
    query_right_factors,
    o_left,
    o_right,
    member_ids,
):
    tok = tokens.shape[0]
    feats = w_query.shape[1]
    heads = feats // HEAD_DIM
    x, z, c = (lax.axis_index(a) for a in POP)
    y = lax.axis_index("mp")
    k = x * 8 + z
    p = 2 * k + c
    odd = member_ids[0] % 2
    half = jnp.where(odd == 0, 0.5, -0.5).astype(BF16)
    twice = jnp.where(odd == 0, 2.0, -2.0).astype(BF16)
    left_t = query_left_factors[0].T

    sent = call(
        front_kernel,
        shape((32, 8, 1920)),
        (ints(p, odd), tokens, w_query, left_t, query_right_factors[0], o_left[0].T),
        "front",
        smem=1,
        scratch=[pltpu.VMEM((256, feats), F32)],
    )
    recv = lax.all_to_all(sent, CHIPS, 0, 0, tiled=True)

    w_t, parts, own = w_out.T, [], recv
    for at, high in PARTS:
        part = jnp.broadcast_to(after(w_t, own)[None, at : at + high], (8, high, feats))
        own = lax.all_to_all(part, "pop_1", 0, 0, tiled=True)
        up, down = shift(own, "pop_0", 4, 1), shift(own, "pop_0", 4, 3)
        far = [shift(up[:4], "pop_0", 4, 1), shift(down[4:], "pop_0", 4, 3)]
        parts.append([own, up, down, *far])
    where = ints(c, *[(x + d - y) % 4 for d in (0, -1, 1, 2)])

    cos_all, sin_all = tables(jnp.arange(tok, dtype=F32), HEAD_DIM)
    k32 = jnp.dot(tokens, w_key, preferred_element_type=F32)
    keys = (k32 * cos_all + jnp.roll(k32, 64, axis=1) * sin_all).astype(BF16)
    values = jnp.dot(tokens, w_value, preferred_element_type=F32).astype(BF16)
    cos8, sin8 = tables((k * 8).astype(F32) + jnp.arange(8, dtype=F32), HEAD_DIM)

    half_base = jnp.sum(recv[:, :, :feats].astype(F32), axis=0)
    mixed = call(
        functools.partial(attention_kernel, heads),
        shape((272, feats)),
        (ints(k * 8), recv, half_base, swap(half_base), keys, values, cos8, sin8),
        "attention",
        smem=1,
    )
    mixed_b = swap(mixed)

    def in_parts(a):
        return [a[..., at : at + high].reshape(*a.shape[:-2], 8 * high) for at, high in PARTS]

    o_r = after(o_right[0], mixed)
    o_cut = lax.dynamic_slice(o_r, (0, feats * y), (RANK, feats)).reshape(RANK, 8, 2, 56)
    o_cut = jnp.concatenate(in_parts(jnp.moveaxis(o_cut, 2, 0)), axis=-1) * half
    o_cut = jnp.broadcast_to(o_cut[None], (32, 2, RANK, 448)).reshape(64, RANK, 448)
    cut_q = jnp.moveaxis((after(left_t, mixed) * twice).reshape(RANK, 64, 56), 1, 0)
    cut_o = jnp.moveaxis((o_r * twice).reshape(RANK, 64, 56), 1, 0)
    gap = jnp.zeros((64, RANK, 8), BF16)
    late = jnp.concatenate([cut_q, gap, cut_o, gap, o_cut, jnp.zeros((64, RANK, 64), BF16)], axis=2)
    late = lax.all_to_all(late, POP, 0, 0, tiled=True)
    factors = after(recv, mixed)[:, :, 1024:1920]
    factors_b = swap(factors)
    lefts = late[:, :, :128].reshape(32, 8, 128)
    goal = lax.dynamic_slice(target, (8 * k, 0), (8, feats)).reshape(8, 8, 2, 56)
    goals = in_parts(jnp.where(c == 0, goal[:, :, 0], goal[:, :, 1]))

    err = jnp.zeros((8, 1, 512), F32)
    start = 128
    for (_, high), pieces, goal in zip(PARTS, parts, goals):
        out = call(
            functools.partial(project_kernel, high),
            [shape((high + 2, 8, 512))] * 4,
            (where, *pieces, mixed, mixed_b),
            "project",
            smem=1,
            scratch=[
                pltpu.VMEM((4, 8, high, feats), BF16),
                pltpu.VMEM((2, 272, feats), BF16),
                pltpu.VMEM((4, high + 2, 8, 512), BF16),
                pltpu.SemaphoreType.DMA((11,)),
            ],
            load=False,
        )
        met = [out[0]] + [shift(out[s], "mp", 4, s) for s in (2, 1, 3)]
        right = late[:, :, start : start + 8 * high].reshape(256, 8 * high)
        start += 8 * high
        err = call(error_kernel, shape((8, 1, 512), F32), (*met, right, goal, err), "error")

    err = lax.all_to_all(err, ("pop_2", "mp"), 0, 0, tiled=True)
    err = jnp.sum(err, axis=0, keepdims=True)
    err = lax.all_to_all(jnp.broadcast_to(err, (32, 1, 512)), CHIPS, 0, 0, tiled=True)
    grad_query, grad_out, fitness = call(
        final_kernel,
        [shape((56, feats), F32), shape((56, feats), F32), shape((1, 128), F32)],
        (ints(c, k), err, lefts, factors, factors_b),
        "final",
        smem=1,
    )
    return (grad_query, grad_out.T, fitness[0, :1])


def solution(mesh):
    torus = Mesh(mesh.devices.reshape(4, 8, 2, mesh.shape["mp"]), ("pop_0", "pop_1", "pop_2", "mp"))
    placed = (
        P(),
        P(None, "mp"),
        P(POP, "mp"),
        P(None, "mp"),
        P(None, "mp"),
        P("mp", POP),
        P(POP, None, None),
        P(POP, None, "mp"),
        P(POP, "mp", None),
        P(POP, None, None),
        P(POP),
    )
    return jax.shard_map(
        per_device,
        mesh=torus,
        in_specs=placed,
        out_specs=(P(POP, "mp"), P("mp", POP), P(POP)),
        check_vma=False,
    )
```

```python
import functools
import math

import jax
import jax.numpy as jnp
from jax import lax
from jax.experimental import pallas as pl
from jax.experimental.pallas import tpu as pltpu
from jax.sharding import Mesh
from jax.sharding import PartitionSpec as P

D = 3584
HEAD_DIM = 128
RANK = 4
POP = ("pop_0", "pop_1", "pop_2")
CHIPS = ("pop_0", "pop_1")

rope_base = 1000000.0
spread_floor = 0.001

F32 = jnp.float32
BF16 = jnp.bfloat16
NT = (((1,), (1,)), ((), ()))
TN = (((0,), (0,)), ((), ()))


def iota(shape, dim):
    return lax.broadcasted_iota(jnp.int32, shape, dim)


def shift(x, axis, size, step):
    return lax.ppermute(x, axis, [(i, (i + step) % size) for i in range(size)])


def swap(x):
    return lax.ppermute(x, "pop_2", [(0, 1), (1, 0)])


def tables(position, head_size):
    index = jnp.arange(head_size // 2, dtype=F32)
    freq = jnp.exp(-math.log(rope_base) * 2.0 * index / head_size)
    angle = position[:, None] * freq[None, :]
    c, s = jnp.cos(angle), jnp.sin(angle)
    return jnp.concatenate([c, c], axis=-1), jnp.concatenate([-s, s], axis=-1)


def front_kernel(where_ref, tokens_ref, w_ref, left_ref, right_ref, o_ref, out_ref, pad_ref):
    p = where_ref[0]
    start = pl.multiple_of(jnp.minimum((56 * p) // 128 * 128, 3584 - 256), 128)
    at = pl.multiple_of(56 * p - start, 8)
    pad_ref[...] = jnp.zeros_like(pad_ref)
    pad_ref[pl.ds(at, 56), :] = w_ref[...].astype(F32)
    window = tokens_ref[:, pl.ds(start, 256)]
    share = jnp.dot(window, pad_ref[...].astype(BF16), preferred_element_type=F32)
    out_ref[:, :, 0:896] = share.reshape(32, 8, 896).astype(BF16)
    left = left_ref[...].astype(F32)
    left = jnp.concatenate([left, jnp.zeros_like(left)], axis=0).astype(BF16)
    low = lax.dot_general(tokens_ref[...], left, NT, preferred_element_type=F32)
    low = low.astype(BF16).astype(F32) * jnp.where(where_ref[1] == 0, 0.5, -0.5)
    out_ref[:, :, 896:1024] = jnp.zeros((32, 8, 128), BF16)
    out_ref[:, :, 896:904] = low.reshape(32, 8, 8).astype(BF16)
    both = jnp.concatenate([right_ref[...].astype(F32), o_ref[...].astype(F32)], axis=0)
    out_ref[:, :, 1024:1920] = jnp.broadcast_to(both[None], (32, 8, 896)).astype(BF16)


def attention_kernel(heads, where_ref, recv_ref, base_ref, other_ref, keys_ref, values_ref, cos_ref, sin_ref, mixed_ref):
    tok = keys_ref.shape[0]
    rows = 256
    scale = HEAD_DIM ** (-0.5)
    factors = recv_ref[:, :, 1024:1920].astype(F32).reshape(rows, 896).astype(BF16)
    small = recv_ref[:, :, 896:1024].astype(F32).reshape(rows, 128).astype(BF16)
    lane = iota((128, rows), 1)
    pick = (iota((128, rows), 0) == (lane & 3)).astype(BF16)
    spread = jnp.dot(small, pick, preferred_element_type=F32)
    r, c = iota((rows, rows), 0), iota((rows, rows), 1)
    mine = (r >> 3) == (c >> 3)
    left = jnp.where(mine & ((c & 7) < 4), spread, 0.0).astype(BF16)
    low = jnp.dot(left, factors, preferred_element_type=F32)
    cos = jnp.broadcast_to(cos_ref[...][None], (rows // 8, 8, 128)).reshape(rows, 128)
    sin = jnp.broadcast_to(sin_ref[...][None], (rows // 8, 8, 128)).reshape(rows, 128)
    keys, values = keys_ref[...], values_ref[...]
    seen = (iota((rows, tok), 0) & 7) + where_ref[0] >= iota((rows, tok), 1)
    for h in range(heads):
        at = slice(h * 128, (h + 1) * 128)
        base = base_ref[:, at] + other_ref[:, at]
        q = jnp.broadcast_to(base[None], (rows // 8, 8, 128)).reshape(rows, 128) + low[:, at]
        q = (q * cos + pltpu.roll(q, 64, 1) * sin).astype(BF16)
        s = lax.dot_general(q, keys, NT, preferred_element_type=F32) * scale
        s = jnp.where(seen, s, -1e30)
        e = jnp.exp(s - jnp.max(s, axis=1, keepdims=True))
        p = (e / jnp.sum(e, axis=1, keepdims=True)).astype(BF16)
        mixed_ref[0:256, at] = jnp.dot(p, values, preferred_element_type=F32).astype(BF16)
    d = lax.dot_general(factors, mixed_ref[0:256, :], NT, preferred_element_type=F32)
    d = jnp.where(mine & ((r & 7) >= 4), d, 0.0).reshape(rows // 8, 8, rows)
    d = jnp.sum(d, axis=0)
    hi = d.astype(BF16).astype(F32)
    mixed_ref[256:272, :] = jnp.zeros((16, 896), BF16)
    mixed_ref[256:272, 0:256] = jnp.concatenate([hi, d - hi], axis=0).astype(BF16)


def stack_kernel(*refs):
    for e in range(8):
        for (at, high), out_ref in zip(PARTS, refs[8:]):
            out_ref[e] = refs[e][at : at + high]


def project_kernel(high, where_ref, *refs):
    pieces, (own_ref, other_ref), out_refs = refs[:5], refs[5:7], refs[7:11]
    w_ref, mixed_ref, hold_ref, sems = refs[11:]
    copies = []
    for d in range(4):
        for e in range(8):
            piece = pieces[d].at[e] if d < 3 else pieces[3 + e // 4].at[e % 4]
            place = w_ref.at[where_ref[1 + d], where_ref[5 + e]]
            copies.append(pltpu.make_async_copy(piece, place, sems.at[8 * d + e]))
    copies.append(pltpu.make_async_copy(own_ref, mixed_ref.at[0], sems.at[32]))
    copies.append(pltpu.make_async_copy(other_ref, mixed_ref.at[1], sems.at[33]))
    for copy in copies:
        copy.start()
    for copy in copies:
        copy.wait()
    groups = high
    sides = [pl.ds(pl.multiple_of(256 * a, 128), 256) for a in (where_ref[0], 1 - where_ref[0])]
    outs = []
    for j in range(4):
        w = w_ref[j].astype(F32).reshape(8 * high, 896).astype(BF16)
        for i, at in enumerate(sides):
            got = lax.dot_general(w, mixed_ref[i, 0:256, :], NT, preferred_element_type=F32)
            hold_ref[j, 0:groups, :, at] = got.reshape(groups, 8, 256).astype(BF16)
            low = mixed_ref[i, 256:272, 0:256].astype(F32).reshape(2, 8, 256)
            hold_ref[j, groups : groups + 2, :, at] = low.astype(BF16)
        outs.append(pltpu.make_async_copy(hold_ref.at[j], out_refs[j], sems.at[34 + j]))
        outs[-1].start()
    for copy in outs:
        copy.wait()


def error_kernel(*refs):
    recv_refs, (right_ref, target_ref, so_far_ref, err_ref) = refs[:4], refs[4:]
    groups = recv_refs[0].shape[0] - 2
    feats = groups * 8
    total = low = 0.0
    for ref in recv_refs:
        total = total + ref[0:groups].astype(F32)
        low = low + ref[groups : groups + 2].astype(F32)
    tile = (iota((8, 512), 0) == (iota((8, 512), 1) & 7)).astype(BF16)
    target = lax.dot_general(target_ref[...], tile, TN, preferred_element_type=F32)
    total = total.reshape(feats, 512) - target
    low = low[0] + low[1]
    low = pltpu.roll(low, 4, 0) + low
    low = jnp.broadcast_to(low[None], (32, 8, 512)).reshape(256, 512)
    r, c = iota((256, 512), 0), iota((256, 512), 1)
    mine = ((r >> 3) == ((c & 255) >> 3)) & (((r & 7) >> 2) == (c >> 8))
    low = jnp.where(mine, low, 0.0)
    right = right_ref[...]
    for _ in range(3):
        piece = low.astype(BF16)
        total = total + lax.dot_general(right, piece, TN, preferred_element_type=F32)
        low = low - piece.astype(F32)
    err = jnp.sum((total * total).reshape(groups, 8, 512), axis=0)
    err = jnp.sum(err, axis=0, keepdims=True) + so_far_ref[0]
    err_ref[...] = jnp.broadcast_to(err[None], (8, 1, 512))


def final_kernel(where_ref, err_ref, left_ref, own_ref, other_ref, query_ref, out_ref, fit_ref):
    core, chip = where_ref[0], where_ref[1]
    err = jnp.sum(err_ref[...], axis=0)
    at = iota((256, 512), 1)
    row = iota((256, 512), 0)
    member = ((at & 255) >> 3) * 2 + (at >> 8)
    err = jnp.where(member == (row >> 2), jnp.broadcast_to(err, (256, 512)), 0.0)
    fit = -(jnp.sum(err, axis=1, keepdims=True) / (256 * D))
    mean = jnp.sum(fit, axis=0, keepdims=True) / 256
    away = fit - mean
    spread = jnp.sum(away * away, axis=0, keepdims=True) / 256
    weight = away / jnp.sqrt(spread + spread_floor)
    me = iota((256, 128), 0) == 4 * (2 * chip + core)
    fit_ref[...] = jnp.sum(jnp.where(me, jnp.broadcast_to(fit, (256, 128)), 0.0), axis=0, keepdims=True)
    left = left_ref[...].astype(F32).reshape(256, 128) * weight
    left = left.reshape(32, 8, 128)
    turned = pltpu.roll(left, 4, 1)
    low = jnp.where(core == 0, left, turned)
    high = jnp.where(core == 0, turned, left)
    upper, narrow = iota((32, 8, 128), 1) < 4, iota((32, 8, 128), 2) < 64
    total = 0.0
    for ref, a, b in ((own_ref, low, high), (other_ref, high, low)):
        l = jnp.where(narrow, jnp.where(upper, a, 0.0), jnp.where(upper, 0.0, b)).reshape(256, 128)
        parts = []
        for _ in range(3):
            parts.append(l.astype(BF16))
            l = l - parts[-1].astype(F32)
        right = ref[...].astype(F32).reshape(256, 896).astype(BF16)
        g = lax.dot_general(jnp.concatenate(parts, axis=1), right, TN, preferred_element_type=F32)
        total = total + g[0:128] + g[128:256] + g[256:384]
    query_ref[...] = total[0:56]
    out_ref[...] = total[64:120]


def loaded(kernel, smem, n_in, n_out):
    def body(*refs):
        scalars, refs = refs[:smem], refs[smem:]
        ins, outs, refs = refs[:n_in], refs[n_in : n_in + n_out], refs[n_in + n_out :]
        held, results, refs = refs[:n_in], refs[n_in : n_in + n_out], refs[n_in + n_out :]
        *rest, sems = refs
        copies = [pltpu.make_async_copy(a, b, sems.at[i]) for i, (a, b) in enumerate(zip(ins, held))]
        for copy in copies:
            copy.start()
        for copy in copies:
            copy.wait()
        kernel(*scalars, *held, *results, *rest)
        copies = [pltpu.make_async_copy(b, a, sems.at[n_in + i]) for i, (a, b) in enumerate(zip(outs, results))]
        for copy in copies:
            copy.start()
        for copy in copies:
            copy.wait()

    return body


def call(kernel, out, args, smem=0, flops=10**9, scratch=(), load=True):
    outs = out if isinstance(out, (list, tuple)) else [out]
    ins = args[smem:]
    scratch = list(scratch)
    if load:
        kernel = loaded(kernel, smem, len(ins), len(outs))
        scratch = [pltpu.VMEM(a.shape, a.dtype) for a in (*ins, *outs)] + scratch
        scratch.append(pltpu.SemaphoreType.DMA((len(ins) + len(outs),)))
    hbm = pl.BlockSpec(memory_space=pltpu.HBM)
    return pl.pallas_call(
        kernel,
        out_shape=out,
        in_specs=[pl.BlockSpec(memory_space=pltpu.SMEM)] * smem + [hbm] * len(ins),
        out_specs=jax.tree.map(lambda _: hbm, out),
        scratch_shapes=scratch,
        cost_estimate=pl.CostEstimate(flops=flops, bytes_accessed=2 * 10**6, transcendentals=0),
    )(*args)


def shape(s, t=BF16):
    return jax.ShapeDtypeStruct(s, t)


def after(x, y):
    return lax.optimization_barrier((x, y))[0]


def ints(*values):
    return jnp.stack([jnp.asarray(v, jnp.int32) for v in values])


PARTS = ((0, 32), (32, 24))


def per_device(
    tokens,
    target,
    w_query,
    w_key,
    w_value,
    w_out,
    query_left_factors,
    query_right_factors,
    o_left,
    o_right,
    member_ids,
):
    tok = tokens.shape[0]
    feats = w_query.shape[1]
    heads = feats // HEAD_DIM
    x, z, c = (lax.axis_index(a) for a in POP)
    y = lax.axis_index("mp")
    k = x * 8 + z
    p = 2 * k + c
    odd = member_ids[0] % 2
    half = jnp.where(odd == 0, 0.5, -0.5).astype(BF16)
    twice = jnp.where(odd == 0, 2.0, -2.0).astype(BF16)
    left_t = query_left_factors[0].T

    sent = call(
        front_kernel,
        shape((32, 8, 1920)),
        (ints(p, odd), tokens, w_query, left_t, query_right_factors[0], o_left[0].T),
        smem=1,
        scratch=[pltpu.VMEM((256, feats), F32)],
    )
    recv = lax.all_to_all(sent, CHIPS, 0, 0, tiled=True)

    w_t, parts = after(w_out.T, sent), []
    by_z = [w_t] + [shift(w_t, "pop_1", 8, e) for e in (1, 2, 3, 4, 5, 6, 7)]
    stacked = call(stack_kernel, [shape((8, high, feats)) for _, high in PARTS], by_z)
    for own in stacked:
        up, down = shift(own, "pop_0", 4, 1), shift(own, "pop_0", 4, 3)
        far = [shift(up[:4], "pop_0", 4, 1), shift(down[4:], "pop_0", 4, 3)]
        parts.append([own, up, down, *far])
    where = ints(c, *[(x + d - y) % 4 for d in (0, -1, 1, 2)], *[(z - e) % 8 for e in range(8)])

    cos_all, sin_all = tables(jnp.arange(tok, dtype=F32), HEAD_DIM)
    k32 = jnp.dot(tokens, w_key, preferred_element_type=F32)
    keys = (k32 * cos_all + jnp.roll(k32, 64, axis=1) * sin_all).astype(BF16)
    values = jnp.dot(tokens, w_value, preferred_element_type=F32).astype(BF16)
    cos8, sin8 = tables((k * 8).astype(F32) + jnp.arange(8, dtype=F32), HEAD_DIM)

    half_base = jnp.sum(recv[:, :, :feats].astype(F32), axis=0)
    mixed = call(
        functools.partial(attention_kernel, heads),
        shape((272, feats)),
        (ints(k * 8), recv, half_base, swap(half_base), keys, values, cos8, sin8),
        smem=1,
    )
    mixed_b = swap(mixed)

    outs = [
        call(
            functools.partial(project_kernel, high),
            [shape((high + 2, 8, 512))] * 4,
            (where, *pieces, mixed, mixed_b),
            smem=1,
            scratch=[
                pltpu.VMEM((4, 8, high, feats), BF16),
                pltpu.VMEM((2, 272, feats), BF16),
                pltpu.VMEM((4, high + 2, 8, 512), BF16),
                pltpu.SemaphoreType.DMA((38,)),
            ],
            load=False,
        )
        for (_, high), pieces in zip(PARTS, parts)
    ]
    mets = []
    for out in outs:
        mets.append([out[0]] + [shift(out[s], "mp", 4, s) for s in (2, 1, 3)])

    def in_parts(a):
        return [a[..., at : at + high].reshape(*a.shape[:-2], 8 * high) for at, high in PARTS]

    o_r = after(o_right[0], mixed)
    o_cut = lax.dynamic_slice(o_r, (0, feats * y), (RANK, feats)).reshape(RANK, 8, 2, 56)
    o_cut = jnp.concatenate(in_parts(jnp.moveaxis(o_cut, 2, 0)), axis=-1) * half
    o_cut = jnp.broadcast_to(o_cut[None], (32, 2, RANK, 448)).reshape(64, RANK, 448)
    cut_q = jnp.moveaxis((after(left_t, mixed) * twice).reshape(RANK, 64, 56), 1, 0)
    cut_o = jnp.moveaxis((o_r * twice).reshape(RANK, 64, 56), 1, 0)
    gap = jnp.zeros((64, RANK, 8), BF16)
    late = jnp.concatenate([cut_q, gap, cut_o, gap, o_cut, jnp.zeros((64, RANK, 64), BF16)], axis=2)
    late = lax.all_to_all(late, POP, 0, 0, tiled=True)
    factors = after(recv, outs[0][0])[:, :, 1024:1920]
    factors_b = swap(factors)
    lefts = late[:, :, :128].reshape(32, 8, 128)
    goal = lax.dynamic_slice(target, (8 * k, 0), (8, feats)).reshape(8, 8, 2, 56)
    goals = in_parts(jnp.where(c == 0, goal[:, :, 0], goal[:, :, 1]))

    err = jnp.zeros((8, 1, 512), F32)
    start = 128
    for (_, high), met, goal in zip(PARTS, mets, goals):
        right = late[:, :, start : start + 8 * high].reshape(256, 8 * high)
        start += 8 * high
        err = call(error_kernel, shape((8, 1, 512), F32), (*met, right, goal, err))

    err = lax.all_to_all(err, ("pop_2", "mp"), 0, 0, tiled=True)
    err = jnp.sum(err, axis=0, keepdims=True)
    err = lax.all_to_all(jnp.broadcast_to(err, (32, 1, 512)), CHIPS, 0, 0, tiled=True)
    grad_query, grad_out, fitness = call(
        final_kernel,
        [shape((56, feats), F32), shape((56, feats), F32), shape((1, 128), F32)],
        (ints(c, k), err, lefts, factors, factors_b),
        smem=1,
    )
    return (grad_query, grad_out.T, fitness[0, :1])


def solution(mesh):
    torus = Mesh(mesh.devices.reshape(4, 8, 2, mesh.shape["mp"]), ("pop_0", "pop_1", "pop_2", "mp"))
    placed = (
        P(),
        P(None, "mp"),
        P(POP, "mp"),
        P(None, "mp"),
        P(None, "mp"),
        P("mp", POP),
        P(POP, None, None),
        P(POP, None, "mp"),
        P(POP, "mp", None),
        P(POP, None, None),
        P(POP),
    )
    return jax.shard_map(
        per_device,
        mesh=torus,
        in_specs=placed,
        out_specs=(P(POP, "mp"), P("mp", POP), P(POP)),
        check_vma=False,
    )
```

```python
import functools
import math

import jax
import jax.numpy as jnp
from jax import lax
from jax.experimental import pallas as pl
from jax.experimental.pallas import tpu as pltpu
from jax.sharding import Mesh
from jax.sharding import PartitionSpec as P

D = 3584
HEAD_DIM = 128
RANK = 4
POP = ("pop_0", "pop_1", "pop_2")
CHIPS = ("pop_0", "pop_1")

rope_base = 1000000.0
spread_floor = 0.001

F32 = jnp.float32
BF16 = jnp.bfloat16
NT = (((1,), (1,)), ((), ()))
TN = (((0,), (0,)), ((), ()))


def iota(shape, dim):
    return lax.broadcasted_iota(jnp.int32, shape, dim)


def shift(x, axis, size, step):
    return lax.ppermute(x, axis, [(i, (i + step) % size) for i in range(size)])


def swap(x):
    return lax.ppermute(x, "pop_2", [(0, 1), (1, 0)])


def tables(position, head_size):
    index = jnp.arange(head_size // 2, dtype=F32)
    freq = jnp.exp(-math.log(rope_base) * 2.0 * index / head_size)
    angle = position[:, None] * freq[None, :]
    c, s = jnp.cos(angle), jnp.sin(angle)
    return jnp.concatenate([c, c], axis=-1), jnp.concatenate([-s, s], axis=-1)


def front_kernel(where_ref, tokens_ref, w_ref, left_ref, right_ref, o_ref, out_ref, pad_ref):
    p = where_ref[0]
    start = pl.multiple_of(jnp.minimum((56 * p) // 128 * 128, 3584 - 256), 128)
    at = pl.multiple_of(56 * p - start, 8)
    pad_ref[...] = jnp.zeros_like(pad_ref)
    pad_ref[pl.ds(at, 56), :] = w_ref[...].astype(F32)
    window = tokens_ref[:, pl.ds(start, 256)]
    share = jnp.dot(window, pad_ref[...].astype(BF16), preferred_element_type=F32)
    out_ref[:, :, 0:896] = share.reshape(32, 8, 896).astype(BF16)
    left = left_ref[...].astype(F32)
    left = jnp.concatenate([left, jnp.zeros_like(left)], axis=0).astype(BF16)
    low = lax.dot_general(tokens_ref[...], left, NT, preferred_element_type=F32)
    low = low.astype(BF16).astype(F32) * jnp.where(where_ref[1] == 0, 0.5, -0.5)
    out_ref[:, :, 896:1024] = jnp.zeros((32, 8, 128), BF16)
    out_ref[:, :, 896:904] = low.reshape(32, 8, 8).astype(BF16)
    both = jnp.concatenate([right_ref[...].astype(F32), o_ref[...].astype(F32)], axis=0)
    out_ref[:, :, 1024:1920] = jnp.broadcast_to(both[None], (32, 8, 896)).astype(BF16)


def attention_kernel(heads, where_ref, recv_ref, base_ref, other_ref, keys_ref, values_ref, cos_ref, sin_ref, mixed_ref):
    tok = keys_ref.shape[0]
    rows = 256
    scale = HEAD_DIM ** (-0.5)
    factors = recv_ref[:, :, 1024:1920].astype(F32).reshape(rows, 896).astype(BF16)
    small = recv_ref[:, :, 896:1024].astype(F32).reshape(rows, 128).astype(BF16)
    lane = iota((128, rows), 1)
    pick = (iota((128, rows), 0) == (lane & 3)).astype(BF16)
    spread = jnp.dot(small, pick, preferred_element_type=F32)
    r, c = iota((rows, rows), 0), iota((rows, rows), 1)
    mine = (r >> 3) == (c >> 3)
    left = jnp.where(mine & ((c & 7) < 4), spread, 0.0).astype(BF16)
    low = jnp.dot(left, factors, preferred_element_type=F32)
    cos = jnp.broadcast_to(cos_ref[...][None], (rows // 8, 8, 128)).reshape(rows, 128)
    sin = jnp.broadcast_to(sin_ref[...][None], (rows // 8, 8, 128)).reshape(rows, 128)
    keys, values = keys_ref[...], values_ref[...]
    seen = (iota((rows, tok), 0) & 7) + where_ref[0] >= iota((rows, tok), 1)
    for h in range(heads):
        at = slice(h * 128, (h + 1) * 128)
        base = base_ref[:, at] + other_ref[:, at]
        q = jnp.broadcast_to(base[None], (rows // 8, 8, 128)).reshape(rows, 128) + low[:, at]
        q = (q * cos + pltpu.roll(q, 64, 1) * sin).astype(BF16)
        s = lax.dot_general(q, keys, NT, preferred_element_type=F32) * scale
        s = jnp.where(seen, s, -1e30)
        e = jnp.exp(s - jnp.max(s, axis=1, keepdims=True))
        p = (e / jnp.sum(e, axis=1, keepdims=True)).astype(BF16)
        mixed_ref[0:256, at] = jnp.dot(p, values, preferred_element_type=F32).astype(BF16)
    d = lax.dot_general(factors, mixed_ref[0:256, :], NT, preferred_element_type=F32)
    d = jnp.where(mine & ((r & 7) >= 4), d, 0.0).reshape(rows // 8, 8, rows)
    d = jnp.sum(d, axis=0)
    hi = d.astype(BF16).astype(F32)
    mixed_ref[256:272, :] = jnp.zeros((16, 896), BF16)
    mixed_ref[256:272, 0:256] = jnp.concatenate([hi, d - hi], axis=0).astype(BF16)


def stack_kernel(*refs):
    *ins, out_ref = refs
    for e in range(out_ref.shape[0] - 1):
        out_ref[e] = ins[e][...]
    at = 0
    for ref in ins[out_ref.shape[0] - 1 :]:
        out_ref[out_ref.shape[0] - 1, at : at + ref.shape[0]] = ref[...]
        at += ref.shape[0]


def project_kernel(where_ref, *refs):
    pieces, (own_ref, other_ref), out_refs = refs[:5], refs[5:7], refs[7:11]
    w_ref, mixed_ref, hold_ref, sems = refs[11:]
    groups = 7 * w_ref.shape[1]
    copies = []
    for d, piece in enumerate(pieces):
        place = w_ref.at[where_ref[1 + min(d, 3)]]
        if d >= 3:
            place = place.at[pl.ds(pieces[3].shape[0] * (d - 3), piece.shape[0])]
        copies.append(pltpu.make_async_copy(piece, place, sems.at[d]))
    copies.append(pltpu.make_async_copy(own_ref, mixed_ref.at[0], sems.at[32]))
    copies.append(pltpu.make_async_copy(other_ref, mixed_ref.at[1], sems.at[33]))
    for copy in copies:
        copy.start()
    for copy in copies:
        copy.wait()
    sides = [pl.ds(pl.multiple_of(256 * a, 128), 256) for a in (where_ref[0], 1 - where_ref[0])]
    outs = []
    for j in range(4):
        w = w_ref[j].astype(F32).reshape(8 * groups, 896).astype(BF16)
        for i, at in enumerate(sides):
            got = lax.dot_general(w, mixed_ref[i, 0:256, :], NT, preferred_element_type=F32)
            hold_ref[j, 0:groups, :, at] = got.reshape(groups, 8, 256).astype(BF16)
            low = mixed_ref[i, 256:272, 0:256].astype(F32).reshape(2, 8, 256)
            hold_ref[j, groups : groups + 2, :, at] = low.astype(BF16)
        outs.append(pltpu.make_async_copy(hold_ref.at[j], out_refs[j], sems.at[34 + j]))
        outs[-1].start()
    for copy in outs:
        copy.wait()


def error_kernel(*refs):
    recv_refs, (right_ref, target_ref, so_far_ref, err_ref) = refs[:4], refs[4:]
    groups = recv_refs[0].shape[0] - 2
    feats = groups * 8
    total = low = 0.0
    for ref in recv_refs:
        total = total + ref[0:groups].astype(F32)
        low = low + ref[groups : groups + 2].astype(F32)
    tile = (iota((8, 512), 0) == (iota((8, 512), 1) & 7)).astype(BF16)
    target = lax.dot_general(target_ref[...], tile, TN, preferred_element_type=F32)
    total = total.reshape(feats, 512) - target
    low = low[0] + low[1]
    low = pltpu.roll(low, 4, 0) + low
    low = jnp.broadcast_to(low[None], (32, 8, 512)).reshape(256, 512)
    r, c = iota((256, 512), 0), iota((256, 512), 1)
    mine = ((r >> 3) == ((c & 255) >> 3)) & (((r & 7) >> 2) == (c >> 8))
    low = jnp.where(mine, low, 0.0)
    right = right_ref[...]
    for _ in range(3):
        piece = low.astype(BF16)
        total = total + lax.dot_general(right, piece, TN, preferred_element_type=F32)
        low = low - piece.astype(F32)
    err = jnp.sum((total * total).reshape(groups, 8, 512), axis=0)
    err = jnp.sum(err, axis=0, keepdims=True) + so_far_ref[0]
    err_ref[...] = jnp.broadcast_to(err[None], (8, 1, 512))


def final_kernel(where_ref, err_ref, left_ref, own_ref, other_ref, query_ref, out_ref, fit_ref):
    core, chip = where_ref[0], where_ref[1]
    err = jnp.sum(err_ref[...], axis=0)
    at = iota((256, 512), 1)
    row = iota((256, 512), 0)
    member = ((at & 255) >> 3) * 2 + (at >> 8)
    err = jnp.where(member == (row >> 2), jnp.broadcast_to(err, (256, 512)), 0.0)
    fit = -(jnp.sum(err, axis=1, keepdims=True) / (256 * D))
    mean = jnp.sum(fit, axis=0, keepdims=True) / 256
    away = fit - mean
    spread = jnp.sum(away * away, axis=0, keepdims=True) / 256
    weight = away / jnp.sqrt(spread + spread_floor)
    me = iota((256, 128), 0) == 4 * (2 * chip + core)
    fit_ref[...] = jnp.sum(jnp.where(me, jnp.broadcast_to(fit, (256, 128)), 0.0), axis=0, keepdims=True)
    left = left_ref[...].astype(F32).reshape(256, 128) * weight
    left = left.reshape(32, 8, 128)
    turned = pltpu.roll(left, 4, 1)
    low = jnp.where(core == 0, left, turned)
    high = jnp.where(core == 0, turned, left)
    upper, narrow = iota((32, 8, 128), 1) < 4, iota((32, 8, 128), 2) < 64
    total = 0.0
    for ref, a, b in ((own_ref, low, high), (other_ref, high, low)):
        l = jnp.where(narrow, jnp.where(upper, a, 0.0), jnp.where(upper, 0.0, b)).reshape(256, 128)
        parts = []
        for _ in range(3):
            parts.append(l.astype(BF16))
            l = l - parts[-1].astype(F32)
        right = ref[...].astype(F32).reshape(256, 896).astype(BF16)
        g = lax.dot_general(jnp.concatenate(parts, axis=1), right, TN, preferred_element_type=F32)
        total = total + g[0:128] + g[128:256] + g[256:384]
    query_ref[...] = total[0:56]
    out_ref[...] = total[64:120]


def loaded(kernel, smem, n_in, n_out):
    def body(*refs):
        scalars, refs = refs[:smem], refs[smem:]
        ins, outs, refs = refs[:n_in], refs[n_in : n_in + n_out], refs[n_in + n_out :]
        held, results, refs = refs[:n_in], refs[n_in : n_in + n_out], refs[n_in + n_out :]
        *rest, sems = refs
        copies = [pltpu.make_async_copy(a, b, sems.at[i]) for i, (a, b) in enumerate(zip(ins, held))]
        for copy in copies:
            copy.start()
        for copy in copies:
            copy.wait()
        kernel(*scalars, *held, *results, *rest)
        copies = [pltpu.make_async_copy(b, a, sems.at[n_in + i]) for i, (a, b) in enumerate(zip(outs, results))]
        for copy in copies:
            copy.start()
        for copy in copies:
            copy.wait()

    return body


def call(kernel, out, args, smem=0, flops=10**9, scratch=(), load=True):
    outs = out if isinstance(out, (list, tuple)) else [out]
    ins = args[smem:]
    scratch = list(scratch)
    if load:
        kernel = loaded(kernel, smem, len(ins), len(outs))
        scratch = [pltpu.VMEM(a.shape, a.dtype) for a in (*ins, *outs)] + scratch
        scratch.append(pltpu.SemaphoreType.DMA((len(ins) + len(outs),)))
    hbm = pl.BlockSpec(memory_space=pltpu.HBM)
    return pl.pallas_call(
        kernel,
        out_shape=out,
        in_specs=[pl.BlockSpec(memory_space=pltpu.SMEM)] * smem + [hbm] * len(ins),
        out_specs=jax.tree.map(lambda _: hbm, out),
        scratch_shapes=scratch,
        cost_estimate=pl.CostEstimate(flops=flops, bytes_accessed=2 * 10**6, transcendentals=0),
    )(*args)


def shape(s, t=BF16):
    return jax.ShapeDtypeStruct(s, t)


def after(x, y):
    return lax.optimization_barrier((x, y))[0]


def ints(*values):
    return jnp.stack([jnp.asarray(v, jnp.int32) for v in values])


GROUPS = ((0, 1, 7, 2, 6), (3, 5, 4))
VIA_UP = (3, 1)


def per_device(
    tokens,
    target,
    w_query,
    w_key,
    w_value,
    w_out,
    query_left_factors,
    query_right_factors,
    o_left,
    o_right,
    member_ids,
):
    tok = tokens.shape[0]
    feats = w_query.shape[1]
    heads = feats // HEAD_DIM
    x, z, c = (lax.axis_index(a) for a in POP)
    y = lax.axis_index("mp")
    k = x * 8 + z
    p = 2 * k + c
    odd = member_ids[0] % 2
    half = jnp.where(odd == 0, 0.5, -0.5).astype(BF16)
    twice = jnp.where(odd == 0, 2.0, -2.0).astype(BF16)
    left_t = query_left_factors[0].T

    sent = call(
        front_kernel,
        shape((32, 8, 1920)),
        (ints(p, odd), tokens, w_query, left_t, query_right_factors[0], o_left[0].T),
        smem=1,
        scratch=[pltpu.VMEM((256, feats), F32)],
    )
    recv = lax.all_to_all(sent, CHIPS, 0, 0, tiled=True)

    w_t, parts = after(w_out.T, sent), []
    z1, z7, z2, z6 = [shift(w_t, "pop_1", 8, e) for e in (1, 7, 2, 6)]
    z3, z5 = shift(z1, "pop_1", 8, 2), shift(z7, "pop_1", 8, 6)
    z4 = [shift(z2[:24], "pop_1", 8, 2), shift(z6[24:], "pop_1", 8, 6)]
    for i, ins in enumerate(([w_t, z1, z7, z2, z6], [z3, z5, *z4])):
        n, via = len(GROUPS[i]), VIA_UP[i]
        own = call(stack_kernel, shape((n, 56, feats)), ins)
        up, down = shift(own, "pop_0", 4, 1), shift(own, "pop_0", 4, 3)
        far = [shift(up[:via], "pop_0", 4, 1), shift(down[via:], "pop_0", 4, 3)]
        parts.append([own, up, down, *far])
    where = ints(c, *[(x + d - y) % 4 for d in (0, -1, 1, 2)])

    cos_all, sin_all = tables(jnp.arange(tok, dtype=F32), HEAD_DIM)
    k32 = jnp.dot(tokens, w_key, preferred_element_type=F32)
    keys = (k32 * cos_all + jnp.roll(k32, 64, axis=1) * sin_all).astype(BF16)
    values = jnp.dot(tokens, w_value, preferred_element_type=F32).astype(BF16)
    cos8, sin8 = tables((k * 8).astype(F32) + jnp.arange(8, dtype=F32), HEAD_DIM)

    half_base = jnp.sum(recv[:, :, :feats].astype(F32), axis=0)
    mixed = call(
        functools.partial(attention_kernel, heads),
        shape((272, feats)),
        (ints(k * 8), recv, half_base, swap(half_base), keys, values, cos8, sin8),
        smem=1,
    )
    mixed_b = swap(mixed)

    outs = [
        call(
            project_kernel,
            [shape((7 * len(group) + 2, 8, 512))] * 4,
            (where, *pieces, mixed, mixed_b),
            smem=1,
            scratch=[
                pltpu.VMEM((4, len(group), 56, feats), BF16),
                pltpu.VMEM((2, 272, feats), BF16),
                pltpu.VMEM((4, 7 * len(group) + 2, 8, 512), BF16),
                pltpu.SemaphoreType.DMA((38,)),
            ],
            load=False,
        )
        for group, pieces in zip(GROUPS, parts)
    ]
    mets = []
    for out in outs:
        mets.append([out[0]] + [shift(out[s], "mp", 4, s) for s in (2, 1, 3)])

    order = jnp.array([e for group in GROUPS for e in group])
    which = (jnp.arange(8)[:, None] - order[None]) % 8
    o_r = after(o_right[0], sent)
    o_cut = lax.dynamic_slice(o_r, (0, feats * y), (RANK, feats)).reshape(RANK, 8, 2, 56) * half
    one = (which[:, :, None] == jnp.arange(8)).astype(BF16)
    o_cut = jnp.einsum("kiz,rzcf->kcrif", one, o_cut, preferred_element_type=F32).astype(BF16)
    o_cut = jnp.broadcast_to(o_cut.reshape(1, 16, RANK, 448), (4, 16, RANK, 448)).reshape(64, RANK, 448)
    cut_q = jnp.moveaxis((after(left_t, sent) * twice).reshape(RANK, 64, 56), 1, 0)
    cut_o = jnp.moveaxis((o_r * twice).reshape(RANK, 64, 56), 1, 0)
    gap = jnp.zeros((64, RANK, 8), BF16)
    late = jnp.concatenate([cut_q, gap, cut_o, gap, o_cut, jnp.zeros((64, RANK, 64), BF16)], axis=2)
    late = lax.all_to_all(late, POP, 0, 0, tiled=True)
    factors = after(recv, outs[0][0])[:, :, 1024:1920]
    factors_b = swap(factors)
    lefts = late[:, :, :128].reshape(32, 8, 128)
    goal = lax.dynamic_slice(target, (8 * k, 0), (8, feats)).reshape(8, 8, 2, 56)
    goal = jnp.where(c == 0, goal[:, :, 0], goal[:, :, 1])
    here = (((z - order) % 8)[:, None] == jnp.arange(8)).astype(BF16)
    goal = jnp.einsum("iz,tzf->tif", here, goal, preferred_element_type=F32).astype(BF16).reshape(8, 448)
    err = jnp.zeros((8, 1, 512), F32)
    start = 128
    for group, met in zip(GROUPS, mets):
        n = 56 * len(group)
        right = late[:, :, start : start + n].reshape(256, n)
        part = goal[:, start - 128 : start - 128 + n]
        start += n
        err = call(error_kernel, shape((8, 1, 512), F32), (*met, right, part, err))

    err = lax.all_to_all(err, ("pop_2", "mp"), 0, 0, tiled=True)
    err = jnp.sum(err, axis=0, keepdims=True)
    err = lax.all_to_all(jnp.broadcast_to(err, (32, 1, 512)), CHIPS, 0, 0, tiled=True)
    grad_query, grad_out, fitness = call(
        final_kernel,
        [shape((56, feats), F32), shape((56, feats), F32), shape((1, 128), F32)],
        (ints(c, k), err, lefts, factors, factors_b),
        smem=1,
    )
    return (grad_query, grad_out.T, fitness[0, :1])


def solution(mesh):
    torus = Mesh(mesh.devices.reshape(4, 8, 2, mesh.shape["mp"]), ("pop_0", "pop_1", "pop_2", "mp"))
    placed = (
        P(),
        P(None, "mp"),
        P(POP, "mp"),
        P(None, "mp"),
        P(None, "mp"),
        P("mp", POP),
        P(POP, None, None),
        P(POP, None, "mp"),
        P(POP, "mp", None),
        P(POP, None, None),
        P(POP),
    )
    return jax.shard_map(
        per_device,
        mesh=torus,
        in_specs=placed,
        out_specs=(P(POP, "mp"), P("mp", POP), P(POP)),
        check_vma=False,
    )
```

```python
import functools
import math

import jax
import jax.numpy as jnp
from jax import lax
from jax.experimental import pallas as pl
from jax.experimental.pallas import tpu as pltpu
from jax.sharding import Mesh
from jax.sharding import PartitionSpec as P

D = 3584
HEAD_DIM = 128
RANK = 4
POP = ("pop_0", "pop_1", "pop_2")
CHIPS = ("pop_0", "pop_1")

rope_base = 1000000.0
spread_floor = 0.001

F32 = jnp.float32
BF16 = jnp.bfloat16
NT = (((1,), (1,)), ((), ()))
TN = (((0,), (0,)), ((), ()))


def iota(shape, dim):
    return lax.broadcasted_iota(jnp.int32, shape, dim)


def shift(x, axis, size, step):
    return lax.ppermute(x, axis, [(i, (i + step) % size) for i in range(size)])


def swap(x):
    return lax.ppermute(x, "pop_2", [(0, 1), (1, 0)])


def tables(position, head_size):
    index = jnp.arange(head_size // 2, dtype=F32)
    freq = jnp.exp(-math.log(rope_base) * 2.0 * index / head_size)
    angle = position[:, None] * freq[None, :]
    c, s = jnp.cos(angle), jnp.sin(angle)
    return jnp.concatenate([c, c], axis=-1), jnp.concatenate([-s, s], axis=-1)


def front_kernel(where_ref, tokens_ref, w_ref, left_ref, right_ref, o_ref, turn_ref, out_ref, pad_ref):
    p = where_ref[0]
    start = pl.multiple_of(jnp.minimum((56 * p) // 128 * 128, 3584 - 256), 128)
    at = pl.multiple_of(56 * p - start, 8)
    pad_ref[...] = jnp.zeros_like(pad_ref)
    pad_ref[pl.ds(at, 56), :] = w_ref[...].astype(F32)
    window = tokens_ref[:, pl.ds(start, 256)]
    share = jnp.dot(window, pad_ref[...].astype(BF16), preferred_element_type=F32)
    out_ref[:, :, 0:896] = share.reshape(32, 8, 896).astype(BF16)
    left = left_ref[...].astype(F32)
    left = jnp.concatenate([left, jnp.zeros_like(left)], axis=0).astype(BF16)
    low = lax.dot_general(tokens_ref[...], left, NT, preferred_element_type=F32)
    low = low.astype(BF16).astype(F32) * jnp.where(where_ref[1] == 0, 0.5, -0.5)
    out_ref[:, :, 896:1024] = jnp.zeros((32, 8, 128), BF16)
    out_ref[:, :, 896:904] = low.reshape(32, 8, 8).astype(BF16)
    both = jnp.concatenate([right_ref[...].astype(F32), o_ref[...].astype(F32)], axis=0)
    out_ref[:, :, 1024:1920] = jnp.broadcast_to(both[None], (32, 8, 896)).astype(BF16)
    turn = turn_ref[:, pl.ds(pl.multiple_of(896 * where_ref[2], 128), 896)].astype(F32)
    turn = jnp.concatenate([turn[:, :448], turn[:, 448:]], axis=0) * jnp.where(where_ref[1] == 0, 0.5, -0.5)
    out_ref[:, :, 1920:2368] = jnp.broadcast_to(turn[None], (32, 8, 448)).astype(BF16)


def attention_kernel(heads, where_ref, recv_ref, base_ref, other_ref, keys_ref, values_ref, cos_ref, sin_ref, mixed_ref):
    tok = keys_ref.shape[0]
    rows = 256
    scale = HEAD_DIM ** (-0.5)
    factors = recv_ref[:, :, 1024:1920].astype(F32).reshape(rows, 896).astype(BF16)
    small = recv_ref[:, :, 896:1024].astype(F32).reshape(rows, 128).astype(BF16)
    lane = iota((128, rows), 1)
    pick = (iota((128, rows), 0) == (lane & 3)).astype(BF16)
    spread = jnp.dot(small, pick, preferred_element_type=F32)
    r, c = iota((rows, rows), 0), iota((rows, rows), 1)
    mine = (r >> 3) == (c >> 3)
    left = jnp.where(mine & ((c & 7) < 4), spread, 0.0).astype(BF16)
    low = jnp.dot(left, factors, preferred_element_type=F32)
    cos = jnp.broadcast_to(cos_ref[...][None], (rows // 8, 8, 128)).reshape(rows, 128)
    sin = jnp.broadcast_to(sin_ref[...][None], (rows // 8, 8, 128)).reshape(rows, 128)
    keys, values = keys_ref[...], values_ref[...]
    seen = (iota((rows, tok), 0) & 7) + where_ref[0] >= iota((rows, tok), 1)
    for h in range(heads):
        at = slice(h * 128, (h + 1) * 128)
        base = base_ref[:, at] + other_ref[:, at]
        q = jnp.broadcast_to(base[None], (rows // 8, 8, 128)).reshape(rows, 128) + low[:, at]
        q = (q * cos + pltpu.roll(q, 64, 1) * sin).astype(BF16)
        s = lax.dot_general(q, keys, NT, preferred_element_type=F32) * scale
        s = jnp.where(seen, s, -1e30)
        e = jnp.exp(s - jnp.max(s, axis=1, keepdims=True))
        p = (e / jnp.sum(e, axis=1, keepdims=True)).astype(BF16)
        mixed_ref[0:256, at] = jnp.dot(p, values, preferred_element_type=F32).astype(BF16)
    d = lax.dot_general(factors, mixed_ref[0:256, :], NT, preferred_element_type=F32)
    d = jnp.where(mine & ((r & 7) >= 4), d, 0.0).reshape(rows // 8, 8, rows)
    d = jnp.sum(d, axis=0)
    hi = d.astype(BF16).astype(F32)
    mixed_ref[256:272, :] = jnp.zeros((16, 896), BF16)
    mixed_ref[256:272, 0:256] = jnp.concatenate([hi, d - hi], axis=0).astype(BF16)


def stack_kernel(*refs):
    *ins, out_ref = refs
    for e in range(out_ref.shape[0] - 1):
        out_ref[e] = ins[e][...]
    at = 0
    for ref in ins[out_ref.shape[0] - 1 :]:
        out_ref[out_ref.shape[0] - 1, at : at + ref.shape[0]] = ref[...]
        at += ref.shape[0]


def project_kernel(where_ref, *refs):
    pieces, (own_ref, other_ref), out_refs = refs[:5], refs[5:7], refs[7:11]
    w_ref, mixed_ref, hold_ref, sems = refs[11:]
    groups = w_ref.shape[1] // 8
    copies = []
    for d, piece in enumerate(pieces):
        first = pieces[3].shape[0] if d == 4 else 0
        for e in range(piece.shape[0]):
            place = w_ref.at[where_ref[1 + min(d, 3)], pl.ds(56 * (first + e), 56)]
            copies.append(pltpu.make_async_copy(piece.at[e], place, sems.at[5 * d + e]))
    copies.append(pltpu.make_async_copy(own_ref, mixed_ref.at[0], sems.at[32]))
    copies.append(pltpu.make_async_copy(other_ref, mixed_ref.at[1], sems.at[33]))
    for copy in copies:
        copy.start()
    for copy in copies:
        copy.wait()
    sides = [pl.ds(pl.multiple_of(256 * a, 128), 256) for a in (where_ref[0], 1 - where_ref[0])]
    outs = []
    for j in range(4):
        w = w_ref[j]
        for i, at in enumerate(sides):
            got = lax.dot_general(w, mixed_ref[i, 0:256, :], NT, preferred_element_type=F32)
            hold_ref[j, 0:groups, :, at] = got.reshape(groups, 8, 256).astype(BF16)
            low = mixed_ref[i, 256:272, 0:256].astype(F32).reshape(2, 8, 256)
            hold_ref[j, groups : groups + 2, :, at] = low.astype(BF16)
        outs.append(pltpu.make_async_copy(hold_ref.at[j], out_refs[j], sems.at[34 + j]))
        outs[-1].start()
    for copy in outs:
        copy.wait()


def error_kernel(group, where_ref, *refs):
    recv_refs, (own_ref, other_ref, target_ref, so_far_ref, err_ref) = refs[:4], refs[4:]
    core, z = where_ref[0], where_ref[1]
    groups = recv_refs[0].shape[0] - 2
    feats = groups * 8
    total = low = 0.0
    for ref in recv_refs:
        total = total + ref[0:groups].astype(F32)
        low = low + ref[groups : groups + 2].astype(F32)
    total = total.reshape(feats, 512)
    low = low[0] + low[1]
    low = pltpu.roll(low, 4, 0) + low

    def source(rows):
        g = iota((rows, feats), 1)
        at = g + 56 * core
        for i, e in enumerate(group):
            shift = 112 * lax.rem(z + 8 - e, 8) - 56 * i
            at = at + jnp.where((g >= 56 * i) & (g < 56 * i + 56), shift, 0)
        return at

    wide = (iota((896, feats), 0) == source(896)).astype(BF16)
    at = source(448)
    half = (iota((448, feats), 0) == jnp.where(at >= 448, at - 448, at)).astype(BF16)
    late = source(256) >= 448
    tile = (iota((8, 512), 0) == (iota((8, 512), 1) & 7)).astype(BF16)
    target = jnp.dot(target_ref[...], wide, preferred_element_type=F32).astype(BF16)
    total = total - lax.dot_general(target, tile, TN, preferred_element_type=F32)
    r, c = iota((256, 512), 0), iota((256, 512), 1)
    same = (r >> 3) == ((c & 255) >> 3)
    low = jnp.broadcast_to(low[None], (32, 8, 512)).reshape(256, 512)
    for side, ref in ((core, own_ref), (1 - core, other_ref)):
        right = ref[:, :, 896:1344].astype(F32).reshape(256, 448).astype(BF16)
        right = jnp.dot(right, half, preferred_element_type=F32)
        right = jnp.where(late == ((iota((256, feats), 0) & 7) >= 4), right, 0.0).astype(BF16)
        rest = jnp.where(same & ((c >> 8) == side), low, 0.0)
        for _ in range(3):
            piece = rest.astype(BF16)
            total = total + lax.dot_general(right, piece, TN, preferred_element_type=F32)
            rest = rest - piece.astype(F32)
    err = jnp.sum((total * total).reshape(groups, 8, 512), axis=0)
    err = jnp.sum(err, axis=0, keepdims=True) + so_far_ref[0]
    err_ref[...] = jnp.broadcast_to(err[None], (4, 1, 512))


def final_kernel(where_ref, err_ref, left_ref, own_ref, other_ref, query_ref, out_ref, fit_ref):
    core, chip = where_ref[0], where_ref[1]
    err = jnp.sum(err_ref[...], axis=0)
    at = iota((256, 512), 1)
    row = iota((256, 512), 0)
    member = ((at & 255) >> 3) * 2 + (at >> 8)
    err = jnp.where(member == (row >> 2), jnp.broadcast_to(err, (256, 512)), 0.0)
    fit = -(jnp.sum(err, axis=1, keepdims=True) / (256 * D))
    mean = jnp.sum(fit, axis=0, keepdims=True) / 256
    away = fit - mean
    spread = jnp.sum(away * away, axis=0, keepdims=True) / 256
    weight = away / jnp.sqrt(spread + spread_floor)
    me = iota((256, 128), 0) == 4 * (2 * chip + core)
    fit_ref[...] = jnp.sum(jnp.where(me, jnp.broadcast_to(fit, (256, 128)), 0.0), axis=0, keepdims=True)
    left = left_ref[...].astype(F32).reshape(256, 128) * weight
    left = left.reshape(32, 8, 128)
    turned = pltpu.roll(left, 4, 1)
    low = jnp.where(core == 0, left, turned)
    high = jnp.where(core == 0, turned, left)
    upper, narrow = iota((32, 8, 128), 1) < 4, iota((32, 8, 128), 2) < 64
    total = 0.0
    for ref, a, b in ((own_ref, low, high), (other_ref, high, low)):
        l = jnp.where(narrow, jnp.where(upper, a, 0.0), jnp.where(upper, 0.0, b)).reshape(256, 128)
        parts = []
        for _ in range(3):
            parts.append(l.astype(BF16))
            l = l - parts[-1].astype(F32)
        right = ref[:, :, 0:896].astype(F32).reshape(256, 896).astype(BF16)
        g = lax.dot_general(jnp.concatenate(parts, axis=1), right, TN, preferred_element_type=F32)
        total = total + g[0:128] + g[128:256] + g[256:384]
    query_ref[...] = total[0:56]
    out_ref[...] = total[64:120]


def loaded(kernel, smem, n_in, n_out):
    def body(*refs):
        scalars, refs = refs[:smem], refs[smem:]
        ins, outs, refs = refs[:n_in], refs[n_in : n_in + n_out], refs[n_in + n_out :]
        held, results, refs = refs[:n_in], refs[n_in : n_in + n_out], refs[n_in + n_out :]
        *rest, sems = refs
        copies = [pltpu.make_async_copy(a, b, sems.at[i]) for i, (a, b) in enumerate(zip(ins, held))]
        for copy in copies:
            copy.start()
        for copy in copies:
            copy.wait()
        kernel(*scalars, *held, *results, *rest)
        copies = [pltpu.make_async_copy(b, a, sems.at[n_in + i]) for i, (a, b) in enumerate(zip(outs, results))]
        for copy in copies:
            copy.start()
        for copy in copies:
            copy.wait()

    return body


def call(kernel, out, args, smem=0, flops=10**9, scratch=(), load=True):
    outs = out if isinstance(out, (list, tuple)) else [out]
    ins = args[smem:]
    scratch = list(scratch)
    if load:
        kernel = loaded(kernel, smem, len(ins), len(outs))
        scratch = [pltpu.VMEM(a.shape, a.dtype) for a in (*ins, *outs)] + scratch
        scratch.append(pltpu.SemaphoreType.DMA((len(ins) + len(outs),)))
    hbm = pl.BlockSpec(memory_space=pltpu.HBM)
    return pl.pallas_call(
        kernel,
        out_shape=out,
        in_specs=[pl.BlockSpec(memory_space=pltpu.SMEM)] * smem + [hbm] * len(ins),
        out_specs=jax.tree.map(lambda _: hbm, out),
        scratch_shapes=scratch,
        cost_estimate=pl.CostEstimate(flops=flops, bytes_accessed=2 * 10**6, transcendentals=0),
    )(*args)


def shape(s, t=BF16):
    return jax.ShapeDtypeStruct(s, t)


def after(x, y):
    return lax.optimization_barrier((x, y))[0]


def ints(*values):
    return jnp.stack([jnp.asarray(v, jnp.int32) for v in values])


GROUPS = ((0, 1, 7, 2, 6), (3, 5, 4))
VIA_UP = (3, 1)


def per_device(
    tokens,
    target,
    w_query,
    w_key,
    w_value,
    w_out,
    query_left_factors,
    query_right_factors,
    o_left,
    o_right,
    member_ids,
):
    tok = tokens.shape[0]
    feats = w_query.shape[1]
    heads = feats // HEAD_DIM
    x, z, c = (lax.axis_index(a) for a in POP)
    y = lax.axis_index("mp")
    k = x * 8 + z
    p = 2 * k + c
    odd = member_ids[0] % 2
    half = jnp.where(odd == 0, 0.5, -0.5).astype(BF16)
    twice = jnp.where(odd == 0, 2.0, -2.0).astype(BF16)
    left_t = query_left_factors[0].T

    sent = call(
        front_kernel,
        shape((32, 8, 2368)),
        (ints(p, odd, y), tokens, w_query, left_t, query_right_factors[0], o_left[0].T, o_right[0]),
        smem=1,
        scratch=[pltpu.VMEM((256, feats), F32)],
    )
    recv = lax.all_to_all(sent, CHIPS, 0, 0, tiled=True)

    w_t, parts = after(w_out.T, sent), []
    z1, z7, z2, z6 = [shift(w_t, "pop_1", 8, e) for e in (1, 7, 2, 6)]
    z3, z5 = shift(z1, "pop_1", 8, 2), shift(z7, "pop_1", 8, 6)
    z4 = [shift(z2[:24], "pop_1", 8, 2), shift(z6[24:], "pop_1", 8, 6)]
    for i, ins in enumerate(([w_t, z1, z7, z2, z6], [z3, z5, *z4])):
        n, via = len(GROUPS[i]), VIA_UP[i]
        own = call(stack_kernel, shape((n, 56, feats)), ins)
        up, down = shift(own, "pop_0", 4, 1), shift(own, "pop_0", 4, 3)
        far = [shift(up[:via], "pop_0", 4, 1), shift(down[via:], "pop_0", 4, 3)]
        parts.append([own, up, down, *far])
    where = ints(c, *[(x + d - y) % 4 for d in (0, -1, 1, 2)])

    cos_all, sin_all = tables(jnp.arange(tok, dtype=F32), HEAD_DIM)
    k32 = jnp.dot(tokens, w_key, preferred_element_type=F32)
    keys = (k32 * cos_all + jnp.roll(k32, 64, axis=1) * sin_all).astype(BF16)
    values = jnp.dot(tokens, w_value, preferred_element_type=F32).astype(BF16)
    cos8, sin8 = tables((k * 8).astype(F32) + jnp.arange(8, dtype=F32), HEAD_DIM)

    half_base = jnp.sum(recv[:, :, :feats].astype(F32), axis=0)
    mixed = call(
        functools.partial(attention_kernel, heads),
        shape((272, feats)),
        (ints(k * 8), recv, half_base, swap(half_base), keys, values, cos8, sin8),
        smem=1,
    )
    mixed_b = swap(mixed)

    outs = [
        call(
            project_kernel,
            [shape((7 * len(group) + 2, 8, 512))] * 4,
            (where, *pieces, mixed, mixed_b),
            smem=1,
            scratch=[
                pltpu.VMEM((4, 56 * len(group), feats), BF16),
                pltpu.VMEM((2, 272, feats), BF16),
                pltpu.VMEM((4, 7 * len(group) + 2, 8, 512), BF16),
                pltpu.SemaphoreType.DMA((38,)),
            ],
            load=False,
        )
        for group, pieces in zip(GROUPS, parts)
    ]
    mets = []
    for out in outs:
        mets.append([out[0]] + [shift(out[s], "mp", 4, s) for s in (2, 1, 3)])

    cut_q = jnp.moveaxis((after(left_t, sent) * twice).reshape(RANK, 64, 56), 1, 0)
    cut_o = jnp.moveaxis((after(o_right[0], sent) * twice).reshape(RANK, 64, 56), 1, 0)
    gap = jnp.zeros((64, RANK, 8), BF16)
    late = jnp.concatenate([cut_q, gap, cut_o, gap], axis=2)
    late = lax.all_to_all(late, POP, 0, 0, tiled=True)
    factors = after(recv, mixed)[:, :, 1024:2368]
    factors_b = swap(factors)
    lefts = late.reshape(32, 8, 128)
    goal = lax.dynamic_slice(target, (8 * k, 0), (8, feats))
    err = jnp.zeros((4, 1, 512), F32)
    for group, met in zip(GROUPS, mets):
        err = call(
            functools.partial(error_kernel, group),
            shape((4, 1, 512), F32),
            (ints(c, z), *met, factors, factors_b, goal, err if met is mets[0] else after(err, late)),
            smem=1,
        )

    err = lax.all_to_all(err, "mp", 0, 0, tiled=True)
    err = jnp.sum(err, axis=0, keepdims=True)
    err = lax.all_to_all(jnp.broadcast_to(err, (64, 1, 512)), POP, 0, 0, tiled=True)
    grad_query, grad_out, fitness = call(
        final_kernel,
        [shape((56, feats), F32), shape((56, feats), F32), shape((1, 128), F32)],
        (ints(c, k), err, lefts, factors, factors_b),
        smem=1,
    )
    return (grad_query, grad_out.T, fitness[0, :1])


def solution(mesh):
    torus = Mesh(mesh.devices.reshape(4, 8, 2, mesh.shape["mp"]), ("pop_0", "pop_1", "pop_2", "mp"))
    placed = (
        P(),
        P(None, "mp"),
        P(POP, "mp"),
        P(None, "mp"),
        P(None, "mp"),
        P("mp", POP),
        P(POP, None, None),
        P(POP, None, "mp"),
        P(POP, "mp", None),
        P(POP, None, None),
        P(POP),
    )
    return jax.shard_map(
        per_device,
        mesh=torus,
        in_specs=placed,
        out_specs=(P(POP, "mp"), P("mp", POP), P(POP)),
        check_vma=False,
    )
```

```python
import functools
import math

import jax
import jax.numpy as jnp
from jax import lax
from jax.experimental import pallas as pl
from jax.experimental.pallas import tpu as pltpu
from jax.sharding import Mesh
from jax.sharding import PartitionSpec as P

D = 3584
HEAD_DIM = 128
RANK = 4
POP = ("pop_0", "pop_1", "pop_2")
CHIPS = ("pop_0", "pop_1")

rope_base = 1000000.0
spread_floor = 0.001

F32 = jnp.float32
BF16 = jnp.bfloat16
NT = (((1,), (1,)), ((), ()))
TN = (((0,), (0,)), ((), ()))


def iota(shape, dim):
    return lax.broadcasted_iota(jnp.int32, shape, dim)


def shift(x, axis, size, step):
    return lax.ppermute(x, axis, [(i, (i + step) % size) for i in range(size)])


def swap(x):
    return lax.ppermute(x, "pop_2", [(0, 1), (1, 0)])


def tables(position, head_size):
    index = jnp.arange(head_size // 2, dtype=F32)
    freq = jnp.exp(-math.log(rope_base) * 2.0 * index / head_size)
    angle = position[:, None] * freq[None, :]
    c, s = jnp.cos(angle), jnp.sin(angle)
    return jnp.concatenate([c, c], axis=-1), jnp.concatenate([-s, s], axis=-1)


def front_kernel(where_ref, tokens_ref, w_ref, left_ref, right_ref, o_ref, out_ref, pad_ref):
    p = where_ref[0]
    start = pl.multiple_of(jnp.minimum((56 * p) // 128 * 128, 3584 - 256), 128)
    at = pl.multiple_of(56 * p - start, 8)
    pad_ref[...] = jnp.zeros_like(pad_ref)
    pad_ref[pl.ds(at, 56), :] = w_ref[...].astype(F32)
    window = tokens_ref[:, pl.ds(start, 256)]
    share = jnp.dot(window, pad_ref[...].astype(BF16), preferred_element_type=F32)
    out_ref[:, :, 0:896] = share.reshape(32, 8, 896).astype(BF16)
    left = left_ref[...].astype(F32)
    left = jnp.concatenate([left, jnp.zeros_like(left)], axis=0).astype(BF16)
    low = lax.dot_general(tokens_ref[...], left, NT, preferred_element_type=F32)
    low = low.astype(BF16).astype(F32) * jnp.where(where_ref[1] == 0, 0.5, -0.5)
    out_ref[:, :, 896:1024] = jnp.zeros((32, 8, 128), BF16)
    out_ref[:, :, 896:904] = low.reshape(32, 8, 8).astype(BF16)
    both = jnp.concatenate([right_ref[...].astype(F32), o_ref[...].astype(F32)], axis=0)
    out_ref[:, :, 1024:1920] = jnp.broadcast_to(both[None], (32, 8, 896)).astype(BF16)


def attention_kernel(heads, where_ref, recv_ref, base_ref, other_ref, keys_ref, values_ref, cos_ref, sin_ref, mixed_ref):
    tok = keys_ref.shape[0]
    rows = 256
    scale = HEAD_DIM ** (-0.5)
    factors = recv_ref[:, :, 1024:1920].astype(F32).reshape(rows, 896).astype(BF16)
    small = recv_ref[:, :, 896:1024].astype(F32).reshape(rows, 128).astype(BF16)
    lane = iota((128, rows), 1)
    pick = (iota((128, rows), 0) == (lane & 3)).astype(BF16)
    spread = jnp.dot(small, pick, preferred_element_type=F32)
    r, c = iota((rows, rows), 0), iota((rows, rows), 1)
    mine = (r >> 3) == (c >> 3)
    left = jnp.where(mine & ((c & 7) < 4), spread, 0.0).astype(BF16)
    low = jnp.dot(left, factors, preferred_element_type=F32)
    cos = jnp.broadcast_to(cos_ref[...][None], (rows // 8, 8, 128)).reshape(rows, 128)
    sin = jnp.broadcast_to(sin_ref[...][None], (rows // 8, 8, 128)).reshape(rows, 128)
    keys, values = keys_ref[...], values_ref[...]
    seen = (iota((rows, tok), 0) & 7) + where_ref[0] >= iota((rows, tok), 1)
    for h in range(heads):
        at = slice(h * 128, (h + 1) * 128)
        base = base_ref[:, at] + other_ref[:, at]
        q = jnp.broadcast_to(base[None], (rows // 8, 8, 128)).reshape(rows, 128) + low[:, at]
        q = (q * cos + pltpu.roll(q, 64, 1) * sin).astype(BF16)
        s = lax.dot_general(q, keys, NT, preferred_element_type=F32) * scale
        s = jnp.where(seen, s, -1e30)
        e = jnp.exp(s - jnp.max(s, axis=1, keepdims=True))
        p = (e / jnp.sum(e, axis=1, keepdims=True)).astype(BF16)
        mixed_ref[0:256, at] = jnp.dot(p, values, preferred_element_type=F32).astype(BF16)
    d = lax.dot_general(factors, mixed_ref[0:256, :], NT, preferred_element_type=F32)
    d = jnp.where(mine & ((r & 7) >= 4), d, 0.0).reshape(rows // 8, 8, rows)
    d = jnp.sum(d, axis=0)
    hi = d.astype(BF16).astype(F32)
    mixed_ref[256:272, :] = jnp.zeros((16, 896), BF16)
    mixed_ref[256:272, 0:256] = jnp.concatenate([hi, d - hi], axis=0).astype(BF16)


def stack_kernel(*refs):
    *ins, out_ref = refs
    for e, ref in enumerate(ins):
        out_ref[e] = ref[...]


def project_kernel(where_ref, *refs):
    pieces, (own_ref, other_ref), out_refs = refs[:5], refs[5:7], refs[7:11]
    w_ref, mixed_ref, low_ref, hold_ref, sems = refs[11:]
    groups = 7 * w_ref.shape[1]
    core = where_ref[0]
    copies = []
    for i, (ref, side) in enumerate(((own_ref, core), (other_ref, 1 - core))):
        at = pl.ds(pl.multiple_of(256 * side, 256), 256)
        copies.append(pltpu.make_async_copy(ref.at[pl.ds(0, 256)], mixed_ref.at[at], sems.at[i]))
        copies.append(pltpu.make_async_copy(ref.at[pl.ds(256, 16)], low_ref.at[side], sems.at[2 + i]))
    loads = []
    for d, piece in enumerate(pieces):
        place = w_ref.at[min(d, 3)]
        if d >= 3:
            place = place.at[pl.ds(pieces[3].shape[0] * (d - 3), piece.shape[0])]
        loads.append(pltpu.make_async_copy(piece, place, sems.at[4 + d]))
    for copy in copies + loads:
        copy.start()
    for copy in copies:
        copy.wait()
    low = [low_ref[i, :, 0:256].astype(F32).reshape(2, 8, 256) for i in range(2)]
    low = jnp.concatenate(low, axis=2).astype(BF16)
    for d in range(4):
        for copy in loads[d : d + 1] if d < 3 else loads[3:]:
            copy.wait()
        w = w_ref[d].astype(F32).reshape(8 * groups, 896).astype(BF16)
        got = lax.dot_general(w, mixed_ref[...], NT, preferred_element_type=F32)
        at = where_ref[1 + d]
        hold_ref[at, 0:groups] = got.reshape(groups, 8, 512).astype(BF16)
        hold_ref[at, groups : groups + 2] = low
    outs = [pltpu.make_async_copy(hold_ref.at[j], out_refs[j], sems.at[9 + j]) for j in range(4)]
    for copy in outs:
        copy.start()
    for copy in outs:
        copy.wait()


def error_kernel(core_ref, *refs):
    recv_refs, (right_ref, target_ref, so_far_ref, err_ref) = refs[:4], refs[4:]
    groups = recv_refs[0].shape[0] - 2
    feats = groups * 8
    total = low = 0.0
    for ref in recv_refs:
        total = total + ref[0:groups].astype(F32)
        low = low + ref[groups : groups + 2].astype(F32)
    tile = (iota((8, 512), 0) == (iota((8, 512), 1) & 7)).astype(BF16)
    target = lax.dot_general(target_ref[...], tile, TN, preferred_element_type=F32)
    total = total.reshape(feats, 512) - target
    low = low[0] + low[1]
    low = pltpu.roll(low, 4, 0) + low
    low = jnp.broadcast_to(low[None], (32, 8, 512)).reshape(256, 512)
    r, c = iota((256, 512), 0), iota((256, 512), 1)
    mine = ((r >> 3) == ((c & 255) >> 3)) & (((r & 7) >> 2) == ((c >> 8) ^ core_ref[0]))
    low = jnp.where(mine, low, 0.0)
    right = right_ref[...]
    for _ in range(3):
        piece = low.astype(BF16)
        total = total + lax.dot_general(right, piece, TN, preferred_element_type=F32)
        low = low - piece.astype(F32)
    err = jnp.sum((total * total).reshape(groups, 8, 512), axis=0)
    err = jnp.sum(err, axis=0, keepdims=True) + so_far_ref[0]
    err_ref[...] = jnp.broadcast_to(err[None], (4, 1, 512))


def final_kernel(where_ref, err_ref, left_ref, own_ref, other_ref, query_ref, out_ref, fit_ref):
    core, chip = where_ref[0], where_ref[1]
    err = jnp.sum(err_ref[...], axis=0)
    at = iota((256, 512), 1)
    row = iota((256, 512), 0)
    member = ((at & 255) >> 3) * 2 + (at >> 8)
    mine = 2 * (row >> 3) + (((row & 7) >> 2) ^ core)
    err = jnp.where(member == mine, jnp.broadcast_to(err, (256, 512)), 0.0)
    fit = -(jnp.sum(err, axis=1, keepdims=True) / (256 * D))
    mean = jnp.sum(fit, axis=0, keepdims=True) / 256
    away = fit - mean
    spread = jnp.sum(away * away, axis=0, keepdims=True) / 256
    weight = away / jnp.sqrt(spread + spread_floor)
    me = iota((256, 128), 0) == 8 * chip
    fit_ref[...] = jnp.sum(jnp.where(me, jnp.broadcast_to(fit, (256, 128)), 0.0), axis=0, keepdims=True)
    left = left_ref[...].astype(F32).reshape(256, 128) * weight
    left = left.reshape(32, 8, 128)
    turned = pltpu.roll(left, 4, 1)
    low, high = left, turned
    upper, narrow = iota((32, 8, 128), 1) < 4, iota((32, 8, 128), 2) < 64
    total = 0.0
    for ref, a, b in ((own_ref, low, high), (other_ref, high, low)):
        l = jnp.where(narrow, jnp.where(upper, a, 0.0), jnp.where(upper, 0.0, b)).reshape(256, 128)
        parts = []
        for _ in range(3):
            parts.append(l.astype(BF16))
            l = l - parts[-1].astype(F32)
        right = ref[...].astype(F32).reshape(256, 896).astype(BF16)
        g = lax.dot_general(jnp.concatenate(parts, axis=1), right, TN, preferred_element_type=F32)
        total = total + g[0:128] + g[128:256] + g[256:384]
    query_ref[...] = total[0:56]
    out_ref[...] = total[64:120]


def loaded(kernel, smem, n_in, n_out):
    def body(*refs):
        scalars, refs = refs[:smem], refs[smem:]
        ins, outs, refs = refs[:n_in], refs[n_in : n_in + n_out], refs[n_in + n_out :]
        held, results, refs = refs[:n_in], refs[n_in : n_in + n_out], refs[n_in + n_out :]
        *rest, sems = refs
        copies = [pltpu.make_async_copy(a, b, sems.at[i]) for i, (a, b) in enumerate(zip(ins, held))]
        for copy in copies:
            copy.start()
        for copy in copies:
            copy.wait()
        kernel(*scalars, *held, *results, *rest)
        copies = [pltpu.make_async_copy(b, a, sems.at[n_in + i]) for i, (a, b) in enumerate(zip(outs, results))]
        for copy in copies:
            copy.start()
        for copy in copies:
            copy.wait()

    return body


def call(kernel, out, args, smem=0, flops=10**9, scratch=(), load=True):
    outs = out if isinstance(out, (list, tuple)) else [out]
    ins = args[smem:]
    scratch = list(scratch)
    if load:
        kernel = loaded(kernel, smem, len(ins), len(outs))
        scratch = [pltpu.VMEM(a.shape, a.dtype) for a in (*ins, *outs)] + scratch
        scratch.append(pltpu.SemaphoreType.DMA((len(ins) + len(outs),)))
    hbm = pl.BlockSpec(memory_space=pltpu.HBM)
    return pl.pallas_call(
        kernel,
        out_shape=out,
        in_specs=[pl.BlockSpec(memory_space=pltpu.SMEM)] * smem + [hbm] * len(ins),
        out_specs=jax.tree.map(lambda _: hbm, out),
        scratch_shapes=scratch,
        cost_estimate=pl.CostEstimate(flops=flops, bytes_accessed=2 * 10**6, transcendentals=0),
    )(*args)


def shape(s, t=BF16):
    return jax.ShapeDtypeStruct(s, t)


def after(x, y):
    return lax.optimization_barrier((x, y))[0]


def ints(*values):
    return jnp.stack([jnp.asarray(v, jnp.int32) for v in values])


GROUPS = ((0, 1, 7, 2, 6), (3, 5, 4))
VIA_UP = (3, 1)


def per_device(
    tokens,
    target,
    w_query,
    w_key,
    w_value,
    w_out,
    query_left_factors,
    query_right_factors,
    o_left,
    o_right,
    member_ids,
):
    tok = tokens.shape[0]
    feats = w_query.shape[1]
    heads = feats // HEAD_DIM
    x, z, c = (lax.axis_index(a) for a in POP)
    y = lax.axis_index("mp")
    k = x * 8 + z
    p = 2 * k + c
    odd = member_ids[0] % 2
    half = jnp.where(odd == 0, 0.5, -0.5).astype(BF16)
    twice = jnp.where(odd == 0, 2.0, -2.0).astype(BF16)
    left_t = query_left_factors[0].T

    sent = call(
        front_kernel,
        shape((32, 8, 1920)),
        (ints(p, odd), tokens, w_query, left_t, query_right_factors[0], o_left[0].T),
        smem=1,
        scratch=[pltpu.VMEM((256, feats), F32)],
    )
    recv = lax.all_to_all(sent, CHIPS, 0, 0, tiled=True)

    w_t, parts = after(w_out.T, sent), []
    z1, z7, z2, z6, z3, z5, z4 = [shift(w_t, "pop_1", 8, e) for e in (1, 7, 2, 6, 3, 5, 4)]
    for i, ins in enumerate(([w_t, z1, z7, z2, z6], [z3, z5, z4])):
        n, via = len(GROUPS[i]), VIA_UP[i]
        own = call(stack_kernel, shape((n, 56, feats)), ins)
        up, down = shift(own, "pop_0", 4, 1), shift(own, "pop_0", 4, 3)
        far = [shift(up[:via], "pop_0", 4, 1), shift(down[via:], "pop_0", 4, 3)]
        parts.append([own, up, down, *far])
    where = ints(c, *[(x + d - y) % 4 for d in (0, -1, 1, 2)])

    cos_all, sin_all = tables(jnp.arange(tok, dtype=F32), HEAD_DIM)
    k32 = jnp.dot(tokens, w_key, preferred_element_type=F32)
    keys = (k32 * cos_all + jnp.roll(k32, 64, axis=1) * sin_all).astype(BF16)
    values = jnp.dot(tokens, w_value, preferred_element_type=F32).astype(BF16)
    cos8, sin8 = tables((k * 8).astype(F32) + jnp.arange(8, dtype=F32), HEAD_DIM)

    half_base = jnp.sum(recv[:, :, :feats].astype(F32), axis=0)
    mixed = call(
        functools.partial(attention_kernel, heads),
        shape((272, feats)),
        (ints(k * 8), recv, half_base, swap(half_base), keys, values, cos8, sin8),
        smem=1,
    )
    mixed_b = swap(mixed)

    outs = [
        call(
            project_kernel,
            [shape((7 * len(group) + 2, 8, 512))] * 4,
            (where, *pieces, mixed, mixed_b),
            smem=1,
            scratch=[
                pltpu.VMEM((4, len(group), 56, feats), BF16),
                pltpu.VMEM((512, feats), BF16),
                pltpu.VMEM((2, 16, feats), BF16),
                pltpu.VMEM((4, 7 * len(group) + 2, 8, 512), BF16),
                pltpu.SemaphoreType.DMA((13,)),
            ],
            load=False,
        )
        for group, pieces in zip(GROUPS, parts)
    ]
    mets = []
    for out in outs:
        mets.append([out[0]] + [shift(out[s], "mp", 4, s) for s in (2, 1, 3)])

    order = jnp.array([e for group in GROUPS for e in group])
    which = (jnp.arange(8)[:, None] - order[None]) % 8
    o_r = after(o_right[0], sent)
    o_cut = lax.dynamic_slice(o_r, (0, feats * y), (RANK, feats)).reshape(RANK, 8, 2, 56) * half
    one = (which[:, :, None] == jnp.arange(8)).astype(BF16)
    o_cut = jnp.einsum("kiz,rzcf->kcrif", one, o_cut, preferred_element_type=F32).astype(BF16)
    o_cut = jnp.where(c == 0, o_cut, o_cut[:, ::-1]).reshape(1, 8, 8, 448)
    o_cut = jnp.broadcast_to(o_cut, (4, 8, 8, 448)).reshape(32, 8, 448)

    def cut(a):
        a = jnp.moveaxis((a * twice).reshape(RANK, 32, 2, 56), 0, 2)
        return jnp.where(c == 0, a, a[:, ::-1]).reshape(32, 8, 56)

    gap = jnp.zeros((32, 8, 8), BF16)
    late = [cut(after(left_t, sent)), gap, cut(o_r), gap, o_cut, jnp.zeros((32, 8, 64), BF16)]
    late = jnp.concatenate(late, axis=2)
    late = lax.all_to_all(late, CHIPS, 0, 0, tiled=True)
    late_b = swap(late[:, 4:])
    late = jnp.concatenate([late[:, :4], late_b], axis=1)
    factors = after(recv, outs[0][0])[:, :, 1024:1920]
    factors_b = swap(factors)
    lefts = late[:, :, :128]
    goal = lax.dynamic_slice(target, (8 * k, 0), (8, feats)).reshape(8, 8, 2, 56)
    goal = jnp.where(c == 0, goal[:, :, 0], goal[:, :, 1])
    here = (((z - order) % 8)[:, None] == jnp.arange(8)).astype(BF16)
    goal = jnp.einsum("iz,tzf->tif", here, goal, preferred_element_type=F32).astype(BF16).reshape(8, 448)
    err = jnp.zeros((4, 1, 512), F32)
    start = 128
    for group, met in zip(GROUPS, mets):
        n = 56 * len(group)
        right = late[:, :, start : start + n].reshape(256, n)
        part = goal[:, start - 128 : start - 128 + n]
        start += n
        err = call(error_kernel, shape((4, 1, 512), F32), (ints(c), *met, right, part, err), smem=1)

    err = lax.all_to_all(err, "mp", 0, 0, tiled=True)
    err = jnp.sum(err, axis=0, keepdims=True)
    err = lax.all_to_all(jnp.broadcast_to(err, (64, 1, 512)), POP, 0, 0, tiled=True)
    grad_query, grad_out, fitness = call(
        final_kernel,
        [shape((56, feats), F32), shape((56, feats), F32), shape((1, 128), F32)],
        (ints(c, k), err, lefts, factors, factors_b),
        smem=1,
    )
    return (grad_query, grad_out.T, fitness[0, :1])


def solution(mesh):
    torus = Mesh(mesh.devices.reshape(4, 8, 2, mesh.shape["mp"]), ("pop_0", "pop_1", "pop_2", "mp"))
    placed = (
        P(),
        P(None, "mp"),
        P(POP, "mp"),
        P(None, "mp"),
        P(None, "mp"),
        P("mp", POP),
        P(POP, None, None),
        P(POP, None, "mp"),
        P(POP, "mp", None),
        P(POP, None, None),
        P(POP),
    )
    return jax.shard_map(
        per_device,
        mesh=torus,
        in_specs=placed,
        out_specs=(P(POP, "mp"), P("mp", POP), P(POP)),
        check_vma=False,
    )
```

```python
import functools
import math

import jax
import jax.numpy as jnp
from jax import lax
from jax.experimental import pallas as pl
from jax.experimental.pallas import tpu as pltpu
from jax.sharding import Mesh
from jax.sharding import PartitionSpec as P

D = 3584
HEAD_DIM = 128
RANK = 4
POP = ("pop_0", "pop_1", "pop_2")
CHIPS = ("pop_0", "pop_1")

rope_base = 1000000.0
spread_floor = 0.001

F32 = jnp.float32
BF16 = jnp.bfloat16
NT = (((1,), (1,)), ((), ()))
TN = (((0,), (0,)), ((), ()))


def iota(shape, dim):
    return lax.broadcasted_iota(jnp.int32, shape, dim)


def shift(x, axis, size, step):
    return lax.ppermute(x, axis, [(i, (i + step) % size) for i in range(size)])


def swap(x):
    return lax.ppermute(x, "pop_2", [(0, 1), (1, 0)])


def tables(position, head_size):
    index = jnp.arange(head_size // 2, dtype=F32)
    freq = jnp.exp(-math.log(rope_base) * 2.0 * index / head_size)
    angle = position[:, None] * freq[None, :]
    c, s = jnp.cos(angle), jnp.sin(angle)
    return jnp.concatenate([c, c], axis=-1), jnp.concatenate([-s, s], axis=-1)


def front_kernel(where_ref, tokens_ref, w_ref, left_ref, right_ref, o_ref, out_ref, pad_ref):
    p = where_ref[0]
    start = pl.multiple_of(jnp.minimum((56 * p) // 128 * 128, 3584 - 256), 128)
    at = pl.multiple_of(56 * p - start, 8)
    pad_ref[...] = jnp.zeros_like(pad_ref)
    pad_ref[pl.ds(at, 56), :] = w_ref[...].astype(F32)
    window = tokens_ref[:, pl.ds(start, 256)]
    share = jnp.dot(window, pad_ref[...].astype(BF16), preferred_element_type=F32)
    out_ref[:, :, 0:896] = share.reshape(32, 8, 896).astype(BF16)
    left = left_ref[...].astype(F32)
    left = jnp.concatenate([left, jnp.zeros_like(left)], axis=0).astype(BF16)
    low = lax.dot_general(tokens_ref[...], left, NT, preferred_element_type=F32)
    low = low.astype(BF16).astype(F32) * jnp.where(where_ref[1] == 0, 0.5, -0.5)
    out_ref[:, :, 896:1024] = jnp.zeros((32, 8, 128), BF16)
    out_ref[:, :, 896:904] = low.reshape(32, 8, 8).astype(BF16)
    both = jnp.concatenate([right_ref[...].astype(F32), o_ref[...].astype(F32)], axis=0)
    out_ref[:, :, 1024:1920] = jnp.broadcast_to(both[None], (32, 8, 896)).astype(BF16)


def attention_kernel(heads, where_ref, recv_ref, base_ref, other_ref, keys_ref, values_ref, cos_ref, sin_ref, mixed_ref):
    tok = keys_ref.shape[0]
    rows = 256
    scale = HEAD_DIM ** (-0.5)
    factors = recv_ref[:, :, 1024:1920].astype(F32).reshape(rows, 896).astype(BF16)
    small = recv_ref[:, :, 896:1024].astype(F32).reshape(rows, 128).astype(BF16)
    lane = iota((128, rows), 1)
    pick = (iota((128, rows), 0) == (lane & 3)).astype(BF16)
    spread = jnp.dot(small, pick, preferred_element_type=F32)
    r, c = iota((rows, rows), 0), iota((rows, rows), 1)
    mine = (r >> 3) == (c >> 3)
    left = jnp.where(mine & ((c & 7) < 4), spread, 0.0).astype(BF16)
    low = jnp.dot(left, factors, preferred_element_type=F32)
    cos = jnp.broadcast_to(cos_ref[...][None], (rows // 8, 8, 128)).reshape(rows, 128)
    sin = jnp.broadcast_to(sin_ref[...][None], (rows // 8, 8, 128)).reshape(rows, 128)
    keys, values = keys_ref[...], values_ref[...]
    seen = (iota((rows, tok), 0) & 7) + where_ref[0] >= iota((rows, tok), 1)
    for h in range(heads):
        at = slice(h * 128, (h + 1) * 128)
        base = base_ref[:, at] + other_ref[:, at]
        q = jnp.broadcast_to(base[None], (rows // 8, 8, 128)).reshape(rows, 128) + low[:, at]
        q = (q * cos + pltpu.roll(q, 64, 1) * sin).astype(BF16)
        s = lax.dot_general(q, keys, NT, preferred_element_type=F32) * scale
        s = jnp.where(seen, s, -1e30)
        e = jnp.exp(s - jnp.max(s, axis=1, keepdims=True))
        p = (e / jnp.sum(e, axis=1, keepdims=True)).astype(BF16)
        mixed_ref[0:256, at] = jnp.dot(p, values, preferred_element_type=F32).astype(BF16)
    d = lax.dot_general(factors, mixed_ref[0:256, :], NT, preferred_element_type=F32)
    d = jnp.where(mine & ((r & 7) >= 4), d, 0.0).reshape(rows // 8, 8, rows)
    d = jnp.sum(d, axis=0)
    hi = d.astype(BF16).astype(F32)
    mixed_ref[256:272, :] = jnp.zeros((16, 896), BF16)
    mixed_ref[256:272, 0:256] = jnp.concatenate([hi, d - hi], axis=0).astype(BF16)


def stack_kernel(*refs):
    *ins, out_ref = refs
    for e, ref in enumerate(ins):
        out_ref[e] = ref[...]


def project_kernel(plan, where_ref, *refs):
    n = sum(len(of) for of in plan)
    pieces, (own_ref, other_ref), out_refs = list(refs[:n]), refs[n : n + 2], refs[n + 2 : n + 6]
    w_ref, mixed_ref, low_ref, hold_ref, sems = refs[n + 6 :]
    groups = 7 * w_ref.shape[1]
    core = where_ref[0]
    copies = []
    for i, (ref, side) in enumerate(((own_ref, core), (other_ref, 1 - core))):
        at = pl.ds(pl.multiple_of(256 * side, 256), 256)
        copies.append(pltpu.make_async_copy(ref.at[pl.ds(0, 256)], mixed_ref.at[at], sems.at[i]))
        copies.append(pltpu.make_async_copy(ref.at[pl.ds(256, 16)], low_ref.at[side], sems.at[2 + i]))
    loads, used = [], 4
    for d, of in enumerate(plan):
        at, group = 0, []
        for count in of:
            place = w_ref.at[d, pl.ds(at, count)]
            group.append(pltpu.make_async_copy(pieces.pop(0), place, sems.at[used]))
            at, used = at + count, used + 1
        loads.append(group)
    for group in [copies] + loads:
        for copy in group:
            copy.start()
    for copy in copies:
        copy.wait()
    low = [low_ref[i, :, 0:256].astype(F32).reshape(2, 8, 256) for i in range(2)]
    low = jnp.concatenate(low, axis=2).astype(BF16)
    for d in range(4):
        for copy in loads[d]:
            copy.wait()
        w = w_ref[d].astype(F32).reshape(8 * groups, 896).astype(BF16)
        got = lax.dot_general(w, mixed_ref[...], NT, preferred_element_type=F32)
        at = where_ref[1 + d]
        hold_ref[at, 0:groups] = got.reshape(groups, 8, 512).astype(BF16)
        hold_ref[at, groups : groups + 2] = low
    outs = [pltpu.make_async_copy(hold_ref.at[j], out_refs[j], sems.at[used + j]) for j in range(4)]
    for copy in outs:
        copy.start()
    for copy in outs:
        copy.wait()


def error_kernel(core_ref, *refs):
    recv_refs, (right_ref, target_ref, so_far_ref, err_ref) = refs[:4], refs[4:]
    groups = recv_refs[0].shape[0] - 2
    feats = groups * 8
    total = low = 0.0
    for ref in recv_refs:
        total = total + ref[0:groups].astype(F32)
        low = low + ref[groups : groups + 2].astype(F32)
    tile = (iota((8, 512), 0) == (iota((8, 512), 1) & 7)).astype(BF16)
    target = lax.dot_general(target_ref[...], tile, TN, preferred_element_type=F32)
    total = total.reshape(feats, 512) - target
    low = low[0] + low[1]
    low = pltpu.roll(low, 4, 0) + low
    low = jnp.broadcast_to(low[None], (32, 8, 512)).reshape(256, 512)
    r, c = iota((256, 512), 0), iota((256, 512), 1)
    mine = ((r >> 3) == ((c & 255) >> 3)) & (((r & 7) >> 2) == ((c >> 8) ^ core_ref[0]))
    low = jnp.where(mine, low, 0.0)
    right = right_ref[...]
    for _ in range(3):
        piece = low.astype(BF16)
        total = total + lax.dot_general(right, piece, TN, preferred_element_type=F32)
        low = low - piece.astype(F32)
    err = jnp.sum((total * total).reshape(groups, 8, 512), axis=0)
    err = jnp.sum(err, axis=0, keepdims=True) + so_far_ref[0]
    err_ref[...] = jnp.broadcast_to(err[None], (4, 1, 512))


def final_kernel(where_ref, err_ref, left_ref, own_ref, other_ref, query_ref, out_ref, fit_ref):
    core, chip = where_ref[0], where_ref[1]
    err = jnp.sum(err_ref[...], axis=0)
    at = iota((256, 512), 1)
    row = iota((256, 512), 0)
    member = ((at & 255) >> 3) * 2 + (at >> 8)
    mine = 2 * (row >> 3) + (((row & 7) >> 2) ^ core)
    err = jnp.where(member == mine, jnp.broadcast_to(err, (256, 512)), 0.0)
    fit = -(jnp.sum(err, axis=1, keepdims=True) / (256 * D))
    mean = jnp.sum(fit, axis=0, keepdims=True) / 256
    away = fit - mean
    spread = jnp.sum(away * away, axis=0, keepdims=True) / 256
    weight = away / jnp.sqrt(spread + spread_floor)
    me = iota((256, 128), 0) == 8 * chip
    fit_ref[...] = jnp.sum(jnp.where(me, jnp.broadcast_to(fit, (256, 128)), 0.0), axis=0, keepdims=True)
    left = left_ref[...].astype(F32).reshape(256, 128) * weight
    left = left.reshape(32, 8, 128)
    turned = pltpu.roll(left, 4, 1)
    low, high = left, turned
    upper, narrow = iota((32, 8, 128), 1) < 4, iota((32, 8, 128), 2) < 64
    total = 0.0
    for ref, a, b in ((own_ref, low, high), (other_ref, high, low)):
        l = jnp.where(narrow, jnp.where(upper, a, 0.0), jnp.where(upper, 0.0, b)).reshape(256, 128)
        parts = []
        for _ in range(3):
            parts.append(l.astype(BF16))
            l = l - parts[-1].astype(F32)
        right = ref[...].astype(F32).reshape(256, 896).astype(BF16)
        g = lax.dot_general(jnp.concatenate(parts, axis=1), right, TN, preferred_element_type=F32)
        total = total + g[0:128] + g[128:256] + g[256:384]
    query_ref[...] = total[0:56]
    out_ref[...] = total[64:120]


def loaded(kernel, smem, n_in, n_out):
    def body(*refs):
        scalars, refs = refs[:smem], refs[smem:]
        ins, outs, refs = refs[:n_in], refs[n_in : n_in + n_out], refs[n_in + n_out :]
        held, results, refs = refs[:n_in], refs[n_in : n_in + n_out], refs[n_in + n_out :]
        *rest, sems = refs
        copies = [pltpu.make_async_copy(a, b, sems.at[i]) for i, (a, b) in enumerate(zip(ins, held))]
        for copy in copies:
            copy.start()
        for copy in copies:
            copy.wait()
        kernel(*scalars, *held, *results, *rest)
        copies = [pltpu.make_async_copy(b, a, sems.at[n_in + i]) for i, (a, b) in enumerate(zip(outs, results))]
        for copy in copies:
            copy.start()
        for copy in copies:
            copy.wait()

    return body


def call(kernel, out, args, smem=0, flops=10**9, scratch=(), load=True):
    outs = out if isinstance(out, (list, tuple)) else [out]
    ins = args[smem:]
    scratch = list(scratch)
    if load:
        kernel = loaded(kernel, smem, len(ins), len(outs))
        scratch = [pltpu.VMEM(a.shape, a.dtype) for a in (*ins, *outs)] + scratch
        scratch.append(pltpu.SemaphoreType.DMA((len(ins) + len(outs),)))
    hbm = pl.BlockSpec(memory_space=pltpu.HBM)
    return pl.pallas_call(
        kernel,
        out_shape=out,
        in_specs=[pl.BlockSpec(memory_space=pltpu.SMEM)] * smem + [hbm] * len(ins),
        out_specs=jax.tree.map(lambda _: hbm, out),
        scratch_shapes=scratch,
        cost_estimate=pl.CostEstimate(flops=flops, bytes_accessed=2 * 10**6, transcendentals=0),
    )(*args)


def shape(s, t=BF16):
    return jax.ShapeDtypeStruct(s, t)


def after(x, y):
    return lax.optimization_barrier((x, y))[0]


def ints(*values):
    return jnp.stack([jnp.asarray(v, jnp.int32) for v in values])


GROUPS = ((0, 1, 7, 2, 6), (3, 5, 4))
VIA_UP = (2, 1)


def per_device(
    tokens,
    target,
    w_query,
    w_key,
    w_value,
    w_out,
    query_left_factors,
    query_right_factors,
    o_left,
    o_right,
    member_ids,
):
    tok = tokens.shape[0]
    feats = w_query.shape[1]
    heads = feats // HEAD_DIM
    x, z, c = (lax.axis_index(a) for a in POP)
    y = lax.axis_index("mp")
    k = x * 8 + z
    p = 2 * k + c
    odd = member_ids[0] % 2
    half = jnp.where(odd == 0, 0.5, -0.5).astype(BF16)
    twice = jnp.where(odd == 0, 2.0, -2.0).astype(BF16)
    left_t = query_left_factors[0].T

    sent = call(
        front_kernel,
        shape((32, 8, 1920)),
        (ints(p, odd), tokens, w_query, left_t, query_right_factors[0], o_left[0].T),
        smem=1,
        scratch=[pltpu.VMEM((256, feats), F32)],
    )
    recv = lax.all_to_all(sent, CHIPS, 0, 0, tiled=True)

    w_t, parts = after(w_out.T, sent), []
    z1, z7, z2, z6, z3, z5, z4 = [shift(w_t, "pop_1", 8, e) for e in (1, 7, 2, 6, 3, 5, 4)]
    o1, o3, o2 = [shift(w_t, "pop_0", 4, d)[None] for d in (1, 3, 2)]
    for i, ins in enumerate(([z1, z7, z2, z6], [z3, z5, z4])):
        n, via = len(ins), VIA_UP[i]
        own = call(stack_kernel, shape((n, 56, feats)), ins)
        up, down = shift(own, "pop_0", 4, 1), shift(own, "pop_0", 4, 3)
        far = [shift(up[:via], "pop_0", 4, 1), shift(down[via:], "pop_0", 4, 3)]
        if i == 0:
            parts.append([[w_t[None], own], [o1, up], [o3, down], [o2, *far]])
        else:
            parts.append([[own], [up], [down], far])
    where = ints(c, *[(x + d - y) % 4 for d in (0, -1, 1, 2)])

    cos_all, sin_all = tables(jnp.arange(tok, dtype=F32), HEAD_DIM)
    k32 = jnp.dot(tokens, w_key, preferred_element_type=F32)
    keys = (k32 * cos_all + jnp.roll(k32, 64, axis=1) * sin_all).astype(BF16)
    values = jnp.dot(tokens, w_value, preferred_element_type=F32).astype(BF16)
    cos8, sin8 = tables((k * 8).astype(F32) + jnp.arange(8, dtype=F32), HEAD_DIM)

    half_base = jnp.sum(recv[:, :, :feats].astype(F32), axis=0)
    mixed = call(
        functools.partial(attention_kernel, heads),
        shape((272, feats)),
        (ints(k * 8), recv, half_base, swap(half_base), keys, values, cos8, sin8),
        smem=1,
    )
    mixed_b = swap(mixed)

    outs = []
    for group, pieces in zip(GROUPS, parts):
        outs.append(
            call(
                functools.partial(project_kernel, [[a.shape[0] for a in of] for of in pieces]),
                [shape((7 * len(group) + 2, 8, 512))] * 4,
                (where, *sum(pieces, []), mixed, mixed_b),
                smem=1,
                scratch=[
                    pltpu.VMEM((4, len(group), 56, feats), BF16),
                    pltpu.VMEM((512, feats), BF16),
                    pltpu.VMEM((2, 16, feats), BF16),
                    pltpu.VMEM((4, 7 * len(group) + 2, 8, 512), BF16),
                    pltpu.SemaphoreType.DMA((17,)),
                ],
                load=False,
            )
        )
    mets = []
    for out in outs:
        mets.append([out[0]] + [shift(out[s], "mp", 4, s) for s in (2, 1, 3)])

    order = jnp.array([e for group in GROUPS for e in group])
    which = (jnp.arange(8)[:, None] - order[None]) % 8
    o_r = after(o_right[0], sent)
    o_cut = lax.dynamic_slice(o_r, (0, feats * y), (RANK, feats)).reshape(RANK, 8, 2, 56) * half
    one = (which[:, :, None] == jnp.arange(8)).astype(BF16)
    o_cut = jnp.einsum("kiz,rzcf->kcrif", one, o_cut, preferred_element_type=F32).astype(BF16)
    o_cut = jnp.where(c == 0, o_cut, o_cut[:, ::-1]).reshape(1, 8, 8, 448)
    o_cut = jnp.broadcast_to(o_cut, (4, 8, 8, 448)).reshape(32, 8, 448)

    def cut(a):
        a = jnp.moveaxis((a * twice).reshape(RANK, 32, 2, 56), 0, 2)
        return jnp.where(c == 0, a, a[:, ::-1]).reshape(32, 8, 56)

    gap = jnp.zeros((32, 8, 8), BF16)
    late = [cut(after(left_t, sent)), gap, cut(o_r), gap, o_cut, jnp.zeros((32, 8, 64), BF16)]
    late = jnp.concatenate(late, axis=2)
    late = lax.all_to_all(late, CHIPS, 0, 0, tiled=True)
    late_b = swap(late[:, 4:])
    late = jnp.concatenate([late[:, :4], late_b], axis=1)
    factors = after(recv, outs[0][0])[:, :, 1024:1920]
    factors_b = swap(factors)
    lefts = late[:, :, :128]
    goal = lax.dynamic_slice(target, (8 * k, 0), (8, feats)).reshape(8, 8, 2, 56)
    goal = jnp.where(c == 0, goal[:, :, 0], goal[:, :, 1])
    here = (((z - order) % 8)[:, None] == jnp.arange(8)).astype(BF16)
    goal = jnp.einsum("iz,tzf->tif", here, goal, preferred_element_type=F32).astype(BF16).reshape(8, 448)
    err = jnp.zeros((4, 1, 512), F32)
    start = 128
    for group, met in zip(GROUPS, mets):
        n = 56 * len(group)
        right = late[:, :, start : start + n].reshape(256, n)
        part = goal[:, start - 128 : start - 128 + n]
        start += n
        err = call(error_kernel, shape((4, 1, 512), F32), (ints(c), *met, right, part, err), smem=1)

    err = lax.all_to_all(err, "mp", 0, 0, tiled=True)
    err = jnp.sum(err, axis=0, keepdims=True)
    err = lax.all_to_all(jnp.broadcast_to(err, (64, 1, 512)), POP, 0, 0, tiled=True)
    grad_query, grad_out, fitness = call(
        final_kernel,
        [shape((56, feats), F32), shape((56, feats), F32), shape((1, 128), F32)],
        (ints(c, k), err, lefts, factors, factors_b),
        smem=1,
    )
    return (grad_query, grad_out.T, fitness[0, :1])


def solution(mesh):
    torus = Mesh(mesh.devices.reshape(4, 8, 2, mesh.shape["mp"]), ("pop_0", "pop_1", "pop_2", "mp"))
    placed = (
        P(),
        P(None, "mp"),
        P(POP, "mp"),
        P(None, "mp"),
        P(None, "mp"),
        P("mp", POP),
        P(POP, None, None),
        P(POP, None, "mp"),
        P(POP, "mp", None),
        P(POP, None, None),
        P(POP),
    )
    return jax.shard_map(
        per_device,
        mesh=torus,
        in_specs=placed,
        out_specs=(P(POP, "mp"), P("mp", POP), P(POP)),
        check_vma=False,
    )
```

```python
import functools
import math

import jax
import jax.numpy as jnp
from jax import lax
from jax.experimental import pallas as pl
from jax.experimental.pallas import tpu as pltpu
from jax.sharding import Mesh
from jax.sharding import PartitionSpec as P

D = 3584
HEAD_DIM = 128
RANK = 4
POP = ("pop_0", "pop_1", "pop_2")
CHIPS = ("pop_0", "pop_1")

rope_base = 1000000.0
spread_floor = 0.001

F32 = jnp.float32
BF16 = jnp.bfloat16
NT = (((1,), (1,)), ((), ()))
TN = (((0,), (0,)), ((), ()))


def iota(shape, dim):
    return lax.broadcasted_iota(jnp.int32, shape, dim)


def shift(x, axis, size, step):
    return lax.ppermute(x, axis, [(i, (i + step) % size) for i in range(size)])


def swap(x):
    return lax.ppermute(x, "pop_2", [(0, 1), (1, 0)])


def tables(position, head_size):
    index = jnp.arange(head_size // 2, dtype=F32)
    freq = jnp.exp(-math.log(rope_base) * 2.0 * index / head_size)
    angle = position[:, None] * freq[None, :]
    c, s = jnp.cos(angle), jnp.sin(angle)
    return jnp.concatenate([c, c], axis=-1), jnp.concatenate([-s, s], axis=-1)


def front_kernel(where_ref, tokens_ref, w_ref, left_ref, right_ref, o_ref, out_ref, pad_ref):
    p = where_ref[0]
    start = pl.multiple_of(jnp.minimum((56 * p) // 128 * 128, 3584 - 256), 128)
    at = pl.multiple_of(56 * p - start, 8)
    pad_ref[...] = jnp.zeros_like(pad_ref)
    pad_ref[pl.ds(at, 56), :] = w_ref[...].astype(F32)
    window = tokens_ref[:, pl.ds(start, 256)]
    share = jnp.dot(window, pad_ref[...].astype(BF16), preferred_element_type=F32)
    out_ref[:, :, 0:896] = share.reshape(32, 8, 896).astype(BF16)
    left = left_ref[...].astype(F32)
    left = jnp.concatenate([left, jnp.zeros_like(left)], axis=0).astype(BF16)
    low = lax.dot_general(tokens_ref[...], left, NT, preferred_element_type=F32)
    low = low.astype(BF16).astype(F32) * jnp.where(where_ref[1] == 0, 0.5, -0.5)
    out_ref[:, :, 896:1024] = jnp.zeros((32, 8, 128), BF16)
    out_ref[:, :, 896:904] = low.reshape(32, 8, 8).astype(BF16)
    both = jnp.concatenate([right_ref[...].astype(F32), o_ref[...].astype(F32)], axis=0)
    out_ref[:, :, 1024:1920] = jnp.broadcast_to(both[None], (32, 8, 896)).astype(BF16)


def attention_kernel(heads, where_ref, recv_ref, base_ref, other_ref, keys_ref, values_ref, cos_ref, sin_ref, mixed_ref):
    tok = keys_ref.shape[0]
    rows = 256
    scale = HEAD_DIM ** (-0.5)
    factors = recv_ref[:, :, 1024:1920].astype(F32).reshape(rows, 896).astype(BF16)
    small = recv_ref[:, :, 896:1024].astype(F32).reshape(rows, 128).astype(BF16)
    lane = iota((128, rows), 1)
    pick = (iota((128, rows), 0) == (lane & 3)).astype(BF16)
    spread = jnp.dot(small, pick, preferred_element_type=F32)
    r, c = iota((rows, rows), 0), iota((rows, rows), 1)
    mine = (r >> 3) == (c >> 3)
    left = jnp.where(mine & ((c & 7) < 4), spread, 0.0).astype(BF16)
    low = jnp.dot(left, factors, preferred_element_type=F32)
    cos = jnp.broadcast_to(cos_ref[...][None], (rows // 8, 8, 128)).reshape(rows, 128)
    sin = jnp.broadcast_to(sin_ref[...][None], (rows // 8, 8, 128)).reshape(rows, 128)
    keys, values = keys_ref[...], values_ref[...]
    seen = (iota((rows, tok), 0) & 7) + where_ref[0] >= iota((rows, tok), 1)
    for h in range(heads):
        at = slice(h * 128, (h + 1) * 128)
        base = base_ref[:, at] + other_ref[:, at]
        q = jnp.broadcast_to(base[None], (rows // 8, 8, 128)).reshape(rows, 128) + low[:, at]
        q = (q * cos + pltpu.roll(q, 64, 1) * sin).astype(BF16)
        s = lax.dot_general(q, keys, NT, preferred_element_type=F32) * scale
        s = jnp.where(seen, s, -1e30)
        e = jnp.exp(s - jnp.max(s, axis=1, keepdims=True))
        p = (e / jnp.sum(e, axis=1, keepdims=True)).astype(BF16)
        mixed_ref[0:256, at] = jnp.dot(p, values, preferred_element_type=F32).astype(BF16)
    d = lax.dot_general(factors, mixed_ref[0:256, :], NT, preferred_element_type=F32)
    d = jnp.where(mine & ((r & 7) >= 4), d, 0.0).reshape(rows // 8, 8, rows)
    d = jnp.sum(d, axis=0)
    hi = d.astype(BF16).astype(F32)
    mixed_ref[256:272, :] = jnp.zeros((16, 896), BF16)
    mixed_ref[256:272, 0:256] = jnp.concatenate([hi, d - hi], axis=0).astype(BF16)


def project_kernel(plan, where_ref, *refs):
    n = sum(len(of) for of in plan)
    pieces, (own_ref, other_ref), out_refs = list(refs[:n]), refs[n : n + 2], refs[n + 2 : n + 6]
    w_ref, mixed_ref, low_ref, hold_ref, sems = refs[n + 6 :]
    groups = 7 * w_ref.shape[1]
    core = where_ref[0]
    copies = []
    for i, (ref, side) in enumerate(((own_ref, core), (other_ref, 1 - core))):
        at = pl.ds(pl.multiple_of(256 * side, 256), 256)
        copies.append(pltpu.make_async_copy(ref.at[pl.ds(0, 256)], mixed_ref.at[at], sems.at[i]))
        copies.append(pltpu.make_async_copy(ref.at[pl.ds(256, 16)], low_ref.at[side], sems.at[2 + i]))
    loads, used = [], 4
    for d, of in enumerate(plan):
        at, group = 0, []
        for count in of:
            place = w_ref.at[d, pl.ds(at, count)]
            group.append(pltpu.make_async_copy(pieces.pop(0), place, sems.at[used]))
            at, used = at + count, used + 1
        loads.append(group)
    for group in [copies] + loads:
        for copy in group:
            copy.start()
    for copy in copies:
        copy.wait()
    low = [low_ref[i, :, 0:256].astype(F32).reshape(2, 8, 256) for i in range(2)]
    low = jnp.concatenate(low, axis=2).astype(BF16)
    for d in range(4):
        for copy in loads[d]:
            copy.wait()
        w = w_ref[d].astype(F32).reshape(8 * groups, 896).astype(BF16)
        got = lax.dot_general(w, mixed_ref[...], NT, preferred_element_type=F32)
        at = where_ref[1 + d]
        hold_ref[at, 0:groups] = got.reshape(groups, 8, 512).astype(BF16)
        hold_ref[at, groups : groups + 2] = low
    outs = [pltpu.make_async_copy(hold_ref.at[j], out_refs[j], sems.at[used + j]) for j in range(4)]
    for copy in outs:
        copy.start()
    for copy in outs:
        copy.wait()


def error_kernel(core_ref, *refs):
    recv_refs, (right_ref, target_ref, so_far_ref, err_ref) = refs[:4], refs[4:]
    groups = recv_refs[0].shape[0] - 2
    feats = groups * 8
    total = low = 0.0
    for ref in recv_refs:
        total = total + ref[0:groups].astype(F32)
        low = low + ref[groups : groups + 2].astype(F32)
    tile = (iota((8, 512), 0) == (iota((8, 512), 1) & 7)).astype(BF16)
    target = lax.dot_general(target_ref[...], tile, TN, preferred_element_type=F32)
    total = total.reshape(feats, 512) - target
    low = low[0] + low[1]
    low = pltpu.roll(low, 4, 0) + low
    low = jnp.broadcast_to(low[None], (32, 8, 512)).reshape(256, 512)
    r, c = iota((256, 512), 0), iota((256, 512), 1)
    mine = ((r >> 3) == ((c & 255) >> 3)) & (((r & 7) >> 2) == ((c >> 8) ^ core_ref[0]))
    low = jnp.where(mine, low, 0.0)
    right = right_ref[...]
    for _ in range(3):
        piece = low.astype(BF16)
        total = total + lax.dot_general(right, piece, TN, preferred_element_type=F32)
        low = low - piece.astype(F32)
    err = jnp.sum((total * total).reshape(groups, 8, 512), axis=0)
    err = jnp.sum(err, axis=0, keepdims=True) + so_far_ref[0]
    err_ref[...] = jnp.broadcast_to(err[None], (32, 1, 512))


def final_kernel(where_ref, err_ref, left_ref, own_ref, other_ref, query_ref, out_ref, fit_ref):
    core, chip = where_ref[0], where_ref[1]
    err = jnp.sum(err_ref[...], axis=0)
    at = iota((256, 512), 1)
    row = iota((256, 512), 0)
    member = ((at & 255) >> 3) * 2 + (at >> 8)
    mine = 2 * (row >> 3) + (((row & 7) >> 2) ^ core)
    err = jnp.where(member == mine, jnp.broadcast_to(err, (256, 512)), 0.0)
    fit = -(jnp.sum(err, axis=1, keepdims=True) / (256 * D))
    mean = jnp.sum(fit, axis=0, keepdims=True) / 256
    away = fit - mean
    spread = jnp.sum(away * away, axis=0, keepdims=True) / 256
    weight = away / jnp.sqrt(spread + spread_floor)
    me = iota((256, 128), 0) == 8 * chip
    fit_ref[...] = jnp.sum(jnp.where(me, jnp.broadcast_to(fit, (256, 128)), 0.0), axis=0, keepdims=True)
    left = left_ref[...].astype(F32).reshape(256, 128) * weight
    left = left.reshape(32, 8, 128)
    turned = pltpu.roll(left, 4, 1)
    low, high = left, turned
    upper, narrow = iota((32, 8, 128), 1) < 4, iota((32, 8, 128), 2) < 64
    total = 0.0
    for ref, a, b in ((own_ref, low, high), (other_ref, high, low)):
        l = jnp.where(narrow, jnp.where(upper, a, 0.0), jnp.where(upper, 0.0, b)).reshape(256, 128)
        parts = []
        for _ in range(3):
            parts.append(l.astype(BF16))
            l = l - parts[-1].astype(F32)
        right = ref[...].astype(F32).reshape(256, 896).astype(BF16)
        g = lax.dot_general(jnp.concatenate(parts, axis=1), right, TN, preferred_element_type=F32)
        total = total + g[0:128] + g[128:256] + g[256:384]
    query_ref[...] = total[0:56]
    out_ref[...] = total[64:120]


def loaded(kernel, smem, n_in, n_out):
    def body(*refs):
        scalars, refs = refs[:smem], refs[smem:]
        ins, outs, refs = refs[:n_in], refs[n_in : n_in + n_out], refs[n_in + n_out :]
        held, results, refs = refs[:n_in], refs[n_in : n_in + n_out], refs[n_in + n_out :]
        *rest, sems = refs
        copies = [pltpu.make_async_copy(a, b, sems.at[i]) for i, (a, b) in enumerate(zip(ins, held))]
        for copy in copies:
            copy.start()
        for copy in copies:
            copy.wait()
        kernel(*scalars, *held, *results, *rest)
        copies = [pltpu.make_async_copy(b, a, sems.at[n_in + i]) for i, (a, b) in enumerate(zip(outs, results))]
        for copy in copies:
            copy.start()
        for copy in copies:
            copy.wait()

    return body


def call(kernel, out, args, smem=0, flops=10**9, scratch=(), load=True):
    outs = out if isinstance(out, (list, tuple)) else [out]
    ins = args[smem:]
    scratch = list(scratch)
    if load:
        kernel = loaded(kernel, smem, len(ins), len(outs))
        scratch = [pltpu.VMEM(a.shape, a.dtype) for a in (*ins, *outs)] + scratch
        scratch.append(pltpu.SemaphoreType.DMA((len(ins) + len(outs),)))
    hbm = pl.BlockSpec(memory_space=pltpu.HBM)
    return pl.pallas_call(
        kernel,
        out_shape=out,
        in_specs=[pl.BlockSpec(memory_space=pltpu.SMEM)] * smem + [hbm] * len(ins),
        out_specs=jax.tree.map(lambda _: hbm, out),
        scratch_shapes=scratch,
        cost_estimate=pl.CostEstimate(flops=flops, bytes_accessed=2 * 10**6, transcendentals=0),
    )(*args)


def shape(s, t=BF16):
    return jax.ShapeDtypeStruct(s, t)


def after(x, y):
    return lax.optimization_barrier((x, y))[0]


def ints(*values):
    return jnp.stack([jnp.asarray(v, jnp.int32) for v in values])


GROUPS = ((0, 1, 7, 2, 6), (3, 5, 4))
VIA_UP = (2, 1)


def per_device(
    tokens,
    target,
    w_query,
    w_key,
    w_value,
    w_out,
    query_left_factors,
    query_right_factors,
    o_left,
    o_right,
    member_ids,
):
    tok = tokens.shape[0]
    feats = w_query.shape[1]
    heads = feats // HEAD_DIM
    x, z, c = (lax.axis_index(a) for a in POP)
    y = lax.axis_index("mp")
    k = x * 8 + z
    p = 2 * k + c
    odd = member_ids[0] % 2
    half = jnp.where(odd == 0, 0.5, -0.5).astype(BF16)
    twice = jnp.where(odd == 0, 2.0, -2.0).astype(BF16)
    left_t = query_left_factors[0].T

    sent = call(
        front_kernel,
        shape((32, 8, 1920)),
        (ints(p, odd), tokens, w_query, left_t, query_right_factors[0], o_left[0].T),
        smem=1,
        scratch=[pltpu.VMEM((256, feats), F32)],
    )
    recv = lax.all_to_all(sent, CHIPS, 0, 0, tiled=True)

    w_t, parts = after(w_out.T, sent), []
    z1, z7, z2, z6, z3, z5, z4 = [shift(w_t, "pop_1", 8, e) for e in (1, 7, 2, 6, 3, 5, 4)]
    o1, o3, o2 = [shift(w_t, "pop_0", 4, d)[None] for d in (1, 3, 2)]
    for i, ins in enumerate(([z1, z7, z2, z6], [z3, z5, z4])):
        n, via = len(ins), VIA_UP[i]
        own = jnp.stack(ins)
        up, down = shift(own, "pop_0", 4, 1), shift(own, "pop_0", 4, 3)
        far = [shift(up[:via], "pop_0", 4, 1), shift(down[via:], "pop_0", 4, 3)]
        if i == 0:
            parts.append([[w_t[None], own], [o1, up], [o3, down], [o2, *far]])
        else:
            parts.append([[own], [up], [down], far])
    where = ints(c, *[(x + d - y) % 4 for d in (0, -1, 1, 2)])

    cos_all, sin_all = tables(jnp.arange(tok, dtype=F32), HEAD_DIM)
    k32 = jnp.dot(tokens, w_key, preferred_element_type=F32)
    keys = (k32 * cos_all + jnp.roll(k32, 64, axis=1) * sin_all).astype(BF16)
    values = jnp.dot(tokens, w_value, preferred_element_type=F32).astype(BF16)
    cos8, sin8 = tables((k * 8).astype(F32) + jnp.arange(8, dtype=F32), HEAD_DIM)

    half_base = jnp.sum(recv[:, :, :feats].astype(F32), axis=0)
    mixed = call(
        functools.partial(attention_kernel, heads),
        shape((272, feats)),
        (ints(k * 8), recv, half_base, swap(half_base), keys, values, cos8, sin8),
        smem=1,
    )
    mixed_b = swap(mixed)

    outs = []
    for group, pieces in zip(GROUPS, parts):
        outs.append(
            call(
                functools.partial(project_kernel, [[a.shape[0] for a in of] for of in pieces]),
                [shape((7 * len(group) + 2, 8, 512))] * 4,
                (where, *sum(pieces, []), mixed, mixed_b),
                smem=1,
                scratch=[
                    pltpu.VMEM((4, len(group), 56, feats), BF16),
                    pltpu.VMEM((512, feats), BF16),
                    pltpu.VMEM((2, 16, feats), BF16),
                    pltpu.VMEM((4, 7 * len(group) + 2, 8, 512), BF16),
                    pltpu.SemaphoreType.DMA((17,)),
                ],
                load=False,
            )
        )
    mets = []
    for out in outs:
        mets.append([out[0]] + [shift(out[s], "mp", 4, s) for s in (2, 1, 3)])

    order = jnp.array([e for group in GROUPS for e in group])
    which = (jnp.arange(8)[:, None] - order[None]) % 8
    o_r = after(o_right[0], sent)
    o_cut = lax.dynamic_slice(o_r, (0, feats * y), (RANK, feats)).reshape(RANK, 8, 2, 56) * half
    one = (which[:, :, None] == jnp.arange(8)).astype(BF16)
    o_cut = jnp.einsum("kiz,rzcf->kcrif", one, o_cut, preferred_element_type=F32).astype(BF16)
    o_cut = jnp.where(c == 0, o_cut, o_cut[:, ::-1]).reshape(1, 8, 8, 448)
    o_cut = jnp.broadcast_to(o_cut, (4, 8, 8, 448)).reshape(32, 8, 448)

    def cut(a):
        a = jnp.moveaxis((a * twice).reshape(RANK, 32, 2, 56), 0, 2)
        return jnp.where(c == 0, a, a[:, ::-1]).reshape(32, 8, 56)

    gap = jnp.zeros((32, 8, 8), BF16)
    late = [cut(after(left_t, sent)), gap, cut(o_r), gap, o_cut, jnp.zeros((32, 8, 64), BF16)]
    late = jnp.concatenate(late, axis=2)
    late = lax.all_to_all(late, CHIPS, 0, 0, tiled=True)
    late_b = swap(late[:, 4:])
    late = jnp.concatenate([late[:, :4], late_b], axis=1)
    factors = after(recv, outs[0][0])[:, :, 1024:1920]
    factors_b = swap(factors)
    lefts = late[:, :, :128]
    goal = lax.dynamic_slice(target, (8 * k, 0), (8, feats)).reshape(8, 8, 2, 56)
    goal = jnp.where(c == 0, goal[:, :, 0], goal[:, :, 1])
    here = (((z - order) % 8)[:, None] == jnp.arange(8)).astype(BF16)
    goal = jnp.einsum("iz,tzf->tif", here, goal, preferred_element_type=F32).astype(BF16).reshape(8, 448)
    err = jnp.zeros((32, 1, 512), F32)
    start = 128
    for group, met in zip(GROUPS, mets):
        n = 56 * len(group)
        right = late[:, :, start : start + n].reshape(256, n)
        part = goal[:, start - 128 : start - 128 + n]
        start += n
        err = call(error_kernel, shape((32, 1, 512), F32), (ints(c), *met, right, part, err), smem=1)

    err = lax.all_to_all(err, ("pop_0", "pop_2", "mp"), 0, 0, tiled=True)
    err = jnp.sum(err, axis=0, keepdims=True)
    err = lax.all_to_all(jnp.broadcast_to(err, (8, 1, 512)), "pop_1", 0, 0, tiled=True)
    grad_query, grad_out, fitness = call(
        final_kernel,
        [shape((56, feats), F32), shape((56, feats), F32), shape((1, 128), F32)],
        (ints(c, k), err, lefts, factors, factors_b),
        smem=1,
    )
    return (grad_query, grad_out.T, fitness[0, :1])


def solution(mesh):
    torus = Mesh(mesh.devices.reshape(4, 8, 2, mesh.shape["mp"]), ("pop_0", "pop_1", "pop_2", "mp"))
    placed = (
        P(),
        P(None, "mp"),
        P(POP, "mp"),
        P(None, "mp"),
        P(None, "mp"),
        P("mp", POP),
        P(POP, None, None),
        P(POP, None, "mp"),
        P(POP, "mp", None),
        P(POP, None, None),
        P(POP),
    )
    return jax.shard_map(
        per_device,
        mesh=torus,
        in_specs=placed,
        out_specs=(P(POP, "mp"), P("mp", POP), P(POP)),
        check_vma=False,
    )
```

```python
import functools
import math

import jax
import jax.numpy as jnp
from jax import lax
from jax.experimental import pallas as pl
from jax.experimental.pallas import tpu as pltpu
from jax.sharding import Mesh
from jax.sharding import PartitionSpec as P

D = 3584
HEAD_DIM = 128
RANK = 4
POP = ("pop_0", "pop_1", "pop_2")
CHIPS = ("pop_0", "pop_1")

rope_base = 1000000.0
spread_floor = 0.001

F32 = jnp.float32
BF16 = jnp.bfloat16
NT = (((1,), (1,)), ((), ()))
TN = (((0,), (0,)), ((), ()))


def iota(shape, dim):
    return lax.broadcasted_iota(jnp.int32, shape, dim)


def shift(x, axis, size, step):
    return lax.ppermute(x, axis, [(i, (i + step) % size) for i in range(size)])


def swap(x):
    return lax.ppermute(x, "pop_2", [(0, 1), (1, 0)])


def tables(position, head_size):
    index = jnp.arange(head_size // 2, dtype=F32)
    freq = jnp.exp(-math.log(rope_base) * 2.0 * index / head_size)
    angle = position[:, None] * freq[None, :]
    c, s = jnp.cos(angle), jnp.sin(angle)
    return jnp.concatenate([c, c], axis=-1), jnp.concatenate([-s, s], axis=-1)


def front_kernel(where_ref, tokens_ref, w_ref, left_ref, right_ref, o_ref, out_ref, pad_ref):
    p = where_ref[0]
    start = pl.multiple_of(jnp.minimum((56 * p) // 128 * 128, 3584 - 256), 128)
    at = pl.multiple_of(56 * p - start, 8)
    pad_ref[...] = jnp.zeros_like(pad_ref)
    pad_ref[pl.ds(at, 56), :] = w_ref[...].astype(F32)
    window = tokens_ref[:, pl.ds(start, 256)]
    share = jnp.dot(window, pad_ref[...].astype(BF16), preferred_element_type=F32)
    out_ref[:, :, 0:896] = share.reshape(32, 8, 896).astype(BF16)
    left = left_ref[...].astype(F32)
    left = jnp.concatenate([left, jnp.zeros_like(left)], axis=0).astype(BF16)
    low = lax.dot_general(tokens_ref[...], left, NT, preferred_element_type=F32)
    low = low.astype(BF16).astype(F32) * jnp.where(where_ref[1] == 0, 0.5, -0.5)
    out_ref[:, :, 896:1024] = jnp.zeros((32, 8, 128), BF16)
    out_ref[:, :, 896:904] = low.reshape(32, 8, 8).astype(BF16)
    both = jnp.concatenate([right_ref[...].astype(F32), o_ref[...].astype(F32)], axis=0)
    out_ref[:, :, 1024:1920] = jnp.broadcast_to(both[None], (32, 8, 896)).astype(BF16)


def attention_kernel(heads, where_ref, recv_ref, base_ref, other_ref, keys_ref, values_ref, cos_ref, sin_ref, mixed_ref):
    tok = keys_ref.shape[0]
    rows = 256
    scale = HEAD_DIM ** (-0.5)
    factors = recv_ref[:, :, 1024:1920].astype(F32).reshape(rows, 896).astype(BF16)
    small = recv_ref[:, :, 896:1024].astype(F32).reshape(rows, 128).astype(BF16)
    lane = iota((128, rows), 1)
    pick = (iota((128, rows), 0) == (lane & 3)).astype(BF16)
    spread = jnp.dot(small, pick, preferred_element_type=F32)
    r, c = iota((rows, rows), 0), iota((rows, rows), 1)
    mine = (r >> 3) == (c >> 3)
    left = jnp.where(mine & ((c & 7) < 4), spread, 0.0).astype(BF16)
    low = jnp.dot(left, factors, preferred_element_type=F32)
    cos = jnp.broadcast_to(cos_ref[...][None], (rows // 8, 8, 128)).reshape(rows, 128)
    sin = jnp.broadcast_to(sin_ref[...][None], (rows // 8, 8, 128)).reshape(rows, 128)
    keys, values = keys_ref[...], values_ref[...]
    seen = (iota((rows, tok), 0) & 7) + where_ref[0] >= iota((rows, tok), 1)
    for h in range(heads):
        at = slice(h * 128, (h + 1) * 128)
        base = base_ref[:, at] + other_ref[:, at]
        q = jnp.broadcast_to(base[None], (rows // 8, 8, 128)).reshape(rows, 128) + low[:, at]
        q = (q * cos + pltpu.roll(q, 64, 1) * sin).astype(BF16)
        s = lax.dot_general(q, keys, NT, preferred_element_type=F32) * scale
        s = jnp.where(seen, s, -1e30)
        e = jnp.exp(s - jnp.max(s, axis=1, keepdims=True))
        p = (e / jnp.sum(e, axis=1, keepdims=True)).astype(BF16)
        mixed_ref[0:256, at] = jnp.dot(p, values, preferred_element_type=F32).astype(BF16)
    d = lax.dot_general(factors, mixed_ref[0:256, :], NT, preferred_element_type=F32)
    d = jnp.where(mine & ((r & 7) >= 4), d, 0.0).reshape(rows // 8, 8, rows)
    d = jnp.sum(d, axis=0)
    hi = d.astype(BF16).astype(F32)
    mixed_ref[256:272, :] = jnp.zeros((16, 896), BF16)
    mixed_ref[256:272, 0:256] = jnp.concatenate([hi, d - hi], axis=0).astype(BF16)


def project_kernel(plan, where_ref, *refs):
    n = sum(len(of) for of in plan)
    pieces, (own_ref, other_ref), out_refs = list(refs[:n]), refs[n : n + 2], refs[n + 2 : n + 6]
    w_ref, mixed_ref, low_ref, hold_ref, sems = refs[n + 6 :]
    groups = 7 * w_ref.shape[1]
    has_low = hold_ref.shape[1] > groups
    core = where_ref[0]
    copies = []
    for i, (ref, side) in enumerate(((own_ref, core), (other_ref, 1 - core))):
        at = pl.ds(pl.multiple_of(256 * side, 256), 256)
        copies.append(pltpu.make_async_copy(ref.at[pl.ds(0, 256)], mixed_ref.at[at], sems.at[i]))
        copies.append(pltpu.make_async_copy(ref.at[pl.ds(256, 16)], low_ref.at[side], sems.at[2 + i]))
    loads, used = [], 4
    for d, of in enumerate(plan):
        at, group = 0, []
        for count in of:
            place = w_ref.at[d, pl.ds(at, count)]
            group.append(pltpu.make_async_copy(pieces.pop(0), place, sems.at[used]))
            at, used = at + count, used + 1
        loads.append(group)
    for group in [copies] + loads:
        for copy in group:
            copy.start()
    for copy in copies:
        copy.wait()
    low = [low_ref[i, :, 0:256].astype(F32).reshape(2, 8, 256) for i in range(2)]
    low = jnp.concatenate(low, axis=2).astype(BF16)
    for d in range(4):
        for copy in loads[d]:
            copy.wait()
        w = w_ref[d].astype(F32).reshape(8 * groups, 896).astype(BF16)
        got = lax.dot_general(w, mixed_ref[...], NT, preferred_element_type=F32)
        at = where_ref[1 + d]
        hold_ref[at, 0:groups] = got.reshape(groups, 8, 512).astype(BF16)
        if has_low:
            hold_ref[at, groups : groups + 2] = low
    outs = [pltpu.make_async_copy(hold_ref.at[j], out_refs[j], sems.at[used + j]) for j in range(4)]
    for copy in outs:
        copy.start()
    for copy in outs:
        copy.wait()


def error_kernel(core_ref, *refs):
    recv_refs, (right_a, target_a, right_b, target_b, err_ref, rest_ref) = refs[:4], refs[4:]
    groups = recv_refs[0].shape[0] - 2
    total = low = 0.0
    for ref in recv_refs:
        total = total + ref[0:groups].astype(F32)
        low = low + ref[groups : groups + 2].astype(F32)
    low = low[0] + low[1]
    low = pltpu.roll(low, 4, 0) + low
    low = jnp.broadcast_to(low[None], (32, 8, 512)).reshape(256, 512)
    r, c = iota((256, 512), 0), iota((256, 512), 1)
    mine = ((r >> 3) == ((c & 255) >> 3)) & (((r & 7) >> 2) == ((c >> 8) ^ core_ref[0]))
    low = jnp.where(mine, low, 0.0)
    pieces = []
    for _ in range(3):
        pieces.append(low.astype(BF16))
        low = low - pieces[-1].astype(F32)
    tile = (iota((8, 512), 0) == (iota((8, 512), 1) & 7)).astype(BF16)

    def without_target(right_ref, target_ref):
        away = -lax.dot_general(target_ref[...], tile, TN, preferred_element_type=F32)
        for piece in pieces:
            away = away + lax.dot_general(right_ref[...], piece, TN, preferred_element_type=F32)
        return away

    total = total.reshape(8 * groups, 512) + without_target(right_a, target_a)
    err = jnp.sum((total * total).reshape(groups, 8, 512), axis=0)
    err_ref[...] = err
    rest_ref[...] = without_target(right_b, target_b)


def last_error_kernel(*refs):
    recv_refs, (rest_ref, so_far_ref, err_ref) = refs[:4], refs[4:]
    groups = recv_refs[0].shape[0]
    total = 0.0
    for ref in recv_refs:
        total = total + ref[...].astype(F32)
    total = total + rest_ref[...].reshape(groups, 8, 512)
    err = jnp.sum(jnp.sum(total * total, axis=0) + so_far_ref[...], axis=0, keepdims=True)
    err_ref[...] = jnp.broadcast_to(err[None], (32, 1, 512))


def final_kernel(where_ref, err_ref, left_ref, own_copy, other_copy, query_ref, out_ref, fit_ref):
    core, chip = where_ref[0], where_ref[1]
    err = jnp.sum(err_ref[...], axis=0)
    at = iota((256, 512), 1)
    row = iota((256, 512), 0)
    member = ((at & 255) >> 3) * 2 + (at >> 8)
    mine = 2 * (row >> 3) + (((row & 7) >> 2) ^ core)
    err = jnp.where(member == mine, jnp.broadcast_to(err, (256, 512)), 0.0)
    fit = -(jnp.sum(err, axis=1, keepdims=True) / (256 * D))
    mean = jnp.sum(fit, axis=0, keepdims=True) / 256
    away = fit - mean
    spread = jnp.sum(away * away, axis=0, keepdims=True) / 256
    weight = away / jnp.sqrt(spread + spread_floor)
    me = iota((256, 128), 0) == 8 * chip
    fit_ref[...] = jnp.sum(jnp.where(me, jnp.broadcast_to(fit, (256, 128)), 0.0), axis=0, keepdims=True)
    left = left_ref[...].astype(F32).reshape(256, 128) * weight
    left = left.reshape(32, 8, 128)
    turned = pltpu.roll(left, 4, 1)
    low, high = left, turned
    upper, narrow = iota((32, 8, 128), 1) < 4, iota((32, 8, 128), 2) < 64
    total = 0.0
    for copy, a, b in ((own_copy, low, high), (other_copy, high, low)):
        l = jnp.where(narrow, jnp.where(upper, a, 0.0), jnp.where(upper, 0.0, b)).reshape(256, 128)
        parts = []
        for _ in range(3):
            parts.append(l.astype(BF16))
            l = l - parts[-1].astype(F32)
        copy.wait()
        right = copy.dst_ref[...].astype(F32).reshape(256, 896).astype(BF16)
        g = lax.dot_general(jnp.concatenate(parts, axis=1), right, TN, preferred_element_type=F32)
        total = total + g[0:128] + g[128:256] + g[256:384]
    query_ref[...] = total[0:56]
    out_ref[...] = total[64:120]


def loaded(kernel, smem, n_in, n_out, direct, lazy):
    def body(*refs):
        scalars, refs = refs[:smem], refs[smem:]
        ins, outs, refs = refs[:n_in], refs[n_in : n_in + n_out], refs[n_in + n_out :]
        space, refs = list(refs[: n_in - len(direct)]), refs[n_in - len(direct) :]
        results, (*rest, sems) = refs[:n_out], refs[n_out:]
        held, copies = [], []
        for i, ref in enumerate(ins):
            if i in direct:
                held.append(ref)
                continue
            copies.append((i, pltpu.make_async_copy(ref, space.pop(0), sems.at[i])))
            held.append(copies[-1][1] if i in lazy else copies[-1][1].dst_ref)
        for _, copy in copies:
            copy.start()
        for i, copy in copies:
            if i not in lazy:
                copy.wait()
        kernel(*scalars, *held, *results, *rest)
        copies = [pltpu.make_async_copy(b, a, sems.at[n_in + i]) for i, (a, b) in enumerate(zip(outs, results))]
        for copy in copies:
            copy.start()
        for copy in copies:
            copy.wait()

    return body


def call(kernel, out, args, smem=0, flops=10**9, scratch=(), load=True, direct=(), lazy=()):
    outs = out if isinstance(out, (list, tuple)) else [out]
    ins = args[smem:]
    scratch = list(scratch)
    if load:
        kernel = loaded(kernel, smem, len(ins), len(outs), direct, lazy)
        moved = [a for i, a in enumerate(ins) if i not in direct]
        scratch = [pltpu.VMEM(a.shape, a.dtype) for a in (*moved, *outs)] + scratch
        scratch.append(pltpu.SemaphoreType.DMA((len(ins) + len(outs),)))
    hbm = pl.BlockSpec(memory_space=pltpu.HBM)
    return pl.pallas_call(
        kernel,
        out_shape=out,
        in_specs=[pl.BlockSpec(memory_space=pltpu.SMEM)] * smem
        + [pl.BlockSpec(memory_space=pltpu.VMEM) if i in direct else hbm for i in range(len(ins))],
        out_specs=jax.tree.map(lambda _: hbm, out),
        scratch_shapes=scratch,
        cost_estimate=pl.CostEstimate(flops=flops, bytes_accessed=2 * 10**6, transcendentals=0),
    )(*args)


def shape(s, t=BF16):
    return jax.ShapeDtypeStruct(s, t)


def after(x, y):
    return lax.optimization_barrier((x, y))[0]


def ints(*values):
    return jnp.stack([jnp.asarray(v, jnp.int32) for v in values])


GROUPS = ((0, 1, 7, 2, 6), (3, 5, 4))
VIA_UP = (2, 1)


def per_device(
    tokens,
    target,
    w_query,
    w_key,
    w_value,
    w_out,
    query_left_factors,
    query_right_factors,
    o_left,
    o_right,
    member_ids,
):
    tok = tokens.shape[0]
    feats = w_query.shape[1]
    heads = feats // HEAD_DIM
    x, z, c = (lax.axis_index(a) for a in POP)
    y = lax.axis_index("mp")
    k = x * 8 + z
    p = 2 * k + c
    odd = member_ids[0] % 2
    half = jnp.where(odd == 0, 0.5, -0.5).astype(BF16)
    twice = jnp.where(odd == 0, 2.0, -2.0).astype(BF16)
    left_t = query_left_factors[0].T

    sent = call(
        front_kernel,
        shape((32, 8, 1920)),
        (ints(p, odd), tokens, w_query, left_t, query_right_factors[0], o_left[0].T),
        smem=1,
        scratch=[pltpu.VMEM((256, feats), F32)],
    )
    recv = lax.all_to_all(sent, CHIPS, 0, 0, tiled=True)

    w_t, parts = after(w_out.T, sent), []
    z1, z7, z2, z6, z3, z5, z4 = [shift(w_t, "pop_1", 8, e) for e in (1, 7, 2, 6, 3, 5, 4)]
    o1, o3, o2 = [shift(w_t, "pop_0", 4, d)[None] for d in (1, 3, 2)]
    for i, ins in enumerate(([z1, z7, z2, z6], [z3, z5, z4])):
        n, via = len(ins), VIA_UP[i]
        own = jnp.stack(ins)
        up, down = shift(own, "pop_0", 4, 1), shift(own, "pop_0", 4, 3)
        far = [shift(up[:via], "pop_0", 4, 1), shift(down[via:], "pop_0", 4, 3)]
        if i == 0:
            parts.append([[w_t[None], own], [o1, up], [o3, down], [o2, *far]])
        else:
            parts.append([[own], [up], [down], far])
    where = ints(c, *[(x + d - y) % 4 for d in (0, -1, 1, 2)])

    cos_all, sin_all = tables(jnp.arange(tok, dtype=F32), HEAD_DIM)
    k32 = jnp.dot(tokens, w_key, preferred_element_type=F32)
    keys = (k32 * cos_all + jnp.roll(k32, 64, axis=1) * sin_all).astype(BF16)
    values = jnp.dot(tokens, w_value, preferred_element_type=F32).astype(BF16)
    cos8, sin8 = tables((k * 8).astype(F32) + jnp.arange(8, dtype=F32), HEAD_DIM)

    half_base = jnp.sum(recv[:, :, :feats].astype(F32), axis=0)
    mixed = call(
        functools.partial(attention_kernel, heads),
        shape((272, feats)),
        (ints(k * 8), recv, half_base, swap(half_base), keys, values, cos8, sin8),
        smem=1,
        direct=(1, 2),
    )
    mixed_b = swap(mixed)

    outs = []
    for i, (group, pieces) in enumerate(zip(GROUPS, parts)):
        outs.append(
            call(
                functools.partial(project_kernel, [[a.shape[0] for a in of] for of in pieces]),
                [shape((7 * len(group) + 2 - 2 * i, 8, 512))] * 4,
                (where, *sum(pieces, []), mixed, mixed_b),
                smem=1,
                scratch=[
                    pltpu.VMEM((4, len(group), 56, feats), BF16),
                    pltpu.VMEM((512, feats), BF16),
                    pltpu.VMEM((2, 16, feats), BF16),
                    pltpu.VMEM((4, 7 * len(group) + 2 - 2 * i, 8, 512), BF16),
                    pltpu.SemaphoreType.DMA((17,)),
                ],
                load=False,
            )
        )
    mets = []
    for out in outs:
        mets.append([out[0]] + [shift(out[s], "mp", 4, s) for s in (1, 3, 2)])

    order = jnp.array([e for group in GROUPS for e in group])
    which = (jnp.arange(8)[:, None] - order[None]) % 8
    o_r = after(o_right[0], sent)
    o_cut = lax.dynamic_slice(o_r, (0, feats * y), (RANK, feats)).reshape(RANK, 8, 2, 56) * half
    one = (which[:, :, None] == jnp.arange(8)).astype(BF16)
    o_cut = jnp.einsum("kiz,rzcf->kcrif", one, o_cut, preferred_element_type=F32).astype(BF16)
    o_cut = jnp.where(c == 0, o_cut, o_cut[:, ::-1]).reshape(1, 8, 8, 448)
    o_cut = jnp.broadcast_to(o_cut, (4, 8, 8, 448)).reshape(32, 8, 448)

    def cut(a):
        a = jnp.moveaxis((a * twice).reshape(RANK, 32, 2, 56), 0, 2)
        return jnp.where(c == 0, a, a[:, ::-1]).reshape(32, 8, 56)

    gap = jnp.zeros((32, 8, 8), BF16)
    late = [cut(after(left_t, sent)), gap, cut(o_r), gap, o_cut, jnp.zeros((32, 8, 64), BF16)]
    late = jnp.concatenate(late, axis=2)
    late = lax.all_to_all(late, CHIPS, 0, 0, tiled=True)
    late_b = swap(late[:, 4:])
    late = jnp.concatenate([late[:, :4], late_b], axis=1)
    factors = after(recv, outs[0][0])[:, :, 1024:1920]
    factors_b = swap(factors)
    lefts = late[:, :, :128]
    goal = lax.dynamic_slice(target, (8 * k, 0), (8, feats)).reshape(8, 8, 2, 56)
    goal = jnp.where(c == 0, goal[:, :, 0], goal[:, :, 1])
    here = (((z - order) % 8)[:, None] == jnp.arange(8)).astype(BF16)
    goal = jnp.einsum("iz,tzf->tif", here, goal, preferred_element_type=F32).astype(BF16).reshape(8, 448)
    n = 56 * len(GROUPS[0])
    right = [late[:, :, 128 : 128 + n].reshape(256, n), late[:, :, 128 + n : 576].reshape(256, 448 - n)]
    err, rest = call(
        error_kernel,
        [shape((8, 512), F32), shape((448 - n, 512), F32)],
        (ints(c), *mets[0], right[0], goal[:, :n], right[1], goal[:, n:]),
        smem=1,
    )
    err = call(last_error_kernel, shape((32, 1, 512), F32), (*mets[1], rest, err))

    err = lax.all_to_all(err, ("pop_0", "pop_2", "mp"), 0, 0, tiled=True)
    err = jnp.sum(err, axis=0, keepdims=True)
    err = lax.all_to_all(jnp.broadcast_to(err, (8, 1, 512)), "pop_1", 0, 0, tiled=True)
    grad_query, grad_out, fitness = call(
        final_kernel,
        [shape((56, feats), F32), shape((56, feats), F32), shape((1, 128), F32)],
        (ints(c, k), err, lefts, factors, factors_b),
        smem=1,
        direct=(0, 1),
        lazy=(2, 3),
    )
    return (grad_query, grad_out.T, fitness[0, :1])


def solution(mesh):
    torus = Mesh(mesh.devices.reshape(4, 8, 2, mesh.shape["mp"]), ("pop_0", "pop_1", "pop_2", "mp"))
    placed = (
        P(),
        P(None, "mp"),
        P(POP, "mp"),
        P(None, "mp"),
        P(None, "mp"),
        P("mp", POP),
        P(POP, None, None),
        P(POP, None, "mp"),
        P(POP, "mp", None),
        P(POP, None, None),
        P(POP),
    )
    return jax.shard_map(
        per_device,
        mesh=torus,
        in_specs=placed,
        out_specs=(P(POP, "mp"), P("mp", POP), P(POP)),
        check_vma=False,
    )
```
